32 devices in a mesh: grp: 2 (over core), seq: 4 (over z), fsdp: 4 (over y, x).
Axes of the slice: x: 2, y: 2, z: 4, core: 2. Of those that a mesh axis runs over, the one named last changes fastest.
Arguments:
- inputs: bfloat16 [8, 1024, 1280], P(('grp', 'fsdp'), 'seq'), may hold values from -6 to 6
- segments: int32 [8, 1024], P(('grp', 'fsdp')), may hold values from 0 to 8, as said below
- w_qkv: bfloat16 [1280, 3840], P('fsdp'), may hold values from -0.15625 to 0.15625
- w_out: bfloat16 [1280, 1280], P('fsdp'), may hold values from -0.15625 to 0.15625
- w_upgate: bfloat16 [1280, 10240], P('fsdp'), may hold values from -0.15625 to 0.15625
- w_down: bfloat16 [5120, 1280], P('fsdp'), may hold values from -0.078125 to 0.078125
- s_qk: float32 [1280], replicated, may hold values from 1 to 1.8
- alpha_attn: float32 [1280], replicated, may hold values from 0.15 to 0.6
- alpha_mlp: float32 [1280], replicated, may hold values from 0.15 to 0.6
- s_up: float32 [5120], replicated, may hold values from 0.5 to 2
- s_gate: float32 [5120], replicated, may hold values from 0.5 to 2
- cotangent: bfloat16 [8, 1024, 1280], P(('grp', 'fsdp'), 'seq'), may hold values from -6 to 6
Outputs:
- outputs: bfloat16 [8, 1024, 1280], P(('grp', 'fsdp'), 'seq')
- grad_inputs: float32 [8, 1024, 1280], P(('grp', 'fsdp'), 'seq')
- grad_w_qkv: float32 [1280, 3840], P('fsdp')
- grad_w_out: float32 [1280, 1280], P('fsdp')
- grad_w_upgate: float32 [1280, 10240], P('fsdp')
- grad_w_down: float32 [5120, 1280], P('fsdp')
- grad_s_qk: float32 [1280], P('fsdp')
- grad_alpha_attn: float32 [1280], P('fsdp')
- grad_alpha_mlp: float32 [1280], P('fsdp')
- grad_s_up: float32 [5120], P('fsdp')
- grad_s_gate: float32 [5120], P('fsdp')
The draws below stay inside these ranges and needn't reach their ends.
Inputs may be any that keep to these rules, and one draw needn't show every extreme that they name: In every group the first 512 tokens have segment 0; the other tokens hold segments 1 to 8 in rising order, each a nonempty run.
All inputs are finite; a program needn't handle non-finite values.
Results may differ from the reference program's by a relative error of at most 0.022.
Values may be sent and summed in bfloat16 or wider, within the bound.
A program may use at most 256 MiB of HBM per device.

```python
import math
import jax
import jax.numpy as jnp
from jax import lax

D = 1280
HEADS = 20
HEAD = 64
FF = 5120
CONTS = 8
GTOK = 1024
PROMPT = 512
CONT = 64
GROUPS = 8


def draw_one_group(group_key):
    half_len = CONT // 2
    spare_rows = GTOK - PROMPT - CONTS * half_len
    cut_points = jnp.sort(jax.random.randint(group_key, (CONTS - 1,), 0, spare_rows + 1))
    bounds = jnp.arange(1, CONTS, dtype=jnp.int32) * half_len + cut_points
    offsets = jnp.arange(GTOK, dtype=jnp.int32) - PROMPT
    inside = 1 + jnp.sum((offsets[:, None] >= bounds[None, :]).astype(jnp.int32), axis=1)
    return jnp.where(offsets < 0, 0, inside).astype(jnp.int32)


def draw_segments(key, part):
    group_keys = jax.random.split(jax.random.fold_in(key, 11), GROUPS)
    return jax.vmap(draw_one_group)(group_keys)


def levels(rng, shape, pieces, low, high):
    gain = 1.0
    for position, parts in pieces:
        heights = jax.random.uniform(jax.random.fold_in(jax.random.fold_in(rng, 6), position), (parts,), jnp.float32, low / len(pieces), high / len(pieces))
        gain = gain * jnp.repeat(jnp.exp(heights), shape[position] // parts).reshape((-1,) + (1,) * (len(shape) - 1 - position))
    return gain


def gaussian(key, dims, spread, limit, pieces=(), held_as=jnp.bfloat16):
    entries = spread * jax.random.normal(key, dims, jnp.float32)
    if pieces:
        entries = entries * levels(key, dims, pieces, -0.22, 0.18)
    return jnp.clip(entries, -limit, limit).astype(held_as)


def setup_inputs(seed: int = 0) -> dict:
    key_of = jax.random.split(jax.random.key(seed), 13)
    return {
        "inputs": gaussian(key_of[0], (GROUPS, GTOK, D), 1.0, 6.0, ((0, 8), (1, 4))),
        "segments": draw_segments(jax.random.fold_in(key_of[12], 71), 0),
        "w_qkv": gaussian(key_of[2], (D, 3 * D), D ** -0.5, 0.15625, ((0, 4),)),
        "w_out": gaussian(key_of[3], (D, D), D ** -0.5, 0.15625, ((0, 4),)),
        "w_upgate": gaussian(key_of[4], (D, 2 * FF), D ** -0.5, 0.15625, ((0, 4),)),
        "w_down": gaussian(key_of[5], (FF, D), FF ** -0.5, 0.078125, ((0, 4),)),
        "s_qk": jnp.clip(jnp.exp(jax.random.uniform(key_of[6], (D,), jnp.float32, math.log(1.0), math.log(1.8))), 1.0, 1.8),
        "alpha_attn": jnp.clip(jnp.exp(jax.random.uniform(key_of[7], (D,), jnp.float32, math.log(0.15), math.log(0.6))), 0.15, 0.6),
        "alpha_mlp": jnp.clip(jnp.exp(jax.random.uniform(key_of[8], (D,), jnp.float32, math.log(0.15), math.log(0.6))), 0.15, 0.6),
        "s_up": jnp.clip(jnp.exp(jax.random.uniform(key_of[9], (FF,), jnp.float32, math.log(0.5), math.log(2.0))), 0.5, 2.0),
        "s_gate": jnp.clip(jnp.exp(jax.random.uniform(key_of[10], (FF,), jnp.float32, math.log(0.5), math.log(2.0))), 0.5, 2.0),
        "cotangent": gaussian(key_of[11], (GROUPS, GTOK, D), 1.0, 6.0, ((0, 8), (1, 4))),
    }


@jax.custom_vjp
def low(v):
    return lax.optimization_barrier(v.astype(jnp.bfloat16)).astype(jnp.float32)

@jax.custom_vjp
def low_back(v):
    return v

def low_keep(v):
    return (low(v), None)

def low_pass(kept, grad):
    return (grad,)

def back_keep(v):
    return (v, None)

def back_low(kept, grad):
    return (low(grad),)
low.defvjp(low_keep, low_pass)
low_back.defvjp(back_keep, back_low)
highest = lax.Precision.HIGHEST
eps_norm = 1e-06
neg_big = -1e+30

def unit_rows(value):
    return value * lax.rsqrt(lax.optimization_barrier(jnp.mean(value * value, axis=-1, keepdims=True)) + eps_norm)

def matmul(former, latter):
    return jnp.dot(former, latter, precision=highest)

def attend(query_part, query_pos, query_seg, keys_unit, values_low, segments_row):
    key_pos = jnp.arange(keys_unit.shape[0], dtype=jnp.int32)
    scores = jnp.einsum('qhe,khe->hqk', query_part, keys_unit, precision=highest) * HEAD ** (-0.5)
    scores = low_back(scores)
    allowed = (key_pos[None, :] <= query_pos[:, None]) & ((segments_row[None, :] == 0) | (segments_row[None, :] == query_seg[:, None]))
    scores = jnp.where(allowed[None], scores, neg_big)
    row_max = lax.optimization_barrier(jnp.max(scores, axis=-1, keepdims=True))
    exponent = jnp.exp(scores - row_max)
    probs = low(exponent / lax.optimization_barrier(jnp.sum(exponent, axis=-1, keepdims=True)))
    return jnp.einsum('hqk,khe->qhe', probs, values_low, precision=highest)

def layer(inputs_f, segments_row, w_qkv, w_out, w_upgate, w_down, s_qk, alpha_attn, alpha_mlp, s_up, s_gate):
    token_count = inputs_f.shape[0]
    unit_in = unit_rows(inputs_f)
    projected = low_back(matmul(low(unit_in), w_qkv))
    gains = s_qk.reshape(HEADS, HEAD)
    query_unit = low(unit_rows(projected[:, :D].reshape(token_count, HEADS, HEAD)) * gains)
    keys_unit = low(unit_rows(projected[:, D:2 * D].reshape(token_count, HEADS, HEAD)) * gains)
    values_low = low(projected[:, 2 * D:].reshape(token_count, HEADS, HEAD))
    block_len = min(512, token_count)
    block_count = token_count // block_len
    positions = jnp.arange(token_count, dtype=jnp.int32)

    def one_block(items):
        query_part, query_pos, query_seg = items
        return attend(query_part, query_pos, query_seg, keys_unit, values_low, segments_row)
    mixture = lax.map(jax.checkpoint(one_block), (query_unit.reshape(block_count, block_len, HEADS, HEAD), positions.reshape(block_count, block_len), segments_row.reshape(block_count, block_len)))
    mixture = low_back(low(mixture.reshape(token_count, D)))
    attention = low_back(matmul(mixture, w_out))
    unit_mid = unit_rows(unit_in + alpha_attn * (unit_rows(attention) - unit_in))
    upgate = low_back(matmul(low(unit_mid), w_upgate))
    hidden = low(upgate[:, :FF] * s_up * jax.nn.silu(upgate[:, FF:] * s_gate))
    feed_out = low_back(matmul(hidden, w_down))
    return unit_rows(unit_mid + alpha_mlp * (unit_rows(feed_out) - unit_mid))

def reference(inputs, segments, w_qkv, w_out, w_upgate, w_down, s_qk, alpha_attn, alpha_mlp, s_up, s_gate, cotangent):
    weights = (w_qkv.astype(jnp.float32), w_out.astype(jnp.float32), w_upgate.astype(jnp.float32), w_down.astype(jnp.float32))
    vectors = (s_qk, alpha_attn, alpha_mlp, s_up, s_gate)

    def per_group(carry, items):
        inputs_grp, segments_grp, cotangent_grp = items

        def forward(inputs_f, weight_set, vector_set):
            return layer(inputs_f, segments_grp, weight_set[0], weight_set[1], weight_set[2], weight_set[3], vector_set[0], vector_set[1], vector_set[2], vector_set[3], vector_set[4])
        result, pullback = jax.vjp(forward, inputs_grp.astype(jnp.float32), weights, vectors)
        grad_in, grad_weights, grad_vectors = pullback(cotangent_grp.astype(jnp.float32))
        carry = jax.tree.map(jnp.add, carry, (grad_weights, grad_vectors))
        return (carry, (result.astype(jnp.bfloat16), grad_in))
    zero_grads = jax.tree.map(jnp.zeros_like, (weights, vectors))
    totals, stacked = lax.scan(per_group, zero_grads, (inputs, segments, cotangent))
    grad_weights, grad_vectors = totals
    return (stacked[0], stacked[1], grad_weights[0], grad_weights[1], grad_weights[2], grad_weights[3], grad_vectors[0], grad_vectors[1], grad_vectors[2], grad_vectors[3], grad_vectors[4])
```

```python
import jax
import jax.numpy as jnp
from jax import lax
from jax.sharding import PartitionSpec as P

D = 1280
HEADS = 20
HEAD = 64

eps_norm = 1e-06
neg_big = -1e30
BF = jnp.bfloat16
F32 = jnp.float32


def inv_rms(value):
    return lax.rsqrt(jnp.mean(value * value, axis=-1, keepdims=True) + eps_norm)


def back(unit, inv, grad):
    return (grad - unit * jnp.mean(grad * unit, axis=-1, keepdims=True)) * inv


def mm(a, b):
    return jnp.dot(a, b, preferred_element_type=F32)


def mm_nt(a, b):
    return lax.dot_general(a, b, (((1,), (1,)), ((), ())), preferred_element_type=F32)


def mm_tn(a, b):
    return lax.dot_general(a, b, (((0,), (0,)), ((), ())), preferred_element_type=F32)


def gather(x, axes, dim=0):
    return lax.all_gather(x, axes, axis=dim, tiled=True)


def scatter(x, axes, dim=0):
    return lax.psum_scatter(x, axes, scatter_dimension=dim, tiled=True)


def attention(q, k, v, seg):
    n = seg.shape[0]
    pos = jnp.arange(n, dtype=jnp.int32)
    allowed = (pos[None, :] <= pos[:, None]) & ((seg[None, :] == 0) | (seg[None, :] == seg[:, None]))
    scores = jnp.einsum("qhe,khe->hqk", q, k, preferred_element_type=F32) * HEAD**-0.5
    scores = jnp.where(allowed[None], scores, neg_big)
    top = jnp.max(scores, axis=-1, keepdims=True)
    e = jnp.exp(scores - top)
    probs = e / jnp.sum(e, axis=-1, keepdims=True)
    mix = jnp.einsum("hqk,khe->qhe", probs.astype(BF), v, preferred_element_type=F32)
    return mix, probs


def attention_back(q, k, v, probs, gx):
    gp = jnp.einsum("qhe,khe->hqk", gx, v, preferred_element_type=F32)
    delta = jnp.sum(probs * gp, axis=-1, keepdims=True)
    gs = (probs * (gp - delta)).astype(BF)
    dq = jnp.einsum("hqk,khe->qhe", gs, k, preferred_element_type=F32) * HEAD**-0.5
    dk = jnp.einsum("hqk,qhe->khe", gs, q, preferred_element_type=F32) * HEAD**-0.5
    dv = jnp.einsum("hqk,qhe->khe", probs.astype(BF), gx, preferred_element_type=F32)
    return dq, dk, dv


def body(S, FS, inputs, segments, w_qkv, w_out, w_upgate, w_down, s_qk, alpha_attn, alpha_mlp, s_up, s_gate, cotangent):
    z = lax.axis_index("seq")
    f = lax.axis_index("fsdp")
    hp = -(-HEADS // S)
    hw = hp * HEAD
    wide = S * hw
    rows = w_qkv.shape[0]
    ff = s_up.shape[0]
    fl = ff // FS

    def head_pad(a):
        return jnp.pad(a, [(0, 0)] * (a.ndim - 1) + [(0, wide - D)])

    x = inputs[0].astype(F32)
    tok = x.shape[0]
    inv_x = inv_rms(x)
    h = x * inv_x
    hb = h.astype(BF)
    seg = segments[0]
    h_all = gather(hb, "seq")
    total = h_all.shape[0]
    wq = head_pad(w_qkv.reshape(rows, 3, D)).reshape(rows, 3, S, hw)
    wq = lax.dynamic_index_in_dim(wq, z, 2, keepdims=False)
    wq = gather(wq.reshape(rows, 3 * hw), "fsdp")
    wo = gather(w_out, "fsdp")
    wu = lax.all_to_all(w_upgate.reshape(rows, 2, FS, fl), "fsdp", split_axis=2, concat_axis=0, tiled=True)
    wu = wu.reshape(D, 2 * fl)
    gain = lax.dynamic_slice_in_dim(head_pad(s_qk), z * hw, hw).reshape(hp, HEAD)
    qkv = mm(h_all, wq).reshape(total, 3, hp, HEAD)
    inv_qk = inv_rms(qkv[:, :2])
    u_qk = qkv[:, :2] * inv_qk
    n_qk = (u_qk * gain).astype(BF)
    q, k, v = n_qk[:, 0], n_qk[:, 1], qkv[:, 2].astype(BF)
    mix, probs = attention(q, k, v, seg)
    mixb = mix.reshape(total, hw).astype(BF)
    mine = lax.all_to_all(mixb, "seq", split_axis=0, concat_axis=1, tiled=True)[:, :D]
    attn = mm(mine, wo)
    inv_a = inv_rms(attn)
    ua = attn * inv_a
    n = h + alpha_attn * (ua - h)
    inv_n = inv_rms(n)
    mid = n * inv_n
    midb = mid.astype(BF)
    mid_all = gather(midb, "fsdp")
    ug = mm(mid_all, wu)
    up, gate = ug[:, :fl], ug[:, fl:]
    su = lax.dynamic_slice_in_dim(s_up, f * fl, fl)
    sg = lax.dynamic_slice_in_dim(s_gate, f * fl, fl)
    a = gate * sg
    sig = jax.nn.sigmoid(a)
    silu = a * sig
    hidden = (up * su * silu).astype(BF)
    mlp = scatter(mm(hidden, w_down).astype(BF), "fsdp").astype(F32)
    inv_m = inv_rms(mlp)
    um = mlp * inv_m
    m = mid + alpha_mlp * (um - mid)
    inv_o = inv_rms(m)
    out = m * inv_o
    g = cotangent[0].astype(F32)
    g_m = back(out, inv_o, g)
    d_alpha_mlp = jnp.sum(g_m * (um - mid), axis=0)
    g_mlp = back(um, inv_m, alpha_mlp * g_m)
    g_mid1 = (1 - alpha_mlp) * g_m
    gm_all = gather(g_mlp.astype(BF), "fsdp")
    gh = mm_nt(gm_all, w_down)
    d_down = mm_tn(hidden, gm_all)
    g_up = gh * su * silu
    d_su = jnp.sum(up * gh * silu, axis=0)
    g_a = gh * up * su * sig * (1 + a * (1 - sig))
    g_gate = g_a * sg
    d_sg = jnp.sum(gate * g_a, axis=0)
    gu = jnp.concatenate([g_up, g_gate], axis=1).astype(BF)
    g_mid = g_mid1 + scatter(mm_nt(gu, wu).astype(BF), "fsdp").astype(F32)
    d_upgate = mm_tn(mid_all, gu)
    g_n = back(mid, inv_n, g_mid)
    d_alpha_attn = jnp.sum(g_n * (ua - h), axis=0)
    g_attn = back(ua, inv_a, alpha_attn * g_n)
    g_h1 = (1 - alpha_attn) * g_n
    ga = g_attn.astype(BF)
    gmix = head_pad(mm_nt(ga, wo).astype(BF))
    d_out = mm_tn(mine, ga)
    gx = lax.all_to_all(gmix, "seq", split_axis=1, concat_axis=0, tiled=True).reshape(total, hp, HEAD)
    dq, dk, dv = attention_back(q, k, v, probs, gx)
    g_qk = jnp.stack([dq, dk], axis=1)
    d_sqk = jnp.sum(g_qk * u_qk, axis=(0, 1)).reshape(hw)
    g_raw = back(u_qk, inv_qk, g_qk * gain)
    gq = jnp.concatenate([g_raw, dv[:, None]], axis=1).reshape(total, 3 * hw).astype(BF)
    g_h = g_h1 + scatter(mm_nt(gq, wq).astype(BF), "seq").astype(F32)
    d_qkv = mm_tn(h_all, gq)
    g_x = back(h, inv_x, g_h)

    d_down = lax.psum(d_down.astype(BF), ("grp", "seq")).astype(F32)
    d_up = scatter(d_upgate.astype(BF), "grp", 1)
    d_up = scatter(d_up, "seq", 1)
    part = d_up.shape[1]
    d_up = lax.all_to_all(d_up, "fsdp", split_axis=0, concat_axis=1, tiled=True)
    d_up = gather(gather(d_up.reshape(rows, FS, part), "seq", 2), "grp", 2)
    d_up = d_up.reshape(rows, FS, 2, fl).transpose(0, 2, 1, 3).reshape(rows, 2 * ff).astype(F32)
    d_o = scatter(d_out.astype(BF), "fsdp")
    d_o = lax.psum(d_o, ("grp", "seq")).astype(F32)
    d_q = scatter(d_qkv.astype(BF), "fsdp")
    d_q = lax.psum(d_q, "grp")
    d_q = gather(d_q.reshape(rows, 3, hw), "seq", 2)[:, :, :D].reshape(rows, 3 * D).astype(F32)
    slot = jnp.zeros((2, FS, fl), F32)
    slot = lax.dynamic_update_slice(slot, jnp.stack([d_su, d_sg])[:, None], (0, f, 0)).reshape(-1)
    slot_qk = lax.dynamic_update_slice(jnp.zeros((wide,), F32), d_sqk, (z * hw,))[:D]
    flat = lax.psum(jnp.concatenate([slot_qk, d_alpha_attn, d_alpha_mlp, slot]), ("grp", "seq", "fsdp"))

    def own(start, size):
        return lax.dynamic_slice_in_dim(flat, start + f * (size // FS), size // FS)

    return (
        out.astype(BF)[None], g_x[None], d_q, d_o, d_up, d_down,
        own(0, D), own(D, D), own(2 * D, D), own(3 * D, ff), own(3 * D + ff, ff),
    )


def solution(mesh):
    S, FS = mesh.shape["seq"], mesh.shape["fsdp"]
    tok = P(("grp", "fsdp"), "seq", None)
    w = P("fsdp", None)
    in_specs = (tok, P(("grp", "fsdp"), None), w, w, w, w, P(), P(), P(), P(), P(), tok)
    out_specs = (tok, tok, w, w, w, w) + (P("fsdp"),) * 5

    def run(*args):
        return body(S, FS, *args)

    return jax.shard_map(run, mesh=mesh, in_specs=in_specs, out_specs=out_specs, check_vma=False)
```

```python
import jax
import jax.numpy as jnp
from jax import lax
from jax.experimental import pallas as pl
from jax.experimental.pallas import tpu as pltpu
from jax.sharding import PartitionSpec as P

D = 1280
HEADS = 20
HEAD = 64

eps_norm = 1e-06
neg_big = -1e30
BF = jnp.bfloat16
F32 = jnp.float32
MESH = pl.DeviceIdType.MESH
ANY = pl.BlockSpec(memory_space=pl.ANY)
VM = pl.BlockSpec(memory_space=pltpu.VMEM)


def inv_rms(value):
    return lax.rsqrt(jnp.mean(value * value, axis=-1, keepdims=True) + eps_norm)


def back(unit, inv, grad):
    return (grad - unit * jnp.mean(grad * unit, axis=-1, keepdims=True)) * inv


def mm(a, b):
    return jnp.dot(a, b, preferred_element_type=F32)


def mm_nt(a, b):
    return lax.dot_general(a, b, (((1,), (1,)), ((), ())), preferred_element_type=F32)


def mm_tn(a, b):
    return lax.dot_general(a, b, (((0,), (0,)), ((), ())), preferred_element_type=F32)


def rcopy(src, dst, ss, rs, dev):
    return pltpu.make_async_remote_copy(src, dst, ss, rs, device_id=dev, device_id_type=MESH)


def greet(peers):
    bar = pltpu.get_barrier_semaphore()
    for p in peers:
        pl.semaphore_signal(bar, inc=1, device_id=p, device_id_type=MESH)
    pl.semaphore_wait(bar, len(peers))


def ds(start, size, mult):
    return pl.ds(pl.multiple_of(start, mult), size)


def visible(seg_col, seg_row, q0, k0, nq, nk):
    qi = q0 + lax.broadcasted_iota(jnp.int32, (nq, nk), 0)
    ki = k0 + lax.broadcasted_iota(jnp.int32, (nq, nk), 1)
    return (ki <= qi) & ((seg_row == 0) | (seg_row == seg_col))


def attn_bias(S, tok, half, bias, segc, segr):
    for qb in range(S):
        q0 = qb * tok
        k0 = q0 if q0 < half else half
        nk = q0 + tok - k0
        ok = visible(segc[q0 : q0 + tok], segr[:, k0 : k0 + nk], q0, k0, tok, nk)
        bias[qb, :, :nk] = jnp.where(ok, 0.0, neg_big)


def first_kernel(S, FS, hp, x_ref, segc, segr, wqkv, wout, gain, alpha, wup,
                 hall_o, wq_o, wo_o, wu_o, raw_o, qkv_o, res_o, mine_o, attn_o, mid_o,
                 hall, wq, wo, raw, qkv, res, bias, oh, mixs, mine, recv,
                 s_up, r_up, s_dn, r_dn, s_wq, r_wq, s_wo, r_wo, s_wu, r_wu, f_wq, f_wo, f_wu,
                 g_wq, g_wo, g_wu, s_mx, r_mx, out_sem):
    g, z, f = lax.axis_index("grp"), lax.axis_index("seq"), lax.axis_index("fsdp")
    tok = x_ref.shape[0]
    rows = wqkv.shape[0]
    hr = rows // 2
    hw = hp * HEAD
    ff = wup.shape[1] // 2
    fl = ff // FS
    total = S * tok
    half = total // 2
    fpeers = [lax.rem(f + i, FS) for i in range(1, FS)]
    zpeers = [lax.rem(z + i, S) for i in range(1, S)]
    greet([(g, z, p) for p in fpeers] + [(g, p, f) for p in zpeers] + [(1 - g, z, f)])

    x = x_ref[...].astype(F32)
    hall[z] = (x * inv_rms(x)).astype(BF)

    def up(t, b):
        return rcopy(hall.at[b], hall.at[b], s_up.at[t], r_up.at[t], (g, lax.rem(z + 1, S), f))

    def down(t, b):
        return rcopy(hall.at[b], hall.at[b], s_dn.at[t], r_dn.at[t], (g, lax.rem(z + S - 1, S), f))

    @pl.when(z + 1 < S)
    def _():
        up(0, z).start()

    @pl.when(z > 0)
    def _():
        down(0, z).start()

    for k in range(S):
        lo, hi = k * hw, min((k + 1) * hw, D)

        @pl.when(z == k)
        def _():
            parts = []
            for c in range(3):
                if hi > lo:
                    parts.append(wqkv[:, c * D + lo : c * D + hi])
                if hi - lo < hw:
                    parts.append(jnp.zeros((rows, hw - max(hi - lo, 0)), BF))
            wq[ds(f * rows, rows, 16)] = jnp.concatenate(parts, axis=1)

    def wq_half(src, gg):
        return wq.at[ds(src * rows + gg * hr, hr, 16)]

    def wo_half(src, gg):
        return wo.at[ds(src * rows + gg * hr, hr, 16)]

    c_wq = [rcopy(wq_half(f, g), wq_half(f, g), s_wq.at[i], r_wq.at[i], (g, z, p)) for i, p in enumerate(fpeers)]
    for c in c_wq:
        c.start()
    attn_bias(S, tok, half, bias, segc, segr)
    wo[ds(f * rows, rows, 16)] = wout[...]
    qkv[2, :, :, HEAD:] = jnp.where(lax.broadcasted_iota(jnp.int32, (hp, total, HEAD), 2) == 0, 1.0, 0.0).astype(BF)

    bpeers = [lax.rem(f + FS - i, FS) for i in range(1, FS)]
    partner = (1 - g, z, f)
    fw_wq = [rcopy(wq_half(p, g), wq_half(p, g), f_wq.at[i], g_wq.at[i], partner) for i, p in enumerate(bpeers)]
    for i in range(FS - 1):
        c_wq[i].wait_recv()
        fw_wq[i].start()
    c_wo = [rcopy(wo_half(f, g), wo_half(f, g), s_wo.at[i], r_wo.at[i], (g, z, p)) for i, p in enumerate(fpeers)]
    for c in c_wo:
        c.start()

    def wu_cp(i, p):
        return rcopy(wup.at[:, ds(g * ff + p * fl, fl, 128)], wu_o.at[g, f], s_wu.at[i], r_wu.at[i], (g, z, p))

    c_wu = [wu_cp(i, p) for i, p in enumerate(fpeers)]
    for c in c_wu:
        c.start()
    for i in range(FS - 1):
        fw_wq[i].wait_recv()

    def step(i, carry):
        t = lax.div(i - 1, 2)
        is_up = lax.rem(i, 2) == 1
        b = jnp.where(i == 0, z, jnp.where(is_up, z - 1 - t, z + 1 + t))

        @pl.when((b >= 0) & (b < S))
        def _():
            @pl.when((i > 0) & is_up)
            def _():
                up(t, b).wait_recv()

                @pl.when(z + 1 < S)
                def _():
                    up(t + 1, b).start()

            @pl.when((i > 0) & jnp.logical_not(is_up))
            def _():
                down(t, b).wait_recv()

                @pl.when(z > 0)
                def _():
                    down(t + 1, b).start()

            acc = mm(hall[b], wq[...])
            at = ds(b * tok, tok, 16)
            for j in range(hp):
                for c in range(2):
                    v = acc[:, c * hw + j * HEAD : c * hw + (j + 1) * HEAD]
                    raw[c, j, at, :] = v
                    u = v * inv_rms(v) * gain[j : j + 1]
                    qkv[c, j, at, :HEAD] = u.astype(BF)
                qkv[2, j, at, :HEAD] = acc[:, 2 * hw + j * HEAD : 2 * hw + (j + 1) * HEAD].astype(BF)

        return carry

    lax.fori_loop(0, 2 * S - 1, step, 0)
    outs = [
        pltpu.make_async_copy(hall, hall_o, out_sem.at[0]),
        pltpu.make_async_copy(wq, wq_o, out_sem.at[1]),
        pltpu.make_async_copy(raw, raw_o, out_sem.at[2]),
        pltpu.make_async_copy(qkv, qkv_o, out_sem.at[3]),
    ]
    for c in outs:
        c.start()

    def mx(qb):
        return rcopy(mixs.at[qb], recv.at[z], s_mx.at[qb], r_mx.at[z], (g, qb, f))

    for qb in reversed(range(S)):
        q0 = qb * tok
        n = q0 + tok
        k0 = q0 if q0 < half else half

        def head(j, carry):
            q = qkv[0, j, q0:n, :HEAD] * jnp.asarray(HEAD**-0.5, BF)
            s = mm_nt(q, qkv[1, j, :n, :HEAD])
            tail = s[:, k0:] + bias[qb, :, : n - k0]
            e = jnp.exp(jnp.concatenate([s[:, :k0], tail], axis=1) if k0 else tail)
            o = mm(e.astype(BF), qkv[2, j, :n])
            rinv = 1.0 / o[:, HEAD : HEAD + 1]
            o = o[:, :HEAD] * rinv
            res[j, q0:n, :HEAD] = o
            res[j, q0:n, HEAD:] = jnp.broadcast_to(rinv, (tok, HEAD))
            oh[j] = o.astype(BF)
            return carry

        lax.fori_loop(0, hp, head, 0)
        block = jnp.concatenate([oh[j] for j in range(hp)], axis=1)
        mixs[qb] = block

        @pl.when(z != qb)
        def _():
            mx(qb).start()

        @pl.when(z == qb)
        def _():
            recv[qb] = block

        if qb == S - 1:
            fw_wo = [rcopy(wo_half(p, g), wo_half(p, g), f_wo.at[i], g_wo.at[i], partner) for i, p in enumerate(bpeers)]
            for i in range(FS - 1):
                c_wo[i].wait_recv()
                fw_wo[i].start()

    fw_wu = [rcopy(wu_o.at[g, p], wu_o.at[g, p], f_wu.at[i], g_wu.at[i], partner) for i, p in enumerate(bpeers)]
    for i in range(FS - 1):
        c_wu[i].wait_recv()
        fw_wu[i].start()
    for i in range(FS - 1):
        fw_wo[i].wait_recv()
    outs2 = [pltpu.make_async_copy(wo, wo_o, out_sem.at[4]), pltpu.make_async_copy(res, res_o, out_sem.at[5])]
    for c in outs2:
        c.start()
    for k in range(S):
        @pl.when(z != k)
        def _():
            rcopy(mixs.at[0], recv.at[k], s_mx.at[0], r_mx.at[k], (g, k, f)).wait_recv()

    mine[...] = jnp.concatenate([recv[k] for k in range(S)], axis=1)[:, :D]
    attn = mm(mine[...], wo[...])
    attn_o[...] = attn
    mine_o[...] = mine[...]
    x = x_ref[...].astype(F32)
    h = x * inv_rms(x)
    n_ = h + alpha[...] * (attn * inv_rms(attn) - h)
    mid_o[...] = (n_ * inv_rms(n_)).astype(BF)

    for t in range(S - 1):
        @pl.when((z + 1 < S) & (z - t >= 0))
        def _():
            up(t, z).wait_send()

        @pl.when((z > 0) & (z + t < S))
        def _():
            down(t, z).wait_send()

    for i in range(FS - 1):
        c_wq[i].wait_send()
        c_wo[i].wait_send()
        c_wu[i].wait_send()
        fw_wq[i].wait_send()
        fw_wo[i].wait_send()
        fw_wu[i].wait()
    for k in range(S):
        @pl.when(z != k)
        def _():
            mx(k).wait_send()
    for c in outs + outs2:
        c.wait()


def first(S, FS, hp, x, seg, wqkv, wout, gain, alpha, wup):
    tok, total = x.shape[0], seg.shape[0]
    rows = wqkv.shape[0]
    hw = hp * HEAD
    fl = wup.shape[1] // 2 // FS
    sds = jax.ShapeDtypeStruct
    outs = [
        sds((S, tok, D), BF), sds((D, 3 * hw), BF), sds((D, D), BF), sds((2, FS, rows, fl), BF),
        sds((2, hp, total, HEAD), F32), sds((3, hp, total, 2 * HEAD), BF), sds((hp, total, 2 * HEAD), F32),
        sds((tok, D), BF), sds((tok, D), F32), sds((tok, D), BF),
    ]
    dma = lambda n: pltpu.SemaphoreType.DMA((n,))
    F1 = FS - 1
    return pl.pallas_call(
        lambda *refs: first_kernel(S, FS, hp, *refs),
        out_shape=outs,
        in_specs=[VM] * 7 + [ANY],
        out_specs=[ANY] * 7 + [VM] * 3,
        scratch_shapes=[
            pltpu.VMEM((S, tok, D), BF), pltpu.VMEM((D, 3 * hw), BF), pltpu.VMEM((D, D), BF),
            pltpu.VMEM((2, hp, total, HEAD), F32), pltpu.VMEM((3, hp, total, 2 * HEAD), BF),
            pltpu.VMEM((hp, total, 2 * HEAD), F32), pltpu.VMEM((S, tok, total // 2), F32),
            pltpu.VMEM((hp, tok, HEAD), BF), pltpu.VMEM((S, tok, hw), BF), pltpu.VMEM((tok, D), BF),
            pltpu.VMEM((S, tok, hw), BF),
            dma(S), dma(S), dma(S), dma(S), dma(F1), dma(F1), dma(F1), dma(F1), dma(F1), dma(F1),
            dma(F1), dma(F1), dma(F1), dma(F1), dma(F1), dma(F1), dma(S), dma(S), dma(6),
        ],
        compiler_params=pltpu.CompilerParams(collective_id=1, has_side_effects=True, vmem_limit_bytes=60 * 2**20),
        name="first",
    )(x, seg.reshape(total, 1), seg.reshape(1, total), wqkv, wout, gain, alpha.reshape(1, D), wup)


def gather(x, axes, dim=0):
    return lax.all_gather(x, axes, axis=dim, tiled=True)


def scatter(x, axes, dim=0):
    return lax.psum_scatter(x, axes, scatter_dimension=dim, tiled=True)


def attention_back(q, k, v, probs, gx):
    gp = jnp.einsum("qhe,khe->hqk", gx, v, preferred_element_type=F32)
    delta = jnp.sum(probs * gp, axis=-1, keepdims=True)
    gs = (probs * (gp - delta)).astype(BF)
    dq = jnp.einsum("hqk,khe->qhe", gs, k, preferred_element_type=F32) * HEAD**-0.5
    dk = jnp.einsum("hqk,qhe->khe", gs, q, preferred_element_type=F32) * HEAD**-0.5
    dv = jnp.einsum("hqk,qhe->khe", probs.astype(BF), gx, preferred_element_type=F32)
    return dq, dk, dv


def body(S, FS, inputs, segments, w_qkv, w_out, w_upgate, w_down, s_qk, alpha_attn, alpha_mlp, s_up, s_gate, cotangent):
    z = lax.axis_index("seq")
    f = lax.axis_index("fsdp")
    hp = -(-HEADS // S)
    hw = hp * HEAD
    wide = S * hw
    rows = w_qkv.shape[0]
    ff = s_up.shape[0]
    fl = ff // FS

    def head_pad(a):
        return jnp.pad(a, [(0, 0)] * (a.ndim - 1) + [(0, wide - D)])

    x = inputs[0].astype(F32)
    tok = x.shape[0]
    inv_x = inv_rms(x)
    h = x * inv_x
    seg = segments[0]
    total = seg.shape[0]
    gain = lax.dynamic_slice_in_dim(head_pad(s_qk), z * hw, hw).reshape(hp, HEAD)
    h_all, wq, wo, wu4, raw, qkv, res, mine, attn, _ = first(
        S, FS, hp, inputs[0], seg, w_qkv, w_out, gain, alpha_attn, w_upgate
    )
    h_all = h_all.reshape(total, D)
    own = lax.dynamic_slice_in_dim(w_upgate.reshape(rows, 2, ff), f * fl, fl, 2).transpose(1, 0, 2)
    wu4 = lax.dynamic_update_slice(wu4, own[:, None], (0, f, 0, 0))
    wu = wu4.transpose(1, 2, 0, 3).reshape(D, 2 * fl)
    rawt = raw.transpose(2, 0, 1, 3)
    inv_qk = inv_rms(rawt)
    u_qk = rawt * inv_qk
    q, k, v = [qkv[c, :, :, :HEAD].transpose(1, 0, 2) for c in range(3)]
    pos = jnp.arange(total, dtype=jnp.int32)
    allowed = (pos[None, :] <= pos[:, None]) & ((seg[None, :] == 0) | (seg[None, :] == seg[:, None]))
    probs = jnp.einsum("qhe,khe->hqk", q, k, preferred_element_type=F32) * HEAD**-0.5
    probs = jnp.exp(jnp.where(allowed[None], probs, neg_big)) * res[:, :, HEAD : HEAD + 1]
    inv_a = inv_rms(attn)
    ua = attn * inv_a
    n = h + alpha_attn * (ua - h)
    inv_n = inv_rms(n)
    mid = n * inv_n
    midb = mid.astype(BF)
    mid_all = gather(midb, "fsdp")
    ug = mm(mid_all, wu)
    up, gate = ug[:, :fl], ug[:, fl:]
    su = lax.dynamic_slice_in_dim(s_up, f * fl, fl)
    sg = lax.dynamic_slice_in_dim(s_gate, f * fl, fl)
    a = gate * sg
    sig = jax.nn.sigmoid(a)
    silu = a * sig
    hidden = (up * su * silu).astype(BF)
    mlp = scatter(mm(hidden, w_down).astype(BF), "fsdp").astype(F32)
    inv_m = inv_rms(mlp)
    um = mlp * inv_m
    m = mid + alpha_mlp * (um - mid)
    inv_o = inv_rms(m)
    out = m * inv_o
    g = cotangent[0].astype(F32)
    g_m = back(out, inv_o, g)
    d_alpha_mlp = jnp.sum(g_m * (um - mid), axis=0)
    g_mlp = back(um, inv_m, alpha_mlp * g_m)
    g_mid1 = (1 - alpha_mlp) * g_m
    gm_all = gather(g_mlp.astype(BF), "fsdp")
    gh = mm_nt(gm_all, w_down)
    d_down = mm_tn(hidden, gm_all)
    g_up = gh * su * silu
    d_su = jnp.sum(up * gh * silu, axis=0)
    g_a = gh * up * su * sig * (1 + a * (1 - sig))
    g_gate = g_a * sg
    d_sg = jnp.sum(gate * g_a, axis=0)
    gu = jnp.concatenate([g_up, g_gate], axis=1).astype(BF)
    g_mid = g_mid1 + scatter(mm_nt(gu, wu).astype(BF), "fsdp").astype(F32)
    d_upgate = mm_tn(mid_all, gu)
    g_n = back(mid, inv_n, g_mid)
    d_alpha_attn = jnp.sum(g_n * (ua - h), axis=0)
    g_attn = back(ua, inv_a, alpha_attn * g_n)
    g_h1 = (1 - alpha_attn) * g_n
    ga = g_attn.astype(BF)
    gmix = head_pad(mm_nt(ga, wo).astype(BF))
    d_out = mm_tn(mine, ga)
    gx = lax.all_to_all(gmix, "seq", split_axis=1, concat_axis=0, tiled=True).reshape(total, hp, HEAD)
    dq, dk, dv = attention_back(q, k, v, probs, gx)
    g_qk = jnp.stack([dq, dk], axis=1)
    d_sqk = jnp.sum(g_qk * u_qk, axis=(0, 1)).reshape(hw)
    g_raw = back(u_qk, inv_qk, g_qk * gain)
    gq = jnp.concatenate([g_raw, dv[:, None]], axis=1).reshape(total, 3 * hw).astype(BF)
    g_h = g_h1 + scatter(mm_nt(gq, wq).astype(BF), "seq").astype(F32)
    d_qkv = mm_tn(h_all, gq)
    g_x = back(h, inv_x, g_h)

    d_down = lax.psum(d_down.astype(BF), ("grp", "seq")).astype(F32)
    d_up = scatter(d_upgate.astype(BF), "grp", 1)
    d_up = scatter(d_up, "seq", 1)
    part = d_up.shape[1]
    d_up = lax.all_to_all(d_up, "fsdp", split_axis=0, concat_axis=1, tiled=True)
    d_up = gather(gather(d_up.reshape(rows, FS, part), "seq", 2), "grp", 2)
    d_up = d_up.reshape(rows, FS, 2, fl).transpose(0, 2, 1, 3).reshape(rows, 2 * ff).astype(F32)
    d_o = scatter(d_out.astype(BF), "fsdp")
    d_o = lax.psum(d_o, ("grp", "seq")).astype(F32)
    d_q = scatter(d_qkv.astype(BF), "fsdp")
    d_q = lax.psum(d_q, "grp")
    d_q = gather(d_q.reshape(rows, 3, hw), "seq", 2)[:, :, :D].reshape(rows, 3 * D).astype(F32)
    slot = jnp.zeros((2, FS, fl), F32)
    slot = lax.dynamic_update_slice(slot, jnp.stack([d_su, d_sg])[:, None], (0, f, 0)).reshape(-1)
    slot_qk = lax.dynamic_update_slice(jnp.zeros((wide,), F32), d_sqk, (z * hw,))[:D]
    flat = lax.psum(jnp.concatenate([slot_qk, d_alpha_attn, d_alpha_mlp, slot]), ("grp", "seq", "fsdp"))

    def own(start, size):
        return lax.dynamic_slice_in_dim(flat, start + f * (size // FS), size // FS)

    return (
        out.astype(BF)[None], g_x[None], d_q, d_o, d_up, d_down,
        own(0, D), own(D, D), own(2 * D, D), own(3 * D, ff), own(3 * D + ff, ff),
    )


def solution(mesh):
    S, FS = mesh.shape["seq"], mesh.shape["fsdp"]
    tok = P(("grp", "fsdp"), "seq", None)
    w = P("fsdp", None)
    in_specs = (tok, P(("grp", "fsdp"), None), w, w, w, w, P(), P(), P(), P(), P(), tok)
    out_specs = (tok, tok, w, w, w, w) + (P("fsdp"),) * 5

    def run(*args):
        return body(S, FS, *args)

    return jax.shard_map(run, mesh=mesh, in_specs=in_specs, out_specs=out_specs, check_vma=False)
```

```python
import jax
import jax.numpy as jnp
from jax import lax
from jax.experimental import pallas as pl
from jax.experimental.pallas import tpu as pltpu
from jax.sharding import PartitionSpec as P

D = 1280
HEADS = 20
HEAD = 64

eps_norm = 1e-06
neg_big = -1e30
BF = jnp.bfloat16
F32 = jnp.float32
MESH = pl.DeviceIdType.MESH
ANY = pl.BlockSpec(memory_space=pl.ANY)
VM = pl.BlockSpec(memory_space=pltpu.VMEM)


def inv_rms(value):
    return lax.rsqrt(jnp.mean(value * value, axis=-1, keepdims=True) + eps_norm)


def back(unit, inv, grad):
    return (grad - unit * jnp.mean(grad * unit, axis=-1, keepdims=True)) * inv


def mm(a, b):
    return jnp.dot(a, b, preferred_element_type=F32)


def mm_nt(a, b):
    return lax.dot_general(a, b, (((1,), (1,)), ((), ())), preferred_element_type=F32)


def mm_tn(a, b):
    return lax.dot_general(a, b, (((0,), (0,)), ((), ())), preferred_element_type=F32)


def rcopy(src, dst, ss, rs, dev):
    return pltpu.make_async_remote_copy(src, dst, ss, rs, device_id=dev, device_id_type=MESH)


def greet(peers):
    bar = pltpu.get_barrier_semaphore()
    for p in peers:
        pl.semaphore_signal(bar, inc=1, device_id=p, device_id_type=MESH)
    pl.semaphore_wait(bar, len(peers))


def ds(start, size, mult):
    return pl.ds(pl.multiple_of(start, mult), size)


def visible(seg_col, seg_row, q0, k0, nq, nk):
    qi = q0 + lax.broadcasted_iota(jnp.int32, (nq, nk), 0)
    ki = k0 + lax.broadcasted_iota(jnp.int32, (nq, nk), 1)
    return (ki <= qi) & ((seg_row == 0) | (seg_row == seg_col))


def add_into(dst, src, chunk):
    def one(i, carry):
        at = ds(i * chunk, chunk, 16)
        dst[at] = (dst[at].astype(F32) + src[at].astype(F32)).astype(dst.dtype)
        return carry

    lax.fori_loop(0, src.shape[0] // chunk, one, 0)


def attn_bias(S, tok, half, bias, segc, segr):
    for qb in range(S):
        q0 = qb * tok
        k0 = q0 if q0 < half else half
        nk = q0 + tok - k0
        ok = visible(segc[q0 : q0 + tok], segr[:, k0 : k0 + nk], q0, k0, tok, nk)
        bias[qb, :, :nk] = jnp.where(ok, 0.0, neg_big).astype(BF)


def first_kernel(S, FS, hp, x_ref, segc, segr, wqkv, wout, gain, alpha, wup,
                 hall_o, wq_o, wo_o, wu_o, raw_o, qkv_o, res_o, mine_o, attn_o, mid_o,
                 hall, wq, wo, raw, qkv, res, bias, oh, mixs, mine, recv,
                 s_up, r_up, s_dn, r_dn, s_wq, r_wq, s_wo, r_wo, s_wu, r_wu, f_wq, f_wo, f_wu,
                 g_wq, g_wo, g_wu, s_mx, r_mx, out_sem):
    g, z, f = lax.axis_index("grp"), lax.axis_index("seq"), lax.axis_index("fsdp")
    tok = x_ref.shape[0]
    rows = wqkv.shape[0]
    hr = rows // 2
    hw = hp * HEAD
    ff = wup.shape[1] // 2
    fl = ff // FS
    total = S * tok
    half = total // 2
    fpeers = [lax.rem(f + i, FS) for i in range(1, FS)]
    zpeers = [lax.rem(z + i, S) for i in range(1, S)]
    greet([(g, z, p) for p in fpeers] + [(g, p, f) for p in zpeers] + [(1 - g, z, f)])

    x = x_ref[...].astype(F32)
    hall[z] = (x * inv_rms(x)).astype(BF)

    def up(t, b):
        return rcopy(hall.at[b], hall.at[b], s_up.at[t], r_up.at[t], (g, lax.rem(z + 1, S), f))

    def down(t, b):
        return rcopy(hall.at[b], hall.at[b], s_dn.at[t], r_dn.at[t], (g, lax.rem(z + S - 1, S), f))

    @pl.when(z + 1 < S)
    def _():
        up(0, z).start()

    @pl.when(z > 0)
    def _():
        down(0, z).start()

    for k in range(S):
        lo, hi = k * hw, min((k + 1) * hw, D)

        @pl.when(z == k)
        def _():
            parts = []
            for c in range(3):
                if hi > lo:
                    parts.append(wqkv[:, c * D + lo : c * D + hi])
                if hi - lo < hw:
                    parts.append(jnp.zeros((rows, hw - max(hi - lo, 0)), BF))
            wq[ds(f * rows, rows, 16)] = jnp.concatenate(parts, axis=1)

    def wq_half(src, gg):
        return wq.at[ds(src * rows + gg * hr, hr, 16)]

    def wo_half(src, gg):
        return wo.at[ds(src * rows + gg * hr, hr, 16)]

    c_wq = [rcopy(wq_half(f, g), wq_half(f, g), s_wq.at[i], r_wq.at[i], (g, z, p)) for i, p in enumerate(fpeers)]
    for c in c_wq:
        c.start()
    attn_bias(S, tok, half, bias, segc, segr)
    wo[ds(f * rows, rows, 16)] = wout[...]
    qkv[2, :, :, HEAD:] = jnp.where(lax.broadcasted_iota(jnp.int32, (hp, total, HEAD), 2) == 0, 1.0, 0.0).astype(BF)

    bpeers = [lax.rem(f + FS - i, FS) for i in range(1, FS)]
    partner = (1 - g, z, f)
    fw_wq = [rcopy(wq_half(p, g), wq_half(p, g), f_wq.at[i], g_wq.at[i], partner) for i, p in enumerate(bpeers)]
    for i in range(FS - 1):
        c_wq[i].wait_recv()
        fw_wq[i].start()
    c_wo = [rcopy(wo_half(f, g), wo_half(f, g), s_wo.at[i], r_wo.at[i], (g, z, p)) for i, p in enumerate(fpeers)]
    for c in c_wo:
        c.start()

    def wu_cp(i, p):
        return rcopy(wup.at[:, ds(g * ff + p * fl, fl, 128)], wu_o.at[g, f], s_wu.at[i], r_wu.at[i], (g, z, p))

    c_wu = [wu_cp(i, p) for i, p in enumerate(fpeers)]
    for c in c_wu:
        c.start()
    for i in range(FS - 1):
        fw_wq[i].wait_recv()

    def step(i, carry):
        t = lax.div(i - 1, 2)
        is_up = lax.rem(i, 2) == 1
        b = jnp.where(i == 0, z, jnp.where(is_up, z - 1 - t, z + 1 + t))

        @pl.when((b >= 0) & (b < S))
        def _():
            @pl.when((i > 0) & is_up)
            def _():
                up(t, b).wait_recv()

                @pl.when(z + 1 < S)
                def _():
                    up(t + 1, b).start()

            @pl.when((i > 0) & jnp.logical_not(is_up))
            def _():
                down(t, b).wait_recv()

                @pl.when(z > 0)
                def _():
                    down(t + 1, b).start()

            acc = mm(hall[b], wq[...])
            at = ds(b * tok, tok, 16)
            for j in range(hp):
                for c in range(2):
                    v = acc[:, c * hw + j * HEAD : c * hw + (j + 1) * HEAD]
                    raw[c, j, at, :] = v
                    u = v * inv_rms(v) * gain[j : j + 1]
                    qkv[c, j, at, :HEAD] = u.astype(BF)
                qkv[2, j, at, :HEAD] = acc[:, 2 * hw + j * HEAD : 2 * hw + (j + 1) * HEAD].astype(BF)

        return carry

    lax.fori_loop(0, 2 * S - 1, step, 0)
    outs = [
        pltpu.make_async_copy(hall, hall_o, out_sem.at[0]),
        pltpu.make_async_copy(wq, wq_o, out_sem.at[1]),
        pltpu.make_async_copy(raw, raw_o, out_sem.at[2]),
        pltpu.make_async_copy(qkv, qkv_o, out_sem.at[3]),
    ]
    for c in outs:
        c.start()

    def mx(qb):
        return rcopy(mixs.at[qb], recv.at[z], s_mx.at[qb], r_mx.at[z], (g, qb, f))

    for qb in reversed(range(S)):
        q0 = qb * tok
        n = q0 + tok
        k0 = q0 if q0 < half else half

        def head(j, carry):
            q = qkv[0, j, q0:n, :HEAD] * jnp.asarray(HEAD**-0.5, BF)
            s = mm_nt(q, qkv[1, j, :n, :HEAD])
            tail = s[:, k0:] + bias[qb, :, : n - k0].astype(F32)
            e = jnp.exp(jnp.concatenate([s[:, :k0], tail], axis=1) if k0 else tail)
            o = mm(e.astype(BF), qkv[2, j, :n])
            rinv = 1.0 / o[:, HEAD : HEAD + 1]
            o = o[:, :HEAD] * rinv
            res[j, q0:n, :HEAD] = o
            res[j, q0:n, HEAD:] = jnp.broadcast_to(rinv, (tok, HEAD))
            oh[j] = o.astype(BF)
            return carry

        lax.fori_loop(0, hp, head, 0)
        block = jnp.concatenate([oh[j] for j in range(hp)], axis=1)
        mixs[qb] = block

        @pl.when(z != qb)
        def _():
            mx(qb).start()

        @pl.when(z == qb)
        def _():
            recv[qb] = block

        if qb == S - 1:
            fw_wo = [rcopy(wo_half(p, g), wo_half(p, g), f_wo.at[i], g_wo.at[i], partner) for i, p in enumerate(bpeers)]
            for i in range(FS - 1):
                c_wo[i].wait_recv()
                fw_wo[i].start()

    fw_wu = [rcopy(wu_o.at[g, p], wu_o.at[g, p], f_wu.at[i], g_wu.at[i], partner) for i, p in enumerate(bpeers)]
    for i in range(FS - 1):
        c_wu[i].wait_recv()
        fw_wu[i].start()
    for i in range(FS - 1):
        fw_wo[i].wait_recv()
    outs2 = [pltpu.make_async_copy(wo, wo_o, out_sem.at[4]), pltpu.make_async_copy(res, res_o, out_sem.at[5])]
    for c in outs2:
        c.start()
    for k in range(S):
        @pl.when(z != k)
        def _():
            rcopy(mixs.at[0], recv.at[k], s_mx.at[0], r_mx.at[k], (g, k, f)).wait_recv()

    mine[...] = jnp.concatenate([recv[k] for k in range(S)], axis=1)[:, :D]
    attn = mm(mine[...], wo[...])
    attn_o[...] = attn
    mine_o[...] = mine[...]
    x = x_ref[...].astype(F32)
    h = x * inv_rms(x)
    n_ = h + alpha[...] * (attn * inv_rms(attn) - h)
    mid_o[...] = n_ * inv_rms(n_)

    for t in range(S - 1):
        @pl.when((z + 1 < S) & (z - t >= 0))
        def _():
            up(t, z).wait_send()

        @pl.when((z > 0) & (z + t < S))
        def _():
            down(t, z).wait_send()

    for i in range(FS - 1):
        c_wq[i].wait_send()
        c_wo[i].wait_send()
        c_wu[i].wait_send()
        fw_wq[i].wait_send()
        fw_wo[i].wait_send()
        fw_wu[i].wait()
    for k in range(S):
        @pl.when(z != k)
        def _():
            mx(k).wait_send()
    for c in outs + outs2:
        c.wait()


def first(S, FS, hp, x, seg, wqkv, wout, gain, alpha, wup):
    tok, total = x.shape[0], seg.shape[0]
    rows = wqkv.shape[0]
    hw = hp * HEAD
    fl = wup.shape[1] // 2 // FS
    sds = jax.ShapeDtypeStruct
    outs = [
        sds((S, tok, D), BF), sds((D, 3 * hw), BF), sds((D, D), BF), sds((2, FS, rows, fl), BF),
        sds((2, hp, total, HEAD), F32), sds((3, hp, total, 2 * HEAD), BF), sds((hp, total, 2 * HEAD), F32),
        sds((tok, D), BF), sds((tok, D), F32), sds((tok, D), F32),
    ]
    dma = lambda n: pltpu.SemaphoreType.DMA((n,))
    F1 = FS - 1
    return pl.pallas_call(
        lambda *refs: first_kernel(S, FS, hp, *refs),
        out_shape=outs,
        in_specs=[VM] * 7 + [ANY],
        out_specs=[ANY] * 7 + [VM] * 3,
        scratch_shapes=[
            pltpu.VMEM((S, tok, D), BF), pltpu.VMEM((D, 3 * hw), BF), pltpu.VMEM((D, D), BF),
            pltpu.VMEM((2, hp, total, HEAD), F32), pltpu.VMEM((3, hp, total, 2 * HEAD), BF),
            pltpu.VMEM((hp, total, 2 * HEAD), F32), pltpu.VMEM((S, tok, total // 2), BF),
            pltpu.VMEM((hp, tok, HEAD), BF), pltpu.VMEM((S, tok, hw), BF), pltpu.VMEM((tok, D), BF),
            pltpu.VMEM((S, tok, hw), BF),
            dma(S), dma(S), dma(S), dma(S), dma(F1), dma(F1), dma(F1), dma(F1), dma(F1), dma(F1),
            dma(F1), dma(F1), dma(F1), dma(F1), dma(F1), dma(F1), dma(S), dma(S), dma(6),
        ],
        compiler_params=pltpu.CompilerParams(collective_id=1, has_side_effects=True, vmem_limit_bytes=60 * 2**20),
        name="first",
    )(x, seg.reshape(total, 1), seg.reshape(1, total), wqkv, wout, gain, alpha.reshape(1, D), wup)


def second_kernel(S, FS, NC, mid, cot, wd, su, sg, alpha, wu_i, wup,
                  out_o, gmid_o, du_o, dd_o, dal_o, dsu_o, dsg_o,
                  wu, mida, up, gate, hid, ps, pr, gma, gu, dup, ddn, lu, ld,
                  s_a, r_a, s_b, r_b, s_c, r_c, s_d, r_d, w_sem, s_x, r_x, out_sem):
    g, z, f = lax.axis_index("grp"), lax.axis_index("seq"), lax.axis_index("fsdp")
    tok = mid.shape[0]
    ct = tok // NC
    fl = wd.shape[0]
    ff = wup.shape[1] // 2
    rows = wup.shape[0]
    hl = fl // 2
    nt = 256 if fl % 256 == 0 else 128
    M = FS * ct
    peers = [lax.rem(f + i, FS) for i in range(1, FS)]
    bpeers = [lax.rem(f + FS - i, FS) for i in range(1, FS)]
    partner = (1 - g, z, f)
    greet([(g, z, p) for p in peers] + [partner])

    def gather_copy(buf, ss, rs, c, i):
        return rcopy(buf.at[c, f], buf.at[c, f], ss.at[c, i], rs.at[c, i], (g, z, peers[i]))

    def send_partial(ss, rs, c, i):
        return rcopy(ps.at[c, peers[i]], pr.at[c, i], ss.at[c, i], rs.at[c, i], (g, z, peers[i]))

    R = range(FS - 1)
    for c in range(NC):
        mida[c, f] = mid[c * ct : (c + 1) * ct].astype(BF)
        for i in R:
            gather_copy(mida, s_a, r_a, c, i).start()
    loads = []
    for k in range(2):
        loads.append(pltpu.make_async_copy(wup.at[:, ds(k * ff + f * fl, fl, 128)], wu.at[k, ds(f * rows, rows, 16)], w_sem.at[k, 0]))
        for i in R:
            loads.append(pltpu.make_async_copy(wu_i.at[k, peers[i]], wu.at[k, ds(peers[i] * rows, rows, 16)], w_sem.at[k, i + 1]))
    for c in loads:
        c.start()
    dsu_o[...] = jnp.zeros_like(dsu_o)
    dsg_o[...] = jnp.zeros_like(dsg_o)
    dal_o[...] = jnp.zeros_like(dal_o)
    for c in loads:
        c.wait()

    for c in range(NC):
        for i in R:
            gather_copy(mida, s_a, r_a, c, i).wait_recv()

        def fwd(t, carry):
            cols = ds(t * nt, nt, 128)
            a_in = mida[c].reshape(M, D)
            u = mm(a_in, wu[0, :, cols])
            gt = mm(a_in, wu[1, :, cols])
            up[c, :, cols] = u
            gate[c, :, cols] = gt
            a = gt * sg[:, cols]
            hid[c, :, cols] = (u * su[:, cols] * (a * jax.nn.sigmoid(a))).astype(BF)
            return carry

        lax.fori_loop(0, fl // nt, fwd, 0)

        def proj(t, carry):
            cols = ds(t * 256, 256, 128)
            ps[c, :, :, cols] = mm(hid[c], wd[:, cols]).astype(BF).reshape(FS, ct, 256)
            return carry

        lax.fori_loop(0, D // 256, proj, 0)
        for i in R:
            send_partial(s_b, r_b, c, i).start()

    for c in range(NC):
        at = slice(c * ct, (c + 1) * ct)
        for i in R:
            send_partial(s_b, r_b, c, i).wait_recv()
        mlp = ps[c, f].astype(F32)
        for i in R:
            mlp = mlp + pr[c, i].astype(F32)
        al = alpha[...]
        md = mid[at]
        inv_m = inv_rms(mlp)
        um = mlp * inv_m
        dif = um - md
        m = md + al * dif
        inv_o = inv_rms(m)
        o = m * inv_o
        out_o[at] = o.astype(BF)
        g_m = back(o, inv_o, cot[at].astype(F32))
        dal_o[...] += jnp.sum(g_m * dif, axis=0, keepdims=True)
        gmid_o[at] = (1 - al) * g_m
        gma[c, f] = back(um, inv_m, al * g_m).astype(BF)
        for i in R:
            gather_copy(gma, s_c, r_c, c, i).start()

    for c in range(NC):
        for i in R:
            gather_copy(gma, s_c, r_c, c, i).wait_recv()

        def bwd(t, carry):
            cols = ds(t * nt, nt, 128)
            gh = mm_nt(gma[c].reshape(M, D), wd[cols, :])
            u = up[c, :, cols]
            gt = gate[c, :, cols]
            sgc = sg[:, cols]
            suc = su[:, cols]
            a = gt * sgc
            sig = jax.nn.sigmoid(a)
            gs = gh * (a * sig)
            gu[0, c, :, cols] = (gs * suc).astype(BF)
            dsu_o[:, cols] += jnp.sum(u * gs, axis=0, keepdims=True)
            g_a = gh * u * suc * (sig * (1 + a * (1 - sig)))
            gu[1, c, :, cols] = (g_a * sgc).astype(BF)
            dsg_o[:, cols] += jnp.sum(gt * g_a, axis=0, keepdims=True)
            return carry

        lax.fori_loop(0, fl // nt, bwd, 0)
        for i in R:
            send_partial(s_b, r_b, c, i).wait_send()

        def bproj(t, carry):
            cols = ds(t * 256, 256, 128)
            v = mm_nt(gu[0, c], wu[0, cols, :]) + mm_nt(gu[1, c], wu[1, cols, :])
            ps[c, :, :, cols] = v.astype(BF).reshape(FS, ct, 256)
            return carry

        lax.fori_loop(0, D // 256, bproj, 0)
        for i in R:
            send_partial(s_d, r_d, c, i).start()

    def dwd(t, carry):
        cols = ds(t * nt, nt, 128)
        ddn[cols, :] = mm_tn(hid[:, :, cols].reshape(NC * M, nt), gma[...].reshape(NC * M, D)).astype(BF)
        return carry

    lax.fori_loop(0, fl // nt, dwd, 0)
    x_d = rcopy(ddn.at[ds((1 - g) * hl, hl, 16)], ld, s_x.at[0], r_x.at[0], partner)
    x_d.start()

    def dwu(k):
        def one(t, carry):
            cols = ds(t * 256, 256, 128)
            dup[k, cols, :] = mm_tn(mida[:, :, :, cols].reshape(NC * M, 256), gu[k].reshape(NC * M, fl)).astype(BF)
            return carry

        lax.fori_loop(0, D // 256, one, 0)

    dwu(1 - g)
    x_u = rcopy(dup.at[1 - g], lu, s_x.at[1], r_x.at[1], partner)
    x_u.start()
    dwu(g)
    mine = ds(g * hl, hl, 16)
    x_d.wait_recv()
    add_into(ddn.at[mine], ld, 64)
    o_d = pltpu.make_async_copy(ddn.at[mine], dd_o, out_sem.at[0])
    o_d.start()
    x_u.wait_recv()
    add_into(dup.at[g], lu, 64)
    o_u = pltpu.make_async_copy(dup.at[g], du_o, out_sem.at[1])
    o_u.start()

    for c in range(NC):
        at = slice(c * ct, (c + 1) * ct)
        for i in R:
            send_partial(s_d, r_d, c, i).wait_recv()
        acc = gmid_o[at] + ps[c, f].astype(F32)
        for i in R:
            acc = acc + pr[c, i].astype(F32)
        gmid_o[at] = acc
    for c in range(NC):
        for i in R:
            gather_copy(mida, s_a, r_a, c, i).wait_send()
            gather_copy(gma, s_c, r_c, c, i).wait_send()
            send_partial(s_d, r_d, c, i).wait_send()
    x_d.wait_send()
    x_u.wait_send()
    o_d.wait()
    o_u.wait()


def second(S, FS, mid, cot, wd, su, sg, alpha, wu, wup):
    NC = 2
    tok = mid.shape[0]
    ct = tok // NC
    fl = wd.shape[0]
    M = FS * ct
    sds = jax.ShapeDtypeStruct
    outs = [sds((tok, D), BF), sds((tok, D), F32), sds((D, fl), BF), sds((fl // 2, D), BF),
            sds((1, D), F32), sds((1, fl), F32), sds((1, fl), F32)]
    dma = pltpu.SemaphoreType.DMA
    F1 = FS - 1
    return pl.pallas_call(
        lambda *refs: second_kernel(S, FS, NC, *refs),
        out_shape=outs,
        in_specs=[VM] * 6 + [ANY] * 2,
        out_specs=[VM, VM, ANY, ANY, VM, VM, VM],
        scratch_shapes=[
            pltpu.VMEM((2, D, fl), BF), pltpu.VMEM((NC, FS, ct, D), BF), pltpu.VMEM((NC, M, fl), F32),
            pltpu.VMEM((NC, M, fl), F32), pltpu.VMEM((NC, M, fl), BF), pltpu.VMEM((NC, FS, ct, D), BF),
            pltpu.VMEM((NC, F1, ct, D), BF), pltpu.VMEM((NC, FS, ct, D), BF), pltpu.VMEM((2, NC, M, fl), BF),
            pltpu.VMEM((2, D, fl), BF), pltpu.VMEM((fl, D), BF), pltpu.VMEM((D, fl), BF), pltpu.VMEM((fl // 2, D), BF),
        ] + [dma((NC, F1))] * 8 + [dma((2, FS)), dma((2,)), dma((2,)), dma((2,))],
        compiler_params=pltpu.CompilerParams(collective_id=2, has_side_effects=True, vmem_limit_bytes=63 * 2**20),
        name="second",
    )(mid, cot, wd, su, sg, alpha.reshape(1, D), wu, wup)


def third_kernel(S, FS, hp, gmid, x_ref, attn, alpha, mine, segc, segr, gain, wo, wq_i, qkv_i, raw_i, res_i, hall_i,
                 gx_o, dout_o, dqkv_o, dal_o, dsq_o,
                 wq, qkv, raw, res, hall, gh1, ga, gsend, gxr, bias, hx, gqh, dkv, gq, ps, pr, dout, dqk, lo, lq,
                 ld_sem, h_sem, s_gx, r_gx, s_p, r_p, s_x, r_x, out_sem):
    g, z, f = lax.axis_index("grp"), lax.axis_index("seq"), lax.axis_index("fsdp")
    tok = x_ref.shape[0]
    hw = hp * HEAD
    wide = S * hw
    total = S * tok
    half = total // 2
    w2 = 3 * hw // 2
    dh = D // 2
    partner = (1 - g, z, f)
    greet([(g, lax.rem(z + i, S), f) for i in range(1, S)] + [partner])
    loads = [pltpu.make_async_copy(a, b, ld_sem.at[i]) for i, (a, b) in enumerate(
        [(qkv_i, qkv), (raw_i, raw), (res_i, res), (wq_i, wq)])]
    for c in loads:
        c.start()

    def h_tile(t):
        return pltpu.make_async_copy(hall_i.at[:, :, pl.ds(t * 256, 256)], hall.at[t % 2], h_sem.at[t % 2])

    h_tile(0).start()
    h_tile(1).start()
    dal_o[...] = jnp.zeros_like(dal_o)
    dsq_o[...] = jnp.zeros_like(dsq_o)
    cr = tok // 4

    def pre(i, carry):
        at = ds(i * cr, cr, 16)
        x = x_ref[at].astype(F32)
        h = x * inv_rms(x)
        av = attn[at]
        inv_a = inv_rms(av)
        ua = av * inv_a
        al = alpha[...]
        dif = ua - h
        n_ = h + al * dif
        inv_n = inv_rms(n_)
        g_n = back(n_ * inv_n, inv_n, gmid[at])
        dal_o[...] += jnp.sum(g_n * dif, axis=0, keepdims=True)
        gh1[at] = (1 - al) * g_n
        ga[at] = back(ua, inv_a, al * g_n).astype(BF)
        return carry

    lax.fori_loop(0, 4, pre, 0)
    gmix = mm_nt(ga[...], wo[...]).astype(BF)
    if wide > D:
        gmix = jnp.concatenate([gmix, jnp.zeros((tok, wide - D), BF)], axis=1)
    for k in range(S):
        gsend[k] = gmix[:, k * hw : (k + 1) * hw]

    def gx(k):
        return rcopy(gsend.at[k], gxr.at[z], s_gx.at[k], r_gx.at[z], (g, k, f))

    for k in range(S):
        @pl.when(z != k)
        def _():
            gx(k).start()

        @pl.when(z == k)
        def _():
            gxr[k] = gsend[k]

    def dwo(t, carry):
        cols = ds(t * 256, 256, 128)
        v = mm_tn(mine[:, cols], ga[...]).astype(BF)
        dout[0, cols, :] = v[:, :dh]
        dout[1, cols, :] = v[:, dh:]
        return carry

    lax.fori_loop(0, D // 256, dwo, 0)
    x_o = rcopy(dout.at[1 - g], lo, s_x.at[0], r_x.at[0], partner)
    x_o.start()
    attn_bias(S, tok, half, bias, segc, segr)
    for c in loads:
        c.wait()

    def part(k):
        return rcopy(ps.at[k], pr.at[z], s_p.at[k], r_p.at[z], (g, k, f))

    for qb in reversed(range(S)):
        q0 = qb * tok
        n = q0 + tok
        k0 = q0 if q0 < half else half

        @pl.when(z != qb)
        def _():
            rcopy(gsend.at[0], gxr.at[qb], s_gx.at[0], r_gx.at[qb], (g, qb, f)).wait_recv()

        for j in range(hp):
            hx[j] = gxr[qb, :, j * HEAD : (j + 1) * HEAD]

        def head(j, carry):
            q = qkv[0, j, q0:n, :HEAD] * jnp.asarray(HEAD**-0.5, BF)
            keys = qkv[1, j, :n, :HEAD]
            gv = hx[j]
            rinv = res[j, q0:n, HEAD : HEAD + 1]
            delta = jnp.sum(gv.astype(F32) * res[j, q0:n, :HEAD], axis=-1, keepdims=True)
            s = mm_nt(q, keys)
            tail = s[:, k0:] + bias[qb, :, : n - k0].astype(F32)
            p = jnp.exp(jnp.concatenate([s[:, :k0], tail], axis=1) if k0 else tail) * rinv
            dp = mm_nt(gv, qkv[2, j, :n, :HEAD])
            dsb = (p * (dp - delta)).astype(BF)
            dq = mm(dsb, keys) * HEAD**-0.5
            dk = mm_tn(dsb, q)
            dv = mm_tn(p.astype(BF), gv)
            if qb < S - 1:
                dk = dk + dkv[j, :n, :HEAD]
                dv = dv + dkv[j, :n, HEAD:]
            if qb:
                dkv[j, :q0, :HEAD] = dk[:q0]
                dkv[j, :q0, HEAD:] = dv[:q0]
            gj = gain[pl.ds(j, 1), :]
            for c, d in ((0, dq), (1, dk[q0:])):
                v = raw[c, j, q0:n]
                inv = inv_rms(v)
                u = v * inv
                dsq_o[pl.ds(j, 1), :] += jnp.sum(d * u, axis=0, keepdims=True)
                gqh[c, j] = back(u, inv, d * gj).astype(BF)
            gqh[2, j] = dv[q0:].astype(BF)
            return carry

        lax.fori_loop(0, hp, head, 0)
        gq[qb] = jnp.concatenate([gqh[c, j] for c in range(3) for j in range(hp)], axis=1)
        ps[qb] = mm_nt(gq[qb], wq[...]).astype(BF)

        @pl.when(z != qb)
        def _():
            part(qb).start()

    for t in range(D // 256):
        h_tile(t).wait()
        v = mm_tn(hall[t % 2].reshape(total, 256), gq[...].reshape(total, 3 * hw)).astype(BF)
        dqk[0, t * 256 : (t + 1) * 256, :] = v[:, :w2]
        dqk[1, t * 256 : (t + 1) * 256, :] = v[:, w2:]
        if t + 2 < D // 256:
            h_tile(t + 2).start()
    x_q = rcopy(dqk.at[1 - g], lq, s_x.at[1], r_x.at[1], partner)
    x_q.start()
    x_o.wait_recv()
    add_into(dout.at[g], lo, 128)
    o_o = pltpu.make_async_copy(dout.at[g], dout_o, out_sem.at[0])
    o_o.start()
    x_q.wait_recv()
    add_into(dqk.at[g], lq, 128)
    o_q = pltpu.make_async_copy(dqk.at[g], dqkv_o, out_sem.at[1])
    o_q.start()

    add_into(gh1, ps.at[z], 64)
    for k in range(S):
        @pl.when(z != k)
        def _():
            rcopy(ps.at[0], pr.at[k], s_p.at[0], r_p.at[k], (g, k, f)).wait_recv()
            add_into(gh1, pr.at[k], 64)

    def post(i, carry):
        at = ds(i * cr, cr, 16)
        x = x_ref[at].astype(F32)
        inv = inv_rms(x)
        gx_o[at] = back(x * inv, inv, gh1[at])
        return carry

    lax.fori_loop(0, 4, post, 0)
    for k in range(S):
        @pl.when(z != k)
        def _():
            gx(k).wait_send()
            part(k).wait_send()
    x_o.wait_send()
    x_q.wait_send()
    o_o.wait()
    o_q.wait()


def third(S, FS, hp, gmid, x, attn, alpha, mine, seg, gain, wo, wq, qkv, raw, res, hall):
    tok, total = x.shape[0], seg.shape[0]
    hw = hp * HEAD
    sds = jax.ShapeDtypeStruct
    outs = [sds((tok, D), F32), sds((D, D // 2), BF), sds((D, 3 * hw // 2), BF), sds((1, D), F32), sds((hp, HEAD), F32)]
    dma = lambda n: pltpu.SemaphoreType.DMA((n,))
    return pl.pallas_call(
        lambda *refs: third_kernel(S, FS, hp, *refs),
        out_shape=outs,
        in_specs=[VM] * 9 + [ANY] * 5,
        out_specs=[VM, ANY, ANY, VM, VM],
        scratch_shapes=[
            pltpu.VMEM((D, 3 * hw), BF), pltpu.VMEM((3, hp, total, 2 * HEAD), BF), pltpu.VMEM((2, hp, total, HEAD), F32),
            pltpu.VMEM((hp, total, 2 * HEAD), F32), pltpu.VMEM((2, S, tok, 256), BF), pltpu.VMEM((tok, D), F32),
            pltpu.VMEM((tok, D), BF), pltpu.VMEM((S, tok, hw), BF), pltpu.VMEM((S, tok, hw), BF),
            pltpu.VMEM((S, tok, total // 2), BF), pltpu.VMEM((hp, tok, HEAD), BF), pltpu.VMEM((3, hp, tok, HEAD), BF),
            pltpu.VMEM((hp, total, 2 * HEAD), F32), pltpu.VMEM((S, tok, 3 * hw), BF), pltpu.VMEM((S, tok, D), BF),
            pltpu.VMEM((S, tok, D), BF), pltpu.VMEM((2, D, D // 2), BF), pltpu.VMEM((2, D, 3 * hw // 2), BF),
            pltpu.VMEM((D, D // 2), BF), pltpu.VMEM((D, 3 * hw // 2), BF),
            dma(4), dma(2), dma(S), dma(S), dma(S), dma(S), dma(2), dma(2), dma(2),
        ],
        compiler_params=pltpu.CompilerParams(collective_id=3, has_side_effects=True, vmem_limit_bytes=63 * 2**20),
        name="third",
    )(gmid, x, attn, alpha.reshape(1, D), mine, seg.reshape(total, 1), seg.reshape(1, total), gain, wo, wq, qkv, raw, res, hall)


def fourth_kernel(S, FS, hp, vec, du, dd, dout, dqkv,
                  up_o, dn_o, out_o, qkv_o, vec_o, sqk_o,
                  own_u, raw_u, oth_u, own_d, raw_d, oth_d, own_o, raw_o, oth_o, so, xo, sq, xq, agq, va, vb, vf, vz,
                  ld_sem, s_u, r_u, s_xo, r_xo, s_xq, r_xq, s_in, r_raw, r_oth, s_ret,
                  s_aq, r_aq, s_fq, r_fq, s_v, r_v, o_sem, s_o, r_o):
    g, z, f = lax.axis_index("grp"), lax.axis_index("seq"), lax.axis_index("fsdp")
    rows = own_u.shape[1]
    fl = own_u.shape[2]
    hl = own_d.shape[0]
    ff = fl * FS
    hw = hp * HEAD
    w2 = 3 * hw // 2
    dh = D // 2
    peers = [lax.rem(f + i, FS) for i in range(1, FS)]
    bpeers = [lax.rem(f + FS - i, FS) for i in range(1, FS)]
    zpeers = [lax.rem(z + i, S) for i in range(1, S)]
    zb = [lax.rem(z + S - i, S) for i in range(1, S)]
    partner = (1 - g, z, f)
    R = range(FS - 1)
    greet([(g, z, p) for p in peers] + [(g, p, f) for p in zpeers] + [partner])

    def blk(p):
        return ds(p * rows, rows, 16)

    l_d = pltpu.make_async_copy(dd, own_d, ld_sem.at[0])
    l_o = pltpu.make_async_copy(dout.at[blk(f)], so, ld_sem.at[1])
    l_q = pltpu.make_async_copy(dqkv.at[blk(f)], sq, ld_sem.at[2])
    l_u = pltpu.make_async_copy(du.at[blk(f)], own_u.at[f], ld_sem.at[3])
    for c in (l_d, l_o, l_q, l_u):
        c.start()
    c_o = [rcopy(dout.at[blk(p)], xo.at[i], s_xo.at[i], r_xo.at[i], (g, z, p)) for i, p in enumerate(peers)]
    c_q = [rcopy(dqkv.at[blk(p)], xq.at[i], s_xq.at[i], r_xq.at[i], (g, z, p)) for i, p in enumerate(peers)]
    c_u = [rcopy(du.at[blk(p)], own_u.at[f], s_u.at[i], r_u.at[i], (g, z, p)) for i, p in enumerate(peers)]
    va[...] = vec[...]
    v_c = rcopy(va, vb, s_v.at[0], r_v.at[0], partner)
    v_c.start()
    for c in c_q + c_o + c_u:
        c.start()

    lower = z < S // 2
    inner = jnp.where(lower, z + 1, z - 1)
    outer = jnp.where(lower, z - 1, z + 1)
    mid = (z == S // 2 - 1) | (z == S // 2)
    has_outer = (z > 0) & (z < S - 1)
    outer = jnp.where(has_outer, outer, inner)

    pieces = []
    nd = 4
    for i in range(nd):
        a = pl.ds(i * (hl // nd), hl // nd)
        pieces.append((own_d.at[a], raw_d.at[a], oth_d.at[a],
                       lambda o, i=i: o[1].at[ds(g * hl + i * (hl // nd), hl // nd, 16)]))
    order = [(f, -1)] + [(p, i) for i, p in enumerate(bpeers)]
    for p, i in order:
        if i == 0:
            pieces.append((own_o, raw_o, oth_o, lambda o: o[2].at[:, ds(g * dh, dh, 128)]))
        for k in range(2):
            a = pl.ds(k * (rows // 2), rows // 2)
            pieces.append((own_u.at[p, a], raw_u.at[p, a], oth_u.at[p, a],
                           lambda o, p=p, a=a: o[0].at[a, ds(g * ff + p * fl, fl, 128)]))

    def toward(i, to_mid):
        own, raw, oth, _ = pieces[i]
        if to_mid:
            return rcopy(own, oth, s_in.at[i], r_oth.at[i], (g, inner, f))
        return rcopy(own, raw, s_in.at[i], r_raw.at[i], (g, inner, f))

    def returned(i, from_mid):
        own, raw, oth, _ = pieces[i]
        return rcopy(raw if from_mid else oth, oth, s_ret.at[i], r_oth.at[i], (g, outer, f))

    def go_in(i):
        own, raw, oth, _ = pieces[i]

        @pl.when(has_outer)
        def _():
            rcopy(own, raw, s_in.at[i], r_raw.at[i], (g, outer, f)).wait_recv()
            own[...] = (own[...].astype(F32) + raw[...].astype(F32)).astype(BF)

        @pl.when(mid)
        def _():
            toward(i, True).start()

        @pl.when(jnp.logical_not(mid))
        def _():
            toward(i, False).start()

    outs = (up_o, dn_o, out_o)

    def local_out(i, src):
        return pltpu.make_async_copy(src, pieces[i][3](outs), o_sem.at[i])

    def remote_out(i, src):
        dst = pieces[i][3](outs)
        return rcopy(src, dst, s_o.at[i], r_o.at[i], partner)

    def mid_out(i):
        own, raw, oth, _ = pieces[i]
        rcopy(own, oth, s_in.at[i], r_oth.at[i], (g, inner, f)).wait_recv()
        raw[...] = (own[...].astype(F32) + oth[...].astype(F32)).astype(BF)

        @pl.when(has_outer)
        def _():
            returned(i, True).start()

        local_out(i, raw).start()
        remote_out(i, raw).start()

    def other_out(i):
        own, raw, oth, _ = pieces[i]
        rcopy(own, oth, s_in.at[i], r_oth.at[i], (g, inner, f)).wait_recv()

        @pl.when(has_outer)
        def _():
            returned(i, False).start()

        local_out(i, oth).start()
        remote_out(i, oth).start()

    total = len(pieces)
    lag = 5

    def step(i):
        if i < total:
            go_in(i)
        if 1 <= i <= total:
            @pl.when(mid)
            def _():
                mid_out(i - 1)
        if i >= lag:
            @pl.when(jnp.logical_not(mid))
            def _():
                other_out(i - lag)

    def add_all(own, recv):
        acc = own[...].astype(F32)
        for i in R:
            acc = acc + recv[i].astype(F32)
        return acc.astype(BF)

    def aq(i):
        return rcopy(agq.at[z, g], agq.at[z, g], s_aq.at[i], r_aq.at[i], (g, zpeers[i], f))

    def fq(i):
        src = z if i < 0 else zb[i]
        return rcopy(agq.at[src, g], agq.at[src, g], s_fq.at[i + 1], r_fq.at[i + 1], partner)

    l_d.wait()
    for i in range(nd):
        step(i)
    v_c.wait()
    vf[f] = va[...] + vb[...]
    v_f = [rcopy(vf.at[f], vf.at[f], s_v.at[1 + i], r_v.at[1 + i], (g, z, p)) for i, p in enumerate(peers)]
    for c in v_f:
        c.start()
    l_u.wait()
    step(nd)
    step(nd + 1)
    l_o.wait()
    for c in c_o:
        c.wait()
    own_o[...] = add_all(so, xo)
    step(nd + 2)
    for c in v_f:
        c.wait()
    acc = vf[0]
    for i in range(1, FS):
        acc = acc + vf[i]
    sub = lax.broadcasted_iota(jnp.int32, acc.shape, 0)
    vz[z] = jnp.where(sub < 3, acc, vf[f])
    v_z = [rcopy(vz.at[z], vz.at[z], s_v.at[FS + i], r_v.at[FS + i], (g, p, f)) for i, p in enumerate(zpeers)]
    for c in v_z:
        c.start()
    l_q.wait()
    for c in c_q:
        c.wait()
    agq[z, g] = add_all(sq, xq)
    n = nd + 3
    for i in R:
        c_u[i].wait()
        for k in range(2):
            step(n)
            n += 1
        if i == R[-1]:
            for j in range(S - 1):
                aq(j).start()
            fq(-1).start()
    for k in range(lag):
        step(n + k)
    for j in range(S - 1):
        aq(j).wait_recv()
        fq(j).start()
    for c in v_z:
        c.wait()
    acc = vz[0]
    for i in range(1, S):
        acc = acc + vz[i]
    vec_o[...] = acc
    for i in range(S):
        sqk_o[i] = vz[i]
    for j in range(-1, S - 1):
        fq(j).wait_recv()
    full = [jnp.concatenate([agq[k, 0], agq[k, 1]], axis=1) for k in range(S)]
    cols = []
    for c in range(3):
        row = jnp.concatenate([full[k][:, c * hw : (c + 1) * hw] for k in range(S)], axis=1)
        cols.append(row[:, :D])
    qkv_o[...] = jnp.concatenate(cols, axis=1)
    for j in range(-1, S - 1):
        fq(j).wait_send()
    for j in range(S - 1):
        aq(j).wait_send()
    for i in range(n):
        own, raw, oth, _ = pieces[i]
        toward(i, True).wait_send()

        @pl.when(has_outer)
        def _():
            returned(i, True).wait_send()

        local_out(i, raw).wait()
        remote_out(i, raw).wait()


def fourth(S, FS, hp, vec, du, dd, dout, dqkv):
    fl = du.shape[1]
    rows = D // FS
    hl = dd.shape[0]
    hw = hp * HEAD
    w2 = 3 * hw // 2
    dh = D // 2
    n = 5 + 2 * FS
    sds = jax.ShapeDtypeStruct
    outs = [sds((rows, 2 * FS * fl), BF), sds((2 * hl, D), BF), sds((rows, D), BF), sds((rows, 3 * D), BF),
            sds(vec.shape, F32), sds((S,) + vec.shape, F32)]
    dma = lambda k: pltpu.SemaphoreType.DMA((k,))
    F1 = FS - 1
    u, d, o = pltpu.VMEM((FS, rows, fl), BF), pltpu.VMEM((hl, D), BF), pltpu.VMEM((rows, dh), BF)
    v = pltpu.VMEM(vec.shape, F32)
    return pl.pallas_call(
        lambda *refs: fourth_kernel(S, FS, hp, *refs),
        out_shape=outs,
        in_specs=[VM] + [ANY] * 4,
        out_specs=[ANY, ANY, ANY, VM, VM, VM],
        scratch_shapes=[
            u, u, u, d, d, d, o, o, o, o, pltpu.VMEM((F1, rows, dh), BF),
            pltpu.VMEM((rows, w2), BF), pltpu.VMEM((F1, rows, w2), BF), pltpu.VMEM((S, 2, rows, w2), BF),
            v, v, pltpu.VMEM((FS,) + vec.shape, F32), pltpu.VMEM((S,) + vec.shape, F32),
            dma(4), dma(F1), dma(F1), dma(F1), dma(F1), dma(F1), dma(F1), dma(n), dma(n), dma(n), dma(n),
            dma(S), dma(S), dma(S), dma(S), dma(FS + S), dma(FS + S), dma(n), dma(n), dma(n),
        ],
        compiler_params=pltpu.CompilerParams(collective_id=4, has_side_effects=True, vmem_limit_bytes=60 * 2**20),
        name="fourth",
    )(vec, du, dd, dout, dqkv)


def body(S, FS, inputs, segments, w_qkv, w_out, w_upgate, w_down, s_qk, alpha_attn, alpha_mlp, s_up, s_gate, cotangent):
    z = lax.axis_index("seq")
    f = lax.axis_index("fsdp")
    hp = -(-HEADS // S)
    hw = hp * HEAD
    rows = w_qkv.shape[0]
    ff = s_up.shape[0]
    fl = ff // FS
    x = inputs[0]
    seg = segments[0]
    gains = jnp.pad(s_qk, (0, S * hw - D))
    gain = lax.dynamic_slice_in_dim(gains, z * hw, hw).reshape(hp, HEAD)
    hall, wq, wo, wu, raw, qkv, res, mine, attn, mid = first(S, FS, hp, x, seg, w_qkv, w_out, gain, alpha_attn, w_upgate)
    su = lax.dynamic_slice_in_dim(s_up, f * fl, fl).reshape(1, fl)
    sg = lax.dynamic_slice_in_dim(s_gate, f * fl, fl).reshape(1, fl)
    out, g_mid, du, dd, d_mlp, d_su, d_sg = second(S, FS, mid, cotangent[0], w_down, su, sg, alpha_mlp, wu, w_upgate)
    g_x, dout, dqkv, d_attn, d_sqk = third(S, FS, hp, g_mid, x, attn, alpha_attn, mine, seg, gain, wo, wq, qkv, raw, res, hall)

    def row(v):
        return jnp.pad(v.reshape(1, -1), ((0, 0), (0, D - v.size)))

    vec = jnp.concatenate([row(d_mlp), row(d_attn), row(d_sqk), row(d_su), row(d_sg), jnp.zeros((3, D), F32)])
    d_up, d_down, d_o, d_q, tot, parts = fourth(S, FS, hp, vec, du, dd, dout, dqkv)
    sqk = parts[:, 2, :hw].reshape(-1)

    def own(v):
        return lax.dynamic_slice_in_dim(v, f * rows, rows)

    return (
        out[None], g_x[None], d_q.astype(F32), d_o.astype(F32), d_up.astype(F32), d_down.astype(F32),
        own(sqk), own(tot[1]), own(tot[0]), tot[3, :fl], tot[4, :fl],
    )


def solution(mesh):
    S, FS = mesh.shape["seq"], mesh.shape["fsdp"]
    tok = P(("grp", "fsdp"), "seq", None)
    w = P("fsdp", None)
    in_specs = (tok, P(("grp", "fsdp"), None), w, w, w, w, P(), P(), P(), P(), P(), tok)
    out_specs = (tok, tok, w, w, w, w) + (P("fsdp"),) * 5

    def run(*args):
        return body(S, FS, *args)

    return jax.shard_map(run, mesh=mesh, in_specs=in_specs, out_specs=out_specs, check_vma=False)
```

```python
import jax
import jax.numpy as jnp
from jax import lax
from jax.experimental import pallas as pl
from jax.experimental.pallas import tpu as pltpu
from jax.sharding import PartitionSpec as P

D = 1280
HEADS = 20
HEAD = 64

eps_norm = 1e-06
neg_big = -1e30
BF = jnp.bfloat16
F32 = jnp.float32
MESH = pl.DeviceIdType.MESH
ANY = pl.BlockSpec(memory_space=pl.ANY)
VM = pl.BlockSpec(memory_space=pltpu.VMEM)


def inv_rms(value):
    return lax.rsqrt(jnp.mean(value * value, axis=-1, keepdims=True) + eps_norm)


def back(unit, inv, grad):
    return (grad - unit * jnp.mean(grad * unit, axis=-1, keepdims=True)) * inv


def mm(a, b):
    return jnp.dot(a, b, preferred_element_type=F32)


def mm_nt(a, b):
    return lax.dot_general(a, b, (((1,), (1,)), ((), ())), preferred_element_type=F32)


def mm_tn(a, b):
    return lax.dot_general(a, b, (((0,), (0,)), ((), ())), preferred_element_type=F32)


def rcopy(src, dst, ss, rs, dev):
    return pltpu.make_async_remote_copy(src, dst, ss, rs, device_id=dev, device_id_type=MESH)


def greet(peers):
    bar = pltpu.get_barrier_semaphore()
    for p in peers:
        pl.semaphore_signal(bar, inc=1, device_id=p, device_id_type=MESH)
    pl.semaphore_wait(bar, len(peers))


def ds(start, size, mult):
    return pl.ds(pl.multiple_of(start, mult), size)


def visible(seg_col, seg_row, q0, k0, nq, nk):
    qi = q0 + lax.broadcasted_iota(jnp.int32, (nq, nk), 0)
    ki = k0 + lax.broadcasted_iota(jnp.int32, (nq, nk), 1)
    return (ki <= qi) & ((seg_row == 0) | (seg_row == seg_col))


def add_into(dst, src, chunk):
    def one(i, carry):
        at = ds(i * chunk, chunk, 16)
        dst[at] = (dst[at].astype(F32) + src[at].astype(F32)).astype(dst.dtype)
        return carry

    lax.fori_loop(0, src.shape[0] // chunk, one, 0)


def attn_bias(S, tok, half, bias, segc, segr):
    for qb in range(S):
        q0 = qb * tok
        k0 = q0 if q0 < half else half
        nk = q0 + tok - k0
        ok = visible(segc[q0 : q0 + tok], segr[:, k0 : k0 + nk], q0, k0, tok, nk)
        bias[qb, :, :nk] = jnp.where(ok, 0.0, neg_big).astype(BF)


def first_kernel(S, FS, hp, x_ref, segc, segr, wqkv, wout, gain, alpha, wup,
                 hall_o, wq_o, wo_o, wu_o, raw_o, qkv_o, res_o, mine_o, attn_o, mid_o,
                 hall, wq, wo, raw, qkv, res, bias, oh, mixs, mine, recv,
                 s_up, r_up, s_dn, r_dn, s_wq, r_wq, s_wo, r_wo, s_wu, r_wu, f_wq, f_wo, f_wu,
                 g_wq, g_wo, g_wu, s_mx, r_mx, out_sem):
    g, z, f = lax.axis_index("grp"), lax.axis_index("seq"), lax.axis_index("fsdp")
    tok = x_ref.shape[0]
    rows = wqkv.shape[0]
    hr = rows // 2
    hw = hp * HEAD
    ff = wup.shape[1] // 2
    fl = ff // FS
    total = S * tok
    half = total // 2
    fpeers = [lax.rem(f + i, FS) for i in range(1, FS)]
    zpeers = [lax.rem(z + i, S) for i in range(1, S)]
    greet([(g, z, p) for p in fpeers] + [(g, p, f) for p in zpeers] + [(1 - g, z, f)])

    x = x_ref[...].astype(F32)
    hall[z] = (x * inv_rms(x)).astype(BF)

    def up(t, b):
        return rcopy(hall.at[b], hall.at[b], s_up.at[t], r_up.at[t], (g, lax.rem(z + 1, S), f))

    def down(t, b):
        return rcopy(hall.at[b], hall.at[b], s_dn.at[t], r_dn.at[t], (g, lax.rem(z + S - 1, S), f))

    @pl.when(z + 1 < S)
    def _():
        up(0, z).start()

    @pl.when(z > 0)
    def _():
        down(0, z).start()

    for k in range(S):
        lo, hi = k * hw, min((k + 1) * hw, D)

        @pl.when(z == k)
        def _():
            parts = []
            for c in range(3):
                if hi > lo:
                    parts.append(wqkv[:, c * D + lo : c * D + hi])
                if hi - lo < hw:
                    parts.append(jnp.zeros((rows, hw - max(hi - lo, 0)), BF))
            wq[ds(f * rows, rows, 16)] = jnp.concatenate(parts, axis=1)

    def wq_half(src, gg):
        return wq.at[ds(src * rows + gg * hr, hr, 16)]

    def wo_half(src, gg):
        return wo.at[ds(src * rows + gg * hr, hr, 16)]

    c_wq = [rcopy(wq_half(f, g), wq_half(f, g), s_wq.at[i], r_wq.at[i], (g, z, p)) for i, p in enumerate(fpeers)]
    for c in c_wq:
        c.start()
    attn_bias(S, tok, half, bias, segc, segr)
    wo[ds(f * rows, rows, 16)] = wout[...]
    qkv[2, :, :, HEAD:] = jnp.where(lax.broadcasted_iota(jnp.int32, (hp, total, HEAD), 2) == 0, 1.0, 0.0).astype(BF)

    bpeers = [lax.rem(f + FS - i, FS) for i in range(1, FS)]
    partner = (1 - g, z, f)
    fw_wq = [rcopy(wq_half(p, g), wq_half(p, g), f_wq.at[i], g_wq.at[i], partner) for i, p in enumerate(bpeers)]
    for i in range(FS - 1):
        c_wq[i].wait_recv()
        fw_wq[i].start()
    c_wo = [rcopy(wo_half(f, g), wo_half(f, g), s_wo.at[i], r_wo.at[i], (g, z, p)) for i, p in enumerate(fpeers)]
    for c in c_wo:
        c.start()

    def wu_cp(i, p):
        return rcopy(wup.at[:, ds(g * ff + p * fl, fl, 128)], wu_o.at[g, f], s_wu.at[i], r_wu.at[i], (g, z, p))

    c_wu = [wu_cp(i, p) for i, p in enumerate(fpeers)]
    for c in c_wu:
        c.start()
    for i in range(FS - 1):
        fw_wq[i].wait_recv()

    def step(i, carry):
        t = lax.div(i - 1, 2)
        is_up = lax.rem(i, 2) == 1
        b = jnp.where(i == 0, z, jnp.where(is_up, z - 1 - t, z + 1 + t))

        @pl.when((b >= 0) & (b < S))
        def _():
            @pl.when((i > 0) & is_up)
            def _():
                up(t, b).wait_recv()

                @pl.when(z + 1 < S)
                def _():
                    up(t + 1, b).start()

            @pl.when((i > 0) & jnp.logical_not(is_up))
            def _():
                down(t, b).wait_recv()

                @pl.when(z > 0)
                def _():
                    down(t + 1, b).start()

            acc = mm(hall[b], wq[...])
            at = ds(b * tok, tok, 16)
            for j in range(hp):
                for c in range(2):
                    v = acc[:, c * hw + j * HEAD : c * hw + (j + 1) * HEAD]
                    raw[c, j, at, :] = v
                    u = v * inv_rms(v) * gain[j : j + 1]
                    qkv[c, j, at, :HEAD] = u.astype(BF)
                qkv[2, j, at, :HEAD] = acc[:, 2 * hw + j * HEAD : 2 * hw + (j + 1) * HEAD].astype(BF)

        return carry

    lax.fori_loop(0, 2 * S - 1, step, 0)
    outs = [
        pltpu.make_async_copy(hall, hall_o, out_sem.at[0]),
        pltpu.make_async_copy(wq, wq_o, out_sem.at[1]),
        pltpu.make_async_copy(raw, raw_o, out_sem.at[2]),
        pltpu.make_async_copy(qkv, qkv_o, out_sem.at[3]),
    ]
    for c in outs:
        c.start()

    def mx(qb):
        return rcopy(mixs.at[qb], recv.at[z], s_mx.at[qb], r_mx.at[z], (g, qb, f))

    for qb in reversed(range(S)):
        q0 = qb * tok
        n = q0 + tok
        k0 = q0 if q0 < half else half

        def head(j, carry):
            q = qkv[0, j, q0:n, :HEAD] * jnp.asarray(HEAD**-0.5, BF)
            s = mm_nt(q, qkv[1, j, :n, :HEAD])
            tail = s[:, k0:] + bias[qb, :, : n - k0].astype(F32)
            e = jnp.exp(jnp.concatenate([s[:, :k0], tail], axis=1) if k0 else tail)
            o = mm(e.astype(BF), qkv[2, j, :n])
            rinv = 1.0 / o[:, HEAD : HEAD + 1]
            o = o[:, :HEAD] * rinv
            res[j, q0:n, :HEAD] = o
            res[j, q0:n, HEAD:] = jnp.broadcast_to(rinv, (tok, HEAD))
            oh[j] = o.astype(BF)
            return carry

        lax.fori_loop(0, hp, head, 0)
        block = jnp.concatenate([oh[j] for j in range(hp)], axis=1)
        mixs[qb] = block

        @pl.when(z != qb)
        def _():
            mx(qb).start()

        @pl.when(z == qb)
        def _():
            recv[qb] = block

        if qb == S - 1:
            fw_wo = [rcopy(wo_half(p, g), wo_half(p, g), f_wo.at[i], g_wo.at[i], partner) for i, p in enumerate(bpeers)]
            for i in range(FS - 1):
                c_wo[i].wait_recv()
                fw_wo[i].start()

    fw_wu = [rcopy(wu_o.at[g, p], wu_o.at[g, p], f_wu.at[i], g_wu.at[i], partner) for i, p in enumerate(bpeers)]
    for i in range(FS - 1):
        c_wu[i].wait_recv()
        fw_wu[i].start()
    for i in range(FS - 1):
        fw_wo[i].wait_recv()
    outs2 = [pltpu.make_async_copy(wo, wo_o, out_sem.at[4]), pltpu.make_async_copy(res, res_o, out_sem.at[5])]
    for c in outs2:
        c.start()
    for k in range(S):
        @pl.when(z != k)
        def _():
            rcopy(mixs.at[0], recv.at[k], s_mx.at[0], r_mx.at[k], (g, k, f)).wait_recv()

    mine[...] = jnp.concatenate([recv[k] for k in range(S)], axis=1)[:, :D]
    attn = mm(mine[...], wo[...])
    attn_o[...] = attn
    mine_o[...] = mine[...]
    x = x_ref[...].astype(F32)
    h = x * inv_rms(x)
    n_ = h + alpha[...] * (attn * inv_rms(attn) - h)
    mid_o[...] = n_ * inv_rms(n_)

    for t in range(S - 1):
        @pl.when((z + 1 < S) & (z - t >= 0))
        def _():
            up(t, z).wait_send()

        @pl.when((z > 0) & (z + t < S))
        def _():
            down(t, z).wait_send()

    for i in range(FS - 1):
        c_wq[i].wait_send()
        c_wo[i].wait_send()
        c_wu[i].wait_send()
        fw_wq[i].wait_send()
        fw_wo[i].wait_send()
        fw_wu[i].wait()
    for k in range(S):
        @pl.when(z != k)
        def _():
            mx(k).wait_send()
    for c in outs + outs2:
        c.wait()


def first(S, FS, hp, x, seg, wqkv, wout, gain, alpha, wup):
    tok, total = x.shape[0], seg.shape[0]
    rows = wqkv.shape[0]
    hw = hp * HEAD
    fl = wup.shape[1] // 2 // FS
    sds = jax.ShapeDtypeStruct
    outs = [
        sds((S, tok, D), BF), sds((D, 3 * hw), BF), sds((D, D), BF), sds((2, FS, rows, fl), BF),
        sds((2, hp, total, HEAD), F32), sds((3, hp, total, 2 * HEAD), BF), sds((hp, total, 2 * HEAD), F32),
        sds((tok, D), BF), sds((tok, D), F32), sds((tok, D), F32),
    ]
    dma = lambda n: pltpu.SemaphoreType.DMA((n,))
    F1 = FS - 1
    return pl.pallas_call(
        lambda *refs: first_kernel(S, FS, hp, *refs),
        out_shape=outs,
        in_specs=[VM] * 7 + [ANY],
        out_specs=[ANY] * 7 + [VM] * 3,
        scratch_shapes=[
            pltpu.VMEM((S, tok, D), BF), pltpu.VMEM((D, 3 * hw), BF), pltpu.VMEM((D, D), BF),
            pltpu.VMEM((2, hp, total, HEAD), F32), pltpu.VMEM((3, hp, total, 2 * HEAD), BF),
            pltpu.VMEM((hp, total, 2 * HEAD), F32), pltpu.VMEM((S, tok, total // 2), BF),
            pltpu.VMEM((hp, tok, HEAD), BF), pltpu.VMEM((S, tok, hw), BF), pltpu.VMEM((tok, D), BF),
            pltpu.VMEM((S, tok, hw), BF),
            dma(S), dma(S), dma(S), dma(S), dma(F1), dma(F1), dma(F1), dma(F1), dma(F1), dma(F1),
            dma(F1), dma(F1), dma(F1), dma(F1), dma(F1), dma(F1), dma(S), dma(S), dma(6),
        ],
        compiler_params=pltpu.CompilerParams(collective_id=1, has_side_effects=True, vmem_limit_bytes=60 * 2**20),
        name="first",
    )(x, seg.reshape(total, 1), seg.reshape(1, total), wqkv, wout, gain, alpha.reshape(1, D), wup)


def second_kernel(S, FS, NC, mid, cot, wd, su, sg, alpha, wu_i, wup,
                  out_o, gmid_o, du_o, dd_o, dal_o, dsu_o, dsg_o,
                  wu, mida, up, gate, hid, ps, pr, rl, gma, gu, dup, ddn, lu, ld,
                  s_a, r_a, s_b, r_b, s_c, r_c, s_d, r_d, w_sem, s_x, r_x, out_sem):
    g, z, f = lax.axis_index("grp"), lax.axis_index("seq"), lax.axis_index("fsdp")
    tok = mid.shape[0]
    ct = tok // NC
    hc = ct // 2
    fl = wd.shape[0]
    ff = wup.shape[1] // 2
    rows = wup.shape[0]
    hl = fl // 2
    nt = 256 if fl % 256 == 0 else 128
    M = FS * ct
    relay = FS == 4
    peers = [lax.rem(f + i, FS) for i in range(1, FS)]
    partner = (1 - g, z, f)
    greet([(g, z, p) for p in peers] + [partner])
    R = range(FS - 1)
    A, B = pl.ds(0, hc), pl.ds(hc, hc)
    if relay:
        fx, fy, fd = f + 1 - 2 * lax.rem(f, 2), lax.rem(f + 2, 4), 3 - f
        dx, dy = (g, z, fx), (g, z, fy)

    def direct(buf, ss, rs, c, i):
        return rcopy(buf.at[c, f], buf.at[c, f], ss.at[c, i], rs.at[c, i], (g, z, peers[i]))

    def gcopy(buf, ss, rs, c, k):
        src, half, dev = ((f, A, dx), (f, B, dx), (f, B, dy), (f, A, dy), (fx, A, dy), (fy, B, dx))[k]
        view = buf.at[c, src, half]
        return rcopy(view, view, ss.at[c, k], rs.at[c, k], dev)

    def g_issue(buf, ss, rs, c):
        if relay:
            for k in (0, 2, 1, 3):
                gcopy(buf, ss, rs, c, k).start()
        else:
            for i in R:
                direct(buf, ss, rs, c, i).start()

    def g_relay(buf, ss, rs, c):
        if relay:
            for k in (0, 2):
                gcopy(buf, ss, rs, c, k).wait_recv()
                gcopy(buf, ss, rs, c, 4 if k == 0 else 5).start()

    def g_wait(buf, ss, rs, c):
        if relay:
            for k in (1, 3, 4, 5):
                gcopy(buf, ss, rs, c, k).wait_recv()
        else:
            for i in R:
                direct(buf, ss, rs, c, i).wait_recv()

    def g_sent(buf, ss, rs, c):
        if relay:
            for k in range(6):
                gcopy(buf, ss, rs, c, k).wait_send()
        else:
            for i in R:
                direct(buf, ss, rs, c, i).wait_send()

    def scopy(ss, rs, c, k):
        src, dst, dev = (
            (ps.at[c, fd, A], rl.at[c, 0], dx),
            (ps.at[c, fd, B], rl.at[c, 1], dy),
            (ps.at[c, fx, A], pr.at[c, 0, A], dx),
            (ps.at[c, fy, B], pr.at[c, 1, B], dy),
            (ps.at[c, fy, A], pr.at[c, 1, A], dy),
            (ps.at[c, fx, B], pr.at[c, 0, B], dx),
        )[k]
        return rcopy(src, dst, ss.at[c, k], rs.at[c, k], dev)

    def sdirect(ss, rs, c, i):
        return rcopy(ps.at[c, peers[i]], pr.at[c, i], ss.at[c, i], rs.at[c, i], (g, z, peers[i]))

    def s_issue(ss, rs, c):
        if relay:
            for k in range(4):
                scopy(ss, rs, c, k).start()
        else:
            for i in R:
                sdirect(ss, rs, c, i).start()

    def s_relay(ss, rs, c):
        if relay:
            for k, tgt, half in ((0, fy, A), (1, fx, B)):
                scopy(ss, rs, c, k).wait_recv()
                ps[c, tgt, half] = (ps[c, tgt, half].astype(F32) + rl[c, k].astype(F32)).astype(BF)
                scopy(ss, rs, c, 4 + k).start()

    def s_total(ss, rs, c):
        if relay:
            for k in range(2, 6):
                scopy(ss, rs, c, k).wait_recv()
        else:
            for i in R:
                sdirect(ss, rs, c, i).wait_recv()
        acc = ps[c, f].astype(F32)
        for i in range(2 if relay else FS - 1):
            acc = acc + pr[c, i].astype(F32)
        return acc

    def s_sent(ss, rs, c):
        if relay:
            for k in range(6):
                scopy(ss, rs, c, k).wait_send()
        else:
            for i in R:
                sdirect(ss, rs, c, i).wait_send()

    for c in range(NC):
        mida[c, f] = mid[c * ct : (c + 1) * ct].astype(BF)
        g_issue(mida, s_a, r_a, c)
        if c == 0:
            loads = []
            for k in range(2):
                loads.append(pltpu.make_async_copy(wup.at[:, ds(k * ff + f * fl, fl, 128)], wu.at[k, ds(f * rows, rows, 16)], w_sem.at[k, 0]))
                for i in R:
                    loads.append(pltpu.make_async_copy(wu_i.at[k, peers[i]], wu.at[k, ds(peers[i] * rows, rows, 16)], w_sem.at[k, i + 1]))
            for ld_c in loads:
                ld_c.start()
            dsu_o[...] = jnp.zeros_like(dsu_o)
            dsg_o[...] = jnp.zeros_like(dsg_o)
            dal_o[...] = jnp.zeros_like(dal_o)
        g_relay(mida, s_a, r_a, c)
    for ld_c in loads:
        ld_c.wait()

    for c in range(NC):
        g_wait(mida, s_a, r_a, c)

        def fwd(t, carry):
            cols = ds(t * nt, nt, 128)
            a_in = mida[c].reshape(M, D)
            u = mm(a_in, wu[0, :, cols])
            gt = mm(a_in, wu[1, :, cols])
            up[c, :, cols] = u
            gate[c, :, cols] = gt
            a = gt * sg[:, cols]
            hid[c, :, cols] = (u * su[:, cols] * (a * jax.nn.sigmoid(a))).astype(BF)
            return carry

        lax.fori_loop(0, fl // nt, fwd, 0)
        if c:
            s_relay(s_b, r_b, c - 1)

        def proj(t, carry):
            cols = ds(t * 256, 256, 128)
            ps[c, :, :, cols] = mm(hid[c], wd[:, cols]).astype(BF).reshape(FS, ct, 256)
            return carry

        lax.fori_loop(0, D // 256, proj, 0)
        s_issue(s_b, r_b, c)
    s_relay(s_b, r_b, NC - 1)

    for c in range(NC):
        at = slice(c * ct, (c + 1) * ct)
        mlp = s_total(s_b, r_b, c)
        al = alpha[...]
        md = mid[at]
        inv_m = inv_rms(mlp)
        um = mlp * inv_m
        dif = um - md
        m = md + al * dif
        inv_o = inv_rms(m)
        o = m * inv_o
        out_o[at] = o.astype(BF)
        g_m = back(o, inv_o, cot[at].astype(F32))
        dal_o[...] += jnp.sum(g_m * dif, axis=0, keepdims=True)
        gmid_o[at] = (1 - al) * g_m
        gma[c, f] = back(um, inv_m, al * g_m).astype(BF)
        g_issue(gma, s_c, r_c, c)
        g_relay(gma, s_c, r_c, c)

    for c in range(NC):
        g_wait(gma, s_c, r_c, c)

        def bwd(t, carry):
            cols = ds(t * nt, nt, 128)
            gh = mm_nt(gma[c].reshape(M, D), wd[cols, :])
            u = up[c, :, cols]
            gt = gate[c, :, cols]
            sgc = sg[:, cols]
            suc = su[:, cols]
            a = gt * sgc
            sig = jax.nn.sigmoid(a)
            gs = gh * (a * sig)
            gu[0, c, :, cols] = (gs * suc).astype(BF)
            dsu_o[:, cols] += jnp.sum(u * gs, axis=0, keepdims=True)
            g_a = gh * u * suc * (sig * (1 + a * (1 - sig)))
            gu[1, c, :, cols] = (g_a * sgc).astype(BF)
            dsg_o[:, cols] += jnp.sum(gt * g_a, axis=0, keepdims=True)
            return carry

        lax.fori_loop(0, fl // nt, bwd, 0)
        if c:
            s_relay(s_d, r_d, c - 1)
        s_sent(s_b, r_b, c)

        def bproj(t, carry):
            cols = ds(t * 256, 256, 128)
            v = mm_nt(gu[0, c], wu[0, cols, :]) + mm_nt(gu[1, c], wu[1, cols, :])
            ps[c, :, :, cols] = v.astype(BF).reshape(FS, ct, 256)
            return carry

        lax.fori_loop(0, D // 256, bproj, 0)
        s_issue(s_d, r_d, c)

    def dwd(t, carry):
        cols = ds(t * nt, nt, 128)
        ddn[cols, :] = mm_tn(hid[:, :, cols].reshape(NC * M, nt), gma[...].reshape(NC * M, D)).astype(BF)
        return carry

    lax.fori_loop(0, fl // nt, dwd, 0)
    s_relay(s_d, r_d, NC - 1)
    x_d = rcopy(ddn.at[ds((1 - g) * hl, hl, 16)], ld, s_x.at[0], r_x.at[0], partner)
    x_d.start()

    def dwu(k):
        def one(t, carry):
            cols = ds(t * 256, 256, 128)
            dup[k, cols, :] = mm_tn(mida[:, :, :, cols].reshape(NC * M, 256), gu[k].reshape(NC * M, fl)).astype(BF)
            return carry

        lax.fori_loop(0, D // 256, one, 0)

    dwu(1 - g)
    x_u = rcopy(dup.at[1 - g], lu, s_x.at[1], r_x.at[1], partner)
    x_u.start()
    dwu(g)
    mine = ds(g * hl, hl, 16)
    x_d.wait_recv()
    add_into(ddn.at[mine], ld, 64)
    o_d = pltpu.make_async_copy(ddn.at[mine], dd_o, out_sem.at[0])
    o_d.start()
    x_u.wait_recv()
    add_into(dup.at[g], lu, 64)
    o_u = pltpu.make_async_copy(dup.at[g], du_o, out_sem.at[1])
    o_u.start()

    for c in range(NC):
        at = slice(c * ct, (c + 1) * ct)
        gmid_o[at] = gmid_o[at] + s_total(s_d, r_d, c)
    for c in range(NC):
        g_sent(mida, s_a, r_a, c)
        g_sent(gma, s_c, r_c, c)
        s_sent(s_d, r_d, c)
    x_d.wait_send()
    x_u.wait_send()
    o_d.wait()
    o_u.wait()


def second(S, FS, mid, cot, wd, su, sg, alpha, wu, wup):
    NC = 2
    tok = mid.shape[0]
    ct = tok // NC
    fl = wd.shape[0]
    M = FS * ct
    sds = jax.ShapeDtypeStruct
    outs = [sds((tok, D), BF), sds((tok, D), F32), sds((D, fl), BF), sds((fl // 2, D), BF),
            sds((1, D), F32), sds((1, fl), F32), sds((1, fl), F32)]
    dma = pltpu.SemaphoreType.DMA
    F1 = FS - 1
    return pl.pallas_call(
        lambda *refs: second_kernel(S, FS, NC, *refs),
        out_shape=outs,
        in_specs=[VM] * 6 + [ANY] * 2,
        out_specs=[VM, VM, ANY, ANY, VM, VM, VM],
        scratch_shapes=[
            pltpu.VMEM((2, D, fl), BF), pltpu.VMEM((NC, FS, ct, D), BF), pltpu.VMEM((NC, M, fl), F32),
            pltpu.VMEM((NC, M, fl), F32), pltpu.VMEM((NC, M, fl), BF), pltpu.VMEM((NC, FS, ct, D), BF),
            pltpu.VMEM((NC, 2 if FS == 4 else F1, ct, D), BF), pltpu.VMEM((NC, 2, ct // 2, D), BF),
            pltpu.VMEM((NC, FS, ct, D), BF), pltpu.VMEM((2, NC, M, fl), BF),
            pltpu.VMEM((2, D, fl), BF), pltpu.VMEM((fl, D), BF), pltpu.VMEM((D, fl), BF), pltpu.VMEM((fl // 2, D), BF),
        ] + [dma((NC, max(F1, 6)))] * 8 + [dma((2, FS)), dma((2,)), dma((2,)), dma((2,))],
        compiler_params=pltpu.CompilerParams(collective_id=2, has_side_effects=True, vmem_limit_bytes=63 * 2**20),
        name="second",
    )(mid, cot, wd, su, sg, alpha.reshape(1, D), wu, wup)


def third_kernel(S, FS, hp, gmid, x_ref, attn, alpha, mine, segc, segr, gain, wo, wq_i, qkv_i, raw_i, res_i, hall_i,
                 gx_o, dout_o, dqkv_o, dal_o, dsq_o,
                 wq, qkv, raw, res, hall, gh1, ga, gsend, gxr, bias, hx, gqh, dkv, gq, ps, pr, dout, dqk, lo, lq,
                 ld_sem, h_sem, s_gx, r_gx, s_p, r_p, s_x, r_x, out_sem):
    g, z, f = lax.axis_index("grp"), lax.axis_index("seq"), lax.axis_index("fsdp")
    tok = x_ref.shape[0]
    hw = hp * HEAD
    wide = S * hw
    total = S * tok
    half = total // 2
    w2 = 3 * hw // 2
    dh = D // 2
    partner = (1 - g, z, f)
    greet([(g, lax.rem(z + i, S), f) for i in range(1, S)] + [partner])
    loads = [pltpu.make_async_copy(a, b, ld_sem.at[i]) for i, (a, b) in enumerate(
        [(qkv_i, qkv), (raw_i, raw), (res_i, res), (wq_i, wq)])]
    for c in loads:
        c.start()

    def h_tile(t):
        return pltpu.make_async_copy(hall_i.at[:, :, pl.ds(t * 256, 256)], hall.at[t % 2], h_sem.at[t % 2])

    h_tile(0).start()
    h_tile(1).start()
    dal_o[...] = jnp.zeros_like(dal_o)
    dsq_o[...] = jnp.zeros_like(dsq_o)
    cr = tok // 4

    def pre(i, carry):
        at = ds(i * cr, cr, 16)
        x = x_ref[at].astype(F32)
        h = x * inv_rms(x)
        av = attn[at]
        inv_a = inv_rms(av)
        ua = av * inv_a
        al = alpha[...]
        dif = ua - h
        n_ = h + al * dif
        inv_n = inv_rms(n_)
        g_n = back(n_ * inv_n, inv_n, gmid[at])
        dal_o[...] += jnp.sum(g_n * dif, axis=0, keepdims=True)
        gh1[at] = (1 - al) * g_n
        ga[at] = back(ua, inv_a, al * g_n).astype(BF)
        return carry

    lax.fori_loop(0, 4, pre, 0)
    gmix = mm_nt(ga[...], wo[...]).astype(BF)
    if wide > D:
        gmix = jnp.concatenate([gmix, jnp.zeros((tok, wide - D), BF)], axis=1)
    for k in range(S):
        gsend[k] = gmix[:, k * hw : (k + 1) * hw]

    def gx(k):
        return rcopy(gsend.at[k], gxr.at[z], s_gx.at[k], r_gx.at[z], (g, k, f))

    for k in range(S):
        @pl.when(z != k)
        def _():
            gx(k).start()

        @pl.when(z == k)
        def _():
            gxr[k] = gsend[k]

    def dwo(t, carry):
        cols = ds(t * 256, 256, 128)
        v = mm_tn(mine[:, cols], ga[...]).astype(BF)
        dout[0, cols, :] = v[:, :dh]
        dout[1, cols, :] = v[:, dh:]
        return carry

    lax.fori_loop(0, D // 256, dwo, 0)
    x_o = rcopy(dout.at[1 - g], lo, s_x.at[0], r_x.at[0], partner)
    x_o.start()
    attn_bias(S, tok, half, bias, segc, segr)
    for c in loads:
        c.wait()

    def part(k):
        return rcopy(ps.at[k], pr.at[z], s_p.at[k], r_p.at[z], (g, k, f))

    for qb in reversed(range(S)):
        q0 = qb * tok
        n = q0 + tok
        k0 = q0 if q0 < half else half

        @pl.when(z != qb)
        def _():
            rcopy(gsend.at[0], gxr.at[qb], s_gx.at[0], r_gx.at[qb], (g, qb, f)).wait_recv()

        for j in range(hp):
            hx[j] = gxr[qb, :, j * HEAD : (j + 1) * HEAD]

        def head(j, carry):
            q = qkv[0, j, q0:n, :HEAD] * jnp.asarray(HEAD**-0.5, BF)
            keys = qkv[1, j, :n, :HEAD]
            gv = hx[j]
            rinv = res[j, q0:n, HEAD : HEAD + 1]
            delta = jnp.sum(gv.astype(F32) * res[j, q0:n, :HEAD], axis=-1, keepdims=True)
            s = mm_nt(q, keys)
            tail = s[:, k0:] + bias[qb, :, : n - k0].astype(F32)
            p = jnp.exp(jnp.concatenate([s[:, :k0], tail], axis=1) if k0 else tail) * rinv
            dp = mm_nt(gv, qkv[2, j, :n, :HEAD])
            dsb = (p * (dp - delta)).astype(BF)
            dq = mm(dsb, keys) * HEAD**-0.5
            dk = mm_tn(dsb, q)
            dv = mm_tn(p.astype(BF), gv)
            if qb < S - 1:
                dk = dk + dkv[j, :n, :HEAD]
                dv = dv + dkv[j, :n, HEAD:]
            if qb:
                dkv[j, :q0, :HEAD] = dk[:q0]
                dkv[j, :q0, HEAD:] = dv[:q0]
            gj = gain[pl.ds(j, 1), :]
            for c, d in ((0, dq), (1, dk[q0:])):
                v = raw[c, j, q0:n]
                inv = inv_rms(v)
                u = v * inv
                dsq_o[pl.ds(j, 1), :] += jnp.sum(d * u, axis=0, keepdims=True)
                gqh[c, j] = back(u, inv, d * gj).astype(BF)
            gqh[2, j] = dv[q0:].astype(BF)
            return carry

        lax.fori_loop(0, hp, head, 0)
        gq[qb] = jnp.concatenate([gqh[c, j] for c in range(3) for j in range(hp)], axis=1)
        ps[qb] = mm_nt(gq[qb], wq[...]).astype(BF)

        @pl.when(z != qb)
        def _():
            part(qb).start()

    for t in range(D // 256):
        h_tile(t).wait()
        v = mm_tn(hall[t % 2].reshape(total, 256), gq[...].reshape(total, 3 * hw)).astype(BF)
        dqk[0, t * 256 : (t + 1) * 256, :] = v[:, :w2]
        dqk[1, t * 256 : (t + 1) * 256, :] = v[:, w2:]
        if t + 2 < D // 256:
            h_tile(t + 2).start()
    x_q = rcopy(dqk.at[1 - g], lq, s_x.at[1], r_x.at[1], partner)
    x_q.start()
    x_o.wait_recv()
    add_into(dout.at[g], lo, 128)
    o_o = pltpu.make_async_copy(dout.at[g], dout_o, out_sem.at[0])
    o_o.start()
    x_q.wait_recv()
    add_into(dqk.at[g], lq, 128)
    o_q = pltpu.make_async_copy(dqk.at[g], dqkv_o, out_sem.at[1])
    o_q.start()

    add_into(gh1, ps.at[z], 64)
    for k in range(S):
        @pl.when(z != k)
        def _():
            rcopy(ps.at[0], pr.at[k], s_p.at[0], r_p.at[k], (g, k, f)).wait_recv()
            add_into(gh1, pr.at[k], 64)

    def post(i, carry):
        at = ds(i * cr, cr, 16)
        x = x_ref[at].astype(F32)
        inv = inv_rms(x)
        gx_o[at] = back(x * inv, inv, gh1[at])
        return carry

    lax.fori_loop(0, 4, post, 0)
    for k in range(S):
        @pl.when(z != k)
        def _():
            gx(k).wait_send()
            part(k).wait_send()
    x_o.wait_send()
    x_q.wait_send()
    o_o.wait()
    o_q.wait()


def third(S, FS, hp, gmid, x, attn, alpha, mine, seg, gain, wo, wq, qkv, raw, res, hall):
    tok, total = x.shape[0], seg.shape[0]
    hw = hp * HEAD
    sds = jax.ShapeDtypeStruct
    outs = [sds((tok, D), F32), sds((D, D // 2), BF), sds((D, 3 * hw // 2), BF), sds((1, D), F32), sds((hp, HEAD), F32)]
    dma = lambda n: pltpu.SemaphoreType.DMA((n,))
    return pl.pallas_call(
        lambda *refs: third_kernel(S, FS, hp, *refs),
        out_shape=outs,
        in_specs=[VM] * 9 + [ANY] * 5,
        out_specs=[VM, ANY, ANY, VM, VM],
        scratch_shapes=[
            pltpu.VMEM((D, 3 * hw), BF), pltpu.VMEM((3, hp, total, 2 * HEAD), BF), pltpu.VMEM((2, hp, total, HEAD), F32),
            pltpu.VMEM((hp, total, 2 * HEAD), F32), pltpu.VMEM((2, S, tok, 256), BF), pltpu.VMEM((tok, D), F32),
            pltpu.VMEM((tok, D), BF), pltpu.VMEM((S, tok, hw), BF), pltpu.VMEM((S, tok, hw), BF),
            pltpu.VMEM((S, tok, total // 2), BF), pltpu.VMEM((hp, tok, HEAD), BF), pltpu.VMEM((3, hp, tok, HEAD), BF),
            pltpu.VMEM((hp, total, 2 * HEAD), F32), pltpu.VMEM((S, tok, 3 * hw), BF), pltpu.VMEM((S, tok, D), BF),
            pltpu.VMEM((S, tok, D), BF), pltpu.VMEM((2, D, D // 2), BF), pltpu.VMEM((2, D, 3 * hw // 2), BF),
            pltpu.VMEM((D, D // 2), BF), pltpu.VMEM((D, 3 * hw // 2), BF),
            dma(4), dma(2), dma(S), dma(S), dma(S), dma(S), dma(2), dma(2), dma(2),
        ],
        compiler_params=pltpu.CompilerParams(collective_id=3, has_side_effects=True, vmem_limit_bytes=63 * 2**20),
        name="third",
    )(gmid, x, attn, alpha.reshape(1, D), mine, seg.reshape(total, 1), seg.reshape(1, total), gain, wo, wq, qkv, raw, res, hall)


def fourth_kernel(S, FS, hp, vec, du, dd, dout, dqkv,
                  up_o, dn_o, out_o, qkv_o, vec_o, sqk_o,
                  own_u, raw_u, oth_u, own_d, raw_d, oth_d, own_o, raw_o, oth_o, so, xo, sq, xq, agq, va, vb, vf, vz,
                  ld_sem, s_u, r_u, s_xo, r_xo, s_xq, r_xq, s_in, r_raw, r_oth, s_ret,
                  s_aq, r_aq, s_fq, r_fq, s_v, r_v, o_sem, s_o, r_o):
    g, z, f = lax.axis_index("grp"), lax.axis_index("seq"), lax.axis_index("fsdp")
    rows = own_u.shape[1]
    fl = own_u.shape[2]
    hl = own_d.shape[0]
    ff = fl * FS
    hw = hp * HEAD
    w2 = 3 * hw // 2
    dh = D // 2
    peers = [lax.rem(f + i, FS) for i in range(1, FS)]
    bpeers = [lax.rem(f + FS - i, FS) for i in range(1, FS)]
    zpeers = [lax.rem(z + i, S) for i in range(1, S)]
    zb = [lax.rem(z + S - i, S) for i in range(1, S)]
    partner = (1 - g, z, f)
    R = range(FS - 1)
    greet([(g, z, p) for p in peers] + [(g, p, f) for p in zpeers] + [partner])

    def blk(p):
        return ds(p * rows, rows, 16)

    l_d = pltpu.make_async_copy(dd, own_d, ld_sem.at[0])
    l_o = pltpu.make_async_copy(dout.at[blk(f)], so, ld_sem.at[1])
    l_q = pltpu.make_async_copy(dqkv.at[blk(f)], sq, ld_sem.at[2])
    l_u = pltpu.make_async_copy(du.at[blk(f)], own_u.at[f], ld_sem.at[3])
    for c in (l_d, l_o, l_q, l_u):
        c.start()
    c_o = [rcopy(dout.at[blk(p)], xo.at[i], s_xo.at[i], r_xo.at[i], (g, z, p)) for i, p in enumerate(peers)]
    c_q = [rcopy(dqkv.at[blk(p)], xq.at[i], s_xq.at[i], r_xq.at[i], (g, z, p)) for i, p in enumerate(peers)]
    c_u = [rcopy(du.at[blk(p)], own_u.at[f], s_u.at[i], r_u.at[i], (g, z, p)) for i, p in enumerate(peers)]
    va[...] = vec[...]
    v_c = rcopy(va, vb, s_v.at[0], r_v.at[0], partner)
    v_c.start()
    for c in c_q + c_o + c_u:
        c.start()

    lower = z < S // 2
    inner = jnp.where(lower, z + 1, z - 1)
    outer = jnp.where(lower, z - 1, z + 1)
    mid = (z == S // 2 - 1) | (z == S // 2)
    has_outer = (z > 0) & (z < S - 1)
    outer = jnp.where(has_outer, outer, inner)

    pieces = []
    nd = 4
    for i in range(nd):
        a = pl.ds(i * (hl // nd), hl // nd)
        pieces.append((own_d.at[a], raw_d.at[a], oth_d.at[a],
                       lambda o, i=i: o[1].at[ds(g * hl + i * (hl // nd), hl // nd, 16)]))
    order = [(f, -1)] + [(p, i) for i, p in enumerate(bpeers)]
    for p, i in order:
        if i == 0:
            pieces.append((own_o, raw_o, oth_o, lambda o: o[2].at[:, ds(g * dh, dh, 128)]))
        for k in range(2):
            a = pl.ds(k * (rows // 2), rows // 2)
            pieces.append((own_u.at[p, a], raw_u.at[p, a], oth_u.at[p, a],
                           lambda o, p=p, a=a: o[0].at[a, ds(g * ff + p * fl, fl, 128)]))

    def toward(i, to_mid):
        own, raw, oth, _ = pieces[i]
        if to_mid:
            return rcopy(own, oth, s_in.at[i], r_oth.at[i], (g, inner, f))
        return rcopy(own, raw, s_in.at[i], r_raw.at[i], (g, inner, f))

    def returned(i, from_mid):
        own, raw, oth, _ = pieces[i]
        return rcopy(raw if from_mid else oth, oth, s_ret.at[i], r_oth.at[i], (g, outer, f))

    def go_in(i):
        own, raw, oth, _ = pieces[i]

        @pl.when(has_outer)
        def _():
            rcopy(own, raw, s_in.at[i], r_raw.at[i], (g, outer, f)).wait_recv()
            own[...] = (own[...].astype(F32) + raw[...].astype(F32)).astype(BF)

        @pl.when(mid)
        def _():
            toward(i, True).start()

        @pl.when(jnp.logical_not(mid))
        def _():
            toward(i, False).start()

    outs = (up_o, dn_o, out_o)

    def local_out(i, src):
        return pltpu.make_async_copy(src, pieces[i][3](outs), o_sem.at[i])

    def remote_out(i, src):
        dst = pieces[i][3](outs)
        return rcopy(src, dst, s_o.at[i], r_o.at[i], partner)

    def mid_out(i):
        own, raw, oth, _ = pieces[i]
        rcopy(own, oth, s_in.at[i], r_oth.at[i], (g, inner, f)).wait_recv()
        raw[...] = (own[...].astype(F32) + oth[...].astype(F32)).astype(BF)

        @pl.when(has_outer)
        def _():
            returned(i, True).start()

        local_out(i, raw).start()
        remote_out(i, raw).start()

    def other_out(i):
        own, raw, oth, _ = pieces[i]
        rcopy(own, oth, s_in.at[i], r_oth.at[i], (g, inner, f)).wait_recv()

        @pl.when(has_outer)
        def _():
            returned(i, False).start()

        local_out(i, oth).start()
        remote_out(i, oth).start()

    total = len(pieces)
    lag = 5

    def step(i):
        if i < total:
            go_in(i)
        if 1 <= i <= total:
            @pl.when(mid)
            def _():
                mid_out(i - 1)
        if i >= lag:
            @pl.when(jnp.logical_not(mid))
            def _():
                other_out(i - lag)

    def add_all(own, recv):
        acc = own[...].astype(F32)
        for i in R:
            acc = acc + recv[i].astype(F32)
        return acc.astype(BF)

    def aq(i):
        return rcopy(agq.at[z, g], agq.at[z, g], s_aq.at[i], r_aq.at[i], (g, zpeers[i], f))

    def fq(i):
        src = z if i < 0 else zb[i]
        return rcopy(agq.at[src, g], agq.at[src, g], s_fq.at[i + 1], r_fq.at[i + 1], partner)

    l_d.wait()
    for i in range(nd):
        step(i)
    v_c.wait()
    vf[f] = va[...] + vb[...]
    v_f = [rcopy(vf.at[f], vf.at[f], s_v.at[1 + i], r_v.at[1 + i], (g, z, p)) for i, p in enumerate(peers)]
    for c in v_f:
        c.start()
    l_u.wait()
    step(nd)
    step(nd + 1)
    l_o.wait()
    for c in c_o:
        c.wait()
    own_o[...] = add_all(so, xo)
    step(nd + 2)
    for c in v_f:
        c.wait()
    acc = vf[0]
    for i in range(1, FS):
        acc = acc + vf[i]
    sub = lax.broadcasted_iota(jnp.int32, acc.shape, 0)
    vz[z] = jnp.where(sub < 3, acc, vf[f])
    v_z = [rcopy(vz.at[z], vz.at[z], s_v.at[FS + i], r_v.at[FS + i], (g, p, f)) for i, p in enumerate(zpeers)]
    for c in v_z:
        c.start()
    l_q.wait()
    for c in c_q:
        c.wait()
    agq[z, g] = add_all(sq, xq)
    n = nd + 3
    for i in R:
        c_u[i].wait()
        for k in range(2):
            step(n)
            n += 1
        if i == R[-1]:
            for j in range(S - 1):
                aq(j).start()
            fq(-1).start()
    for k in range(lag):
        step(n + k)
    for j in range(S - 1):
        aq(j).wait_recv()
        fq(j).start()
    for c in v_z:
        c.wait()
    acc = vz[0]
    for i in range(1, S):
        acc = acc + vz[i]
    vec_o[...] = acc
    for i in range(S):
        sqk_o[i] = vz[i]
    for j in range(-1, S - 1):
        fq(j).wait_recv()
    full = [jnp.concatenate([agq[k, 0], agq[k, 1]], axis=1) for k in range(S)]
    cols = []
    for c in range(3):
        row = jnp.concatenate([full[k][:, c * hw : (c + 1) * hw] for k in range(S)], axis=1)
        cols.append(row[:, :D])
    qkv_o[...] = jnp.concatenate(cols, axis=1)
    for j in range(-1, S - 1):
        fq(j).wait_send()
    for j in range(S - 1):
        aq(j).wait_send()
    for i in range(n):
        own, raw, oth, _ = pieces[i]
        toward(i, True).wait_send()

        @pl.when(has_outer)
        def _():
            returned(i, True).wait_send()

        local_out(i, raw).wait()
        remote_out(i, raw).wait()


def fourth(S, FS, hp, vec, du, dd, dout, dqkv):
    fl = du.shape[1]
    rows = D // FS
    hl = dd.shape[0]
    hw = hp * HEAD
    w2 = 3 * hw // 2
    dh = D // 2
    n = 5 + 2 * FS
    sds = jax.ShapeDtypeStruct
    outs = [sds((rows, 2 * FS * fl), BF), sds((2 * hl, D), BF), sds((rows, D), BF), sds((rows, 3 * D), BF),
            sds(vec.shape, F32), sds((S,) + vec.shape, F32)]
    dma = lambda k: pltpu.SemaphoreType.DMA((k,))
    F1 = FS - 1
    u, d, o = pltpu.VMEM((FS, rows, fl), BF), pltpu.VMEM((hl, D), BF), pltpu.VMEM((rows, dh), BF)
    v = pltpu.VMEM(vec.shape, F32)
    return pl.pallas_call(
        lambda *refs: fourth_kernel(S, FS, hp, *refs),
        out_shape=outs,
        in_specs=[VM] + [ANY] * 4,
        out_specs=[ANY, ANY, ANY, VM, VM, VM],
        scratch_shapes=[
            u, u, u, d, d, d, o, o, o, o, pltpu.VMEM((F1, rows, dh), BF),
            pltpu.VMEM((rows, w2), BF), pltpu.VMEM((F1, rows, w2), BF), pltpu.VMEM((S, 2, rows, w2), BF),
            v, v, pltpu.VMEM((FS,) + vec.shape, F32), pltpu.VMEM((S,) + vec.shape, F32),
            dma(4), dma(F1), dma(F1), dma(F1), dma(F1), dma(F1), dma(F1), dma(n), dma(n), dma(n), dma(n),
            dma(S), dma(S), dma(S), dma(S), dma(FS + S), dma(FS + S), dma(n), dma(n), dma(n),
        ],
        compiler_params=pltpu.CompilerParams(collective_id=4, has_side_effects=True, vmem_limit_bytes=60 * 2**20),
        name="fourth",
    )(vec, du, dd, dout, dqkv)


def body(S, FS, inputs, segments, w_qkv, w_out, w_upgate, w_down, s_qk, alpha_attn, alpha_mlp, s_up, s_gate, cotangent):
    z = lax.axis_index("seq")
    f = lax.axis_index("fsdp")
    hp = -(-HEADS // S)
    hw = hp * HEAD
    rows = w_qkv.shape[0]
    ff = s_up.shape[0]
    fl = ff // FS
    x = inputs[0]
    seg = segments[0]
    gains = jnp.pad(s_qk, (0, S * hw - D))
    gain = lax.dynamic_slice_in_dim(gains, z * hw, hw).reshape(hp, HEAD)
    hall, wq, wo, wu, raw, qkv, res, mine, attn, mid = first(S, FS, hp, x, seg, w_qkv, w_out, gain, alpha_attn, w_upgate)
    su = lax.dynamic_slice_in_dim(s_up, f * fl, fl).reshape(1, fl)
    sg = lax.dynamic_slice_in_dim(s_gate, f * fl, fl).reshape(1, fl)
    out, g_mid, du, dd, d_mlp, d_su, d_sg = second(S, FS, mid, cotangent[0], w_down, su, sg, alpha_mlp, wu, w_upgate)
    g_x, dout, dqkv, d_attn, d_sqk = third(S, FS, hp, g_mid, x, attn, alpha_attn, mine, seg, gain, wo, wq, qkv, raw, res, hall)

    def row(v):
        return jnp.pad(v.reshape(1, -1), ((0, 0), (0, D - v.size)))

    vec = jnp.concatenate([row(d_mlp), row(d_attn), row(d_sqk), row(d_su), row(d_sg), jnp.zeros((3, D), F32)])
    d_up, d_down, d_o, d_q, tot, parts = fourth(S, FS, hp, vec, du, dd, dout, dqkv)
    sqk = parts[:, 2, :hw].reshape(-1)

    def own(v):
        return lax.dynamic_slice_in_dim(v, f * rows, rows)

    return (
        out[None], g_x[None], d_q.astype(F32), d_o.astype(F32), d_up.astype(F32), d_down.astype(F32),
        own(sqk), own(tot[1]), own(tot[0]), tot[3, :fl], tot[4, :fl],
    )


def solution(mesh):
    S, FS = mesh.shape["seq"], mesh.shape["fsdp"]
    tok = P(("grp", "fsdp"), "seq", None)
    w = P("fsdp", None)
    in_specs = (tok, P(("grp", "fsdp"), None), w, w, w, w, P(), P(), P(), P(), P(), tok)
    out_specs = (tok, tok, w, w, w, w) + (P("fsdp"),) * 5

    def run(*args):
        return body(S, FS, *args)

    return jax.shard_map(run, mesh=mesh, in_specs=in_specs, out_specs=out_specs, check_vma=False)
```

```python
import jax
import jax.numpy as jnp
from jax import lax
from jax.experimental import pallas as pl
from jax.experimental.pallas import tpu as pltpu
from jax.sharding import PartitionSpec as P

D = 1280
HEADS = 20
HEAD = 64

eps_norm = 1e-06
neg_big = -1e30
BF = jnp.bfloat16
F32 = jnp.float32
MESH = pl.DeviceIdType.MESH
ANY = pl.BlockSpec(memory_space=pl.ANY)
VM = pl.BlockSpec(memory_space=pltpu.VMEM)


def inv_rms(value):
    return lax.rsqrt(jnp.mean(value * value, axis=-1, keepdims=True) + eps_norm)


def back(unit, inv, grad):
    return (grad - unit * jnp.mean(grad * unit, axis=-1, keepdims=True)) * inv


def mm(a, b):
    return jnp.dot(a, b, preferred_element_type=F32)


def mm_nt(a, b):
    return lax.dot_general(a, b, (((1,), (1,)), ((), ())), preferred_element_type=F32)


def mm_tn(a, b):
    return lax.dot_general(a, b, (((0,), (0,)), ((), ())), preferred_element_type=F32)


def rcopy(src, dst, ss, rs, dev):
    return pltpu.make_async_remote_copy(src, dst, ss, rs, device_id=dev, device_id_type=MESH)


def greet(peers):
    bar = pltpu.get_barrier_semaphore()
    for p in peers:
        pl.semaphore_signal(bar, inc=1, device_id=p, device_id_type=MESH)
    pl.semaphore_wait(bar, len(peers))


def ds(start, size, mult):
    return pl.ds(pl.multiple_of(start, mult), size)


def visible(seg_col, seg_row, q0, k0, nq, nk):
    qi = q0 + lax.broadcasted_iota(jnp.int32, (nq, nk), 0)
    ki = k0 + lax.broadcasted_iota(jnp.int32, (nq, nk), 1)
    return (ki <= qi) & ((seg_row == 0) | (seg_row == seg_col))


def add_into(dst, src, chunk, out=None):
    out = dst if out is None else out

    def one(i, carry):
        at = ds(i * chunk, chunk, 16)
        out[at] = (dst[at].astype(F32) + src[at].astype(F32)).astype(dst.dtype)
        return carry

    lax.fori_loop(0, src.shape[0] // chunk, one, 0)


def attn_bias(S, tok, half, bias, segc, segr):
    for qb in range(S):
        q0 = qb * tok
        k0 = q0 if q0 < half else half
        nk = q0 + tok - k0
        ok = visible(segc[q0 : q0 + tok], segr[:, k0 : k0 + nk], q0, k0, tok, nk)
        bias[qb, :, :nk] = jnp.where(ok, 0.0, neg_big).astype(BF)


def first_kernel(S, FS, hp, x_ref, segc, segr, wqkv, wout, gain, alpha, wup,
                 hall_o, wq_o, wo_o, wu_o, raw_o, qkv_o, res_o, mine_o, attn_o, mid_o,
                 hall, wq, wo, raw, qkv, res, bias, oh, mixs, mine, recv,
                 s_up, r_up, s_dn, r_dn, s_wq, r_wq, s_wo, r_wo, s_wu, r_wu, f_wq, f_wo, f_wu,
                 g_wq, g_wo, g_wu, s_mx, r_mx, out_sem):
    g, z, f = lax.axis_index("grp"), lax.axis_index("seq"), lax.axis_index("fsdp")
    tok = x_ref.shape[0]
    rows = wqkv.shape[0]
    hr = rows // 2
    hw = hp * HEAD
    ff = wup.shape[1] // 2
    fl = ff // FS
    total = S * tok
    half = total // 2
    fpeers = [lax.rem(f + i, FS) for i in range(1, FS)]
    zpeers = [lax.rem(z + i, S) for i in range(1, S)]
    greet([(g, z, p) for p in fpeers] + [(g, p, f) for p in zpeers] + [(1 - g, z, f)])

    x = x_ref[...].astype(F32)
    hall[z] = (x * inv_rms(x)).astype(BF)

    def up(t, b):
        return rcopy(hall.at[b], hall.at[b], s_up.at[t], r_up.at[t], (g, lax.rem(z + 1, S), f))

    def down(t, b):
        return rcopy(hall.at[b], hall.at[b], s_dn.at[t], r_dn.at[t], (g, lax.rem(z + S - 1, S), f))

    @pl.when(z + 1 < S)
    def _():
        up(0, z).start()

    @pl.when(z > 0)
    def _():
        down(0, z).start()

    for k in range(S):
        lo, hi = k * hw, min((k + 1) * hw, D)

        @pl.when(z == k)
        def _():
            parts = []
            for c in range(3):
                if hi > lo:
                    parts.append(wqkv[:, c * D + lo : c * D + hi])
                if hi - lo < hw:
                    parts.append(jnp.zeros((rows, hw - max(hi - lo, 0)), BF))
            wq[ds(f * rows, rows, 16)] = jnp.concatenate(parts, axis=1)

    def wq_half(src, gg):
        return wq.at[ds(src * rows + gg * hr, hr, 16)]

    def wo_half(src, gg):
        return wo.at[ds(src * rows + gg * hr, hr, 16)]

    c_wq = [rcopy(wq_half(f, g), wq_half(f, g), s_wq.at[i], r_wq.at[i], (g, z, p)) for i, p in enumerate(fpeers)]
    for c in c_wq:
        c.start()
    attn_bias(S, tok, half, bias, segc, segr)
    wo[ds(f * rows, rows, 16)] = wout[...]
    qkv[2, :, :, HEAD:] = jnp.where(lax.broadcasted_iota(jnp.int32, (hp, total, HEAD), 2) == 0, 1.0, 0.0).astype(BF)

    bpeers = [lax.rem(f + FS - i, FS) for i in range(1, FS)]
    partner = (1 - g, z, f)
    fw_wq = [rcopy(wq_half(p, g), wq_half(p, g), f_wq.at[i], g_wq.at[i], partner) for i, p in enumerate(bpeers)]
    for i in range(FS - 1):
        c_wq[i].wait_recv()
        fw_wq[i].start()
    c_wo = [rcopy(wo_half(f, g), wo_half(f, g), s_wo.at[i], r_wo.at[i], (g, z, p)) for i, p in enumerate(fpeers)]
    for c in c_wo:
        c.start()

    def wu_cp(i, p):
        return rcopy(wup.at[:, ds(g * ff + p * fl, fl, 128)], wu_o.at[g, f], s_wu.at[i], r_wu.at[i], (g, z, p))

    c_wu = [wu_cp(i, p) for i, p in enumerate(fpeers)]
    for c in c_wu:
        c.start()
    for i in range(FS - 1):
        fw_wq[i].wait_recv()

    def step(i, carry):
        t = lax.div(i - 1, 2)
        is_up = lax.rem(i, 2) == 1
        b = jnp.where(i == 0, z, jnp.where(is_up, z - 1 - t, z + 1 + t))

        @pl.when((b >= 0) & (b < S))
        def _():
            @pl.when((i > 0) & is_up)
            def _():
                up(t, b).wait_recv()

                @pl.when(z + 1 < S)
                def _():
                    up(t + 1, b).start()

            @pl.when((i > 0) & jnp.logical_not(is_up))
            def _():
                down(t, b).wait_recv()

                @pl.when(z > 0)
                def _():
                    down(t + 1, b).start()

            acc = mm(hall[b], wq[...])
            at = ds(b * tok, tok, 16)
            for j in range(hp):
                for c in range(2):
                    v = acc[:, c * hw + j * HEAD : c * hw + (j + 1) * HEAD]
                    raw[j, at, c * HEAD : (c + 1) * HEAD] = v
                    u = v * inv_rms(v) * gain[j : j + 1]
                    qkv[c, j, at, :HEAD] = u.astype(BF)
                qkv[2, j, at, :HEAD] = acc[:, 2 * hw + j * HEAD : 2 * hw + (j + 1) * HEAD].astype(BF)

        return carry

    lax.fori_loop(0, 2 * S - 1, step, 0)
    outs = [
        pltpu.make_async_copy(hall, hall_o, out_sem.at[0]),
        pltpu.make_async_copy(wq, wq_o, out_sem.at[1]),
        pltpu.make_async_copy(raw, raw_o, out_sem.at[2]),
        pltpu.make_async_copy(qkv, qkv_o, out_sem.at[3]),
    ]
    for c in outs:
        c.start()

    def mx(qb):
        return rcopy(mixs.at[qb], recv.at[z], s_mx.at[qb], r_mx.at[z], (g, qb, f))

    for qb in reversed(range(S)):
        q0 = qb * tok
        n = q0 + tok
        k0 = q0 if q0 < half else half

        def head(j, carry):
            q = qkv[0, j, q0:n, :HEAD] * jnp.asarray(HEAD**-0.5, BF)
            s = mm_nt(q, qkv[1, j, :n, :HEAD])
            tail = s[:, k0:] + bias[qb, :, : n - k0].astype(F32)
            e = jnp.exp(jnp.concatenate([s[:, :k0], tail], axis=1) if k0 else tail)
            o = mm(e.astype(BF), qkv[2, j, :n])
            rinv = 1.0 / o[:, HEAD : HEAD + 1]
            o = o[:, :HEAD] * rinv
            res[j, q0:n, :HEAD] = o
            res[j, q0:n, HEAD:] = jnp.broadcast_to(rinv, (tok, HEAD))
            oh[j] = o.astype(BF)
            return carry

        lax.fori_loop(0, hp, head, 0)
        block = jnp.concatenate([oh[j] for j in range(hp)], axis=1)
        mixs[qb] = block

        @pl.when(z != qb)
        def _():
            mx(qb).start()

        @pl.when(z == qb)
        def _():
            recv[qb] = block

        if qb == S - 1:
            fw_wo = [rcopy(wo_half(p, g), wo_half(p, g), f_wo.at[i], g_wo.at[i], partner) for i, p in enumerate(bpeers)]
            for i in range(FS - 1):
                c_wo[i].wait_recv()
                fw_wo[i].start()

    fw_wu = [rcopy(wu_o.at[g, p], wu_o.at[g, p], f_wu.at[i], g_wu.at[i], partner) for i, p in enumerate(bpeers)]
    for i in range(FS - 1):
        c_wu[i].wait_recv()
        fw_wu[i].start()
    for i in range(FS - 1):
        fw_wo[i].wait_recv()
    outs2 = [pltpu.make_async_copy(wo, wo_o, out_sem.at[4]), pltpu.make_async_copy(res, res_o, out_sem.at[5])]
    for c in outs2:
        c.start()
    for k in range(S):
        @pl.when(z != k)
        def _():
            rcopy(mixs.at[0], recv.at[k], s_mx.at[0], r_mx.at[k], (g, k, f)).wait_recv()

    mine[...] = jnp.concatenate([recv[k] for k in range(S)], axis=1)[:, :D]
    attn = mm(mine[...], wo[...])
    attn_o[...] = attn
    mine_o[...] = mine[...]
    x = x_ref[...].astype(F32)
    h = x * inv_rms(x)
    n_ = h + alpha[...] * (attn * inv_rms(attn) - h)
    mid_o[...] = n_ * inv_rms(n_)

    for t in range(S - 1):
        @pl.when((z + 1 < S) & (z - t >= 0))
        def _():
            up(t, z).wait_send()

        @pl.when((z > 0) & (z + t < S))
        def _():
            down(t, z).wait_send()

    for i in range(FS - 1):
        c_wq[i].wait_send()
        c_wo[i].wait_send()
        c_wu[i].wait_send()
        fw_wq[i].wait_send()
        fw_wo[i].wait_send()
        fw_wu[i].wait()
    for k in range(S):
        @pl.when(z != k)
        def _():
            mx(k).wait_send()
    for c in outs + outs2:
        c.wait()


def first(S, FS, hp, x, seg, wqkv, wout, gain, alpha, wup):
    tok, total = x.shape[0], seg.shape[0]
    rows = wqkv.shape[0]
    hw = hp * HEAD
    fl = wup.shape[1] // 2 // FS
    sds = jax.ShapeDtypeStruct
    outs = [
        sds((S, tok, D), BF), sds((D, 3 * hw), BF), sds((D, D), BF), sds((2, FS, rows, fl), BF),
        sds((hp, total, 2 * HEAD), F32), sds((3, hp, total, 2 * HEAD), BF), sds((hp, total, 2 * HEAD), F32),
        sds((tok, D), BF), sds((tok, D), F32), sds((tok, D), F32),
    ]
    dma = lambda n: pltpu.SemaphoreType.DMA((n,))
    F1 = FS - 1
    return pl.pallas_call(
        lambda *refs: first_kernel(S, FS, hp, *refs),
        out_shape=outs,
        in_specs=[VM] * 7 + [ANY],
        out_specs=[ANY] * 7 + [VM] * 3,
        scratch_shapes=[
            pltpu.VMEM((S, tok, D), BF), pltpu.VMEM((D, 3 * hw), BF), pltpu.VMEM((D, D), BF),
            pltpu.VMEM((hp, total, 2 * HEAD), F32), pltpu.VMEM((3, hp, total, 2 * HEAD), BF),
            pltpu.VMEM((hp, total, 2 * HEAD), F32), pltpu.VMEM((S, tok, total // 2), BF),
            pltpu.VMEM((hp, tok, HEAD), BF), pltpu.VMEM((S, tok, hw), BF), pltpu.VMEM((tok, D), BF),
            pltpu.VMEM((S, tok, hw), BF),
            dma(S), dma(S), dma(S), dma(S), dma(F1), dma(F1), dma(F1), dma(F1), dma(F1), dma(F1),
            dma(F1), dma(F1), dma(F1), dma(F1), dma(F1), dma(F1), dma(S), dma(S), dma(6),
        ],
        compiler_params=pltpu.CompilerParams(collective_id=1, has_side_effects=True, vmem_limit_bytes=60 * 2**20),
        name="first",
    )(x, seg.reshape(total, 1), seg.reshape(1, total), wqkv, wout, gain, alpha.reshape(1, D), wup)


def second_kernel(S, FS, NC, mid, cot, wd, su, sg, alpha, wu_i, wup,
                  out_o, gmid_o, du_o, dd_o, dal_o, dsu_o, dsg_o,
                  wu, mida, up, gate, hid, ps, pr, rl, gma, gu, dup, ddn, lu, ld,
                  s_a, r_a, s_b, r_b, s_c, r_c, s_d, r_d, w_sem, s_x, r_x, out_sem):
    g, z, f = lax.axis_index("grp"), lax.axis_index("seq"), lax.axis_index("fsdp")
    tok = mid.shape[0]
    ct = tok // NC
    hc = ct // 2
    fl = wd.shape[0]
    ff = wup.shape[1] // 2
    rows = wup.shape[0]
    hl = fl // 2
    nt = 256 if fl % 256 == 0 else 128
    M = FS * ct
    relay = FS == 4
    peers = [lax.rem(f + i, FS) for i in range(1, FS)]
    partner = (1 - g, z, f)
    greet([(g, z, p) for p in peers] + [partner])
    R = range(FS - 1)
    A, B = pl.ds(0, hc), pl.ds(hc, hc)
    if relay:
        fx, fy, fd = f + 1 - 2 * lax.rem(f, 2), lax.rem(f + 2, 4), 3 - f
        dx, dy = (g, z, fx), (g, z, fy)

    def direct(buf, ss, rs, c, i):
        return rcopy(buf.at[c, f], buf.at[c, f], ss.at[c, i], rs.at[c, i], (g, z, peers[i]))

    def gcopy(buf, ss, rs, c, k):
        src, half, dev = ((f, A, dx), (f, B, dx), (f, B, dy), (f, A, dy), (fx, A, dy), (fy, B, dx))[k]
        view = buf.at[c, src, half]
        return rcopy(view, view, ss.at[c, k], rs.at[c, k], dev)

    def g_issue(buf, ss, rs, c):
        if relay:
            for k in (0, 2, 1, 3):
                gcopy(buf, ss, rs, c, k).start()
        else:
            for i in R:
                direct(buf, ss, rs, c, i).start()

    def g_relay(buf, ss, rs, c):
        if relay:
            for k in (0, 2):
                gcopy(buf, ss, rs, c, k).wait_recv()
                gcopy(buf, ss, rs, c, 4 if k == 0 else 5).start()

    def g_wait(buf, ss, rs, c):
        if relay:
            for k in (1, 3, 4, 5):
                gcopy(buf, ss, rs, c, k).wait_recv()
        else:
            for i in R:
                direct(buf, ss, rs, c, i).wait_recv()

    def g_sent(buf, ss, rs, c):
        if relay:
            for k in range(6):
                gcopy(buf, ss, rs, c, k).wait_send()
        else:
            for i in R:
                direct(buf, ss, rs, c, i).wait_send()

    def scopy(ss, rs, c, k):
        src, dst, dev = (
            (ps.at[c, fd, A], rl.at[c, 0], dx),
            (ps.at[c, fd, B], rl.at[c, 1], dy),
            (ps.at[c, fx, A], pr.at[c, 0, A], dx),
            (ps.at[c, fy, B], pr.at[c, 1, B], dy),
            (ps.at[c, fy, A], pr.at[c, 1, A], dy),
            (ps.at[c, fx, B], pr.at[c, 0, B], dx),
        )[k]
        return rcopy(src, dst, ss.at[c, k], rs.at[c, k], dev)

    def sdirect(ss, rs, c, i):
        return rcopy(ps.at[c, peers[i]], pr.at[c, i], ss.at[c, i], rs.at[c, i], (g, z, peers[i]))

    def s_issue(ss, rs, c):
        if relay:
            for k in range(4):
                scopy(ss, rs, c, k).start()
        else:
            for i in R:
                sdirect(ss, rs, c, i).start()

    def s_relay(ss, rs, c):
        if relay:
            for k, tgt, half in ((0, fy, A), (1, fx, B)):
                scopy(ss, rs, c, k).wait_recv()
                ps[c, tgt, half] = (ps[c, tgt, half].astype(F32) + rl[c, k].astype(F32)).astype(BF)
                scopy(ss, rs, c, 4 + k).start()

    def s_total(ss, rs, c):
        if relay:
            for k in range(2, 6):
                scopy(ss, rs, c, k).wait_recv()
        else:
            for i in R:
                sdirect(ss, rs, c, i).wait_recv()
        acc = ps[c, f].astype(F32)
        for i in range(2 if relay else FS - 1):
            acc = acc + pr[c, i].astype(F32)
        return acc

    def s_sent(ss, rs, c):
        if relay:
            for k in range(6):
                scopy(ss, rs, c, k).wait_send()
        else:
            for i in R:
                sdirect(ss, rs, c, i).wait_send()

    for c in range(NC):
        mida[c, f] = mid[c * ct : (c + 1) * ct].astype(BF)
        g_issue(mida, s_a, r_a, c)
        if c == 0:
            loads = []
            for k in range(2):
                loads.append(pltpu.make_async_copy(wup.at[:, ds(k * ff + f * fl, fl, 128)], wu.at[k, ds(f * rows, rows, 16)], w_sem.at[k, 0]))
                for i in R:
                    loads.append(pltpu.make_async_copy(wu_i.at[k, peers[i]], wu.at[k, ds(peers[i] * rows, rows, 16)], w_sem.at[k, i + 1]))
            for ld_c in loads:
                ld_c.start()
            dsu_o[...] = jnp.zeros_like(dsu_o)
            dsg_o[...] = jnp.zeros_like(dsg_o)
            dal_o[...] = jnp.zeros_like(dal_o)
        g_relay(mida, s_a, r_a, c)
    for ld_c in loads:
        ld_c.wait()

    for c in range(NC):
        g_wait(mida, s_a, r_a, c)

        def fwd(t, carry):
            cols = ds(t * nt, nt, 128)
            a_in = mida[c].reshape(M, D)
            u = mm(a_in, wu[0, :, cols])
            gt = mm(a_in, wu[1, :, cols])
            up[c, :, cols] = u
            gate[c, :, cols] = gt
            a = gt * sg[:, cols]
            hid[c, :, cols] = (u * su[:, cols] * (a * jax.nn.sigmoid(a))).astype(BF)
            return carry

        lax.fori_loop(0, fl // nt, fwd, 0)
        if c:
            s_relay(s_b, r_b, c - 1)

        def proj(t, carry):
            cols = ds(t * 256, 256, 128)
            ps[c, :, :, cols] = mm(hid[c], wd[:, cols]).astype(BF).reshape(FS, ct, 256)
            return carry

        lax.fori_loop(0, D // 256, proj, 0)
        s_issue(s_b, r_b, c)
    s_relay(s_b, r_b, NC - 1)

    for c in range(NC):
        at = slice(c * ct, (c + 1) * ct)
        mlp = s_total(s_b, r_b, c)
        al = alpha[...]
        md = mid[at]
        inv_m = inv_rms(mlp)
        um = mlp * inv_m
        dif = um - md
        m = md + al * dif
        inv_o = inv_rms(m)
        o = m * inv_o
        out_o[at] = o.astype(BF)
        g_m = back(o, inv_o, cot[at].astype(F32))
        dal_o[...] += jnp.sum(g_m * dif, axis=0, keepdims=True)
        gmid_o[at] = (1 - al) * g_m
        gma[c, f] = back(um, inv_m, al * g_m).astype(BF)
        g_issue(gma, s_c, r_c, c)
        g_relay(gma, s_c, r_c, c)

    for c in range(NC):
        g_wait(gma, s_c, r_c, c)

        def bwd(t, carry):
            cols = ds(t * nt, nt, 128)
            gh = mm_nt(gma[c].reshape(M, D), wd[cols, :])
            u = up[c, :, cols]
            gt = gate[c, :, cols]
            sgc = sg[:, cols]
            suc = su[:, cols]
            a = gt * sgc
            sig = jax.nn.sigmoid(a)
            gs = gh * (a * sig)
            gu[0, c, :, cols] = (gs * suc).astype(BF)
            dsu_o[:, cols] += jnp.sum(u * gs, axis=0, keepdims=True)
            g_a = gh * u * suc * (sig * (1 + a * (1 - sig)))
            gu[1, c, :, cols] = (g_a * sgc).astype(BF)
            dsg_o[:, cols] += jnp.sum(gt * g_a, axis=0, keepdims=True)
            return carry

        lax.fori_loop(0, fl // nt, bwd, 0)
        if c:
            s_relay(s_d, r_d, c - 1)
        s_sent(s_b, r_b, c)

        def bproj(t, carry):
            cols = ds(t * 256, 256, 128)
            v = mm_nt(gu[0, c], wu[0, cols, :]) + mm_nt(gu[1, c], wu[1, cols, :])
            ps[c, :, :, cols] = v.astype(BF).reshape(FS, ct, 256)
            return carry

        lax.fori_loop(0, D // 256, bproj, 0)
        s_issue(s_d, r_d, c)

    def dwd(t, carry):
        cols = ds(t * nt, nt, 128)
        ddn[cols, :] = mm_tn(hid[:, :, cols].reshape(NC * M, nt), gma[...].reshape(NC * M, D)).astype(BF)
        return carry

    lax.fori_loop(0, fl // nt, dwd, 0)
    s_relay(s_d, r_d, NC - 1)
    x_d = rcopy(ddn.at[ds((1 - g) * hl, hl, 16)], ld, s_x.at[0], r_x.at[0], partner)
    x_d.start()

    def dwu(k):
        def one(t, carry):
            cols = ds(t * 256, 256, 128)
            dup[k, cols, :] = mm_tn(mida[:, :, :, cols].reshape(NC * M, 256), gu[k].reshape(NC * M, fl)).astype(BF)
            return carry

        lax.fori_loop(0, D // 256, one, 0)

    dwu(1 - g)
    x_u = rcopy(dup.at[1 - g], lu, s_x.at[1], r_x.at[1], partner)
    x_u.start()
    dwu(g)
    mine = ds(g * hl, hl, 16)
    x_d.wait_recv()
    add_into(ddn.at[mine], ld, 64)
    o_d = pltpu.make_async_copy(ddn.at[mine], dd_o, out_sem.at[0])
    o_d.start()
    x_u.wait_recv()
    add_into(dup.at[g], lu, 64)
    o_u = pltpu.make_async_copy(dup.at[g], du_o, out_sem.at[1])
    o_u.start()

    for c in range(NC):
        at = slice(c * ct, (c + 1) * ct)
        gmid_o[at] = gmid_o[at] + s_total(s_d, r_d, c)
    for c in range(NC):
        g_sent(mida, s_a, r_a, c)
        g_sent(gma, s_c, r_c, c)
        s_sent(s_d, r_d, c)
    x_d.wait_send()
    x_u.wait_send()
    o_d.wait()
    o_u.wait()


def second(S, FS, mid, cot, wd, su, sg, alpha, wu, wup):
    NC = 2
    tok = mid.shape[0]
    ct = tok // NC
    fl = wd.shape[0]
    M = FS * ct
    sds = jax.ShapeDtypeStruct
    outs = [sds((tok, D), BF), sds((tok, D), F32), sds((D, fl), BF), sds((fl // 2, D), BF),
            sds((1, D), F32), sds((1, fl), F32), sds((1, fl), F32)]
    dma = pltpu.SemaphoreType.DMA
    F1 = FS - 1
    return pl.pallas_call(
        lambda *refs: second_kernel(S, FS, NC, *refs),
        out_shape=outs,
        in_specs=[VM] * 6 + [ANY] * 2,
        out_specs=[VM, VM, ANY, ANY, VM, VM, VM],
        scratch_shapes=[
            pltpu.VMEM((2, D, fl), BF), pltpu.VMEM((NC, FS, ct, D), BF), pltpu.VMEM((NC, M, fl), F32),
            pltpu.VMEM((NC, M, fl), F32), pltpu.VMEM((NC, M, fl), BF), pltpu.VMEM((NC, FS, ct, D), BF),
            pltpu.VMEM((NC, 2 if FS == 4 else F1, ct, D), BF), pltpu.VMEM((NC, 2, ct // 2, D), BF),
            pltpu.VMEM((NC, FS, ct, D), BF), pltpu.VMEM((2, NC, M, fl), BF),
            pltpu.VMEM((2, D, fl), BF), pltpu.VMEM((fl, D), BF), pltpu.VMEM((D, fl), BF), pltpu.VMEM((fl // 2, D), BF),
        ] + [dma((NC, max(F1, 6)))] * 8 + [dma((2, FS)), dma((2,)), dma((2,)), dma((2,))],
        compiler_params=pltpu.CompilerParams(collective_id=2, has_side_effects=True, vmem_limit_bytes=63 * 2**20),
        name="second",
    )(mid, cot, wd, su, sg, alpha.reshape(1, D), wu, wup)


def make_chain(S, pieces, outs, sems):
    s_in, r_raw, r_oth, s_ret, o_sem, s_o, r_o = sems
    g, z, f = lax.axis_index("grp"), lax.axis_index("seq"), lax.axis_index("fsdp")
    partner = (1 - g, z, f)
    lower = z < S // 2
    inner = jnp.where(lower, z + 1, z - 1)
    mid = (z == S // 2 - 1) | (z == S // 2)
    has_outer = (z > 0) & (z < S - 1)
    outer = jnp.where(has_outer, jnp.where(lower, z - 1, z + 1), inner)
    rest = jnp.logical_not(mid)

    def toward(i, to_mid):
        own, raw, oth, _ = pieces[i]
        if to_mid:
            return rcopy(own, oth, s_in.at[i], r_oth.at[i], (g, inner, f))
        return rcopy(own, raw, s_in.at[i], r_raw.at[i], (g, inner, f))

    def returned(i, from_mid):
        own, raw, oth, _ = pieces[i]
        return rcopy(raw if from_mid else oth, oth, s_ret.at[i], r_oth.at[i], (g, outer, f))

    def local_out(i, src):
        return pltpu.make_async_copy(src, pieces[i][3](outs), o_sem.at[i])

    def remote_out(i, src):
        return rcopy(src, pieces[i][3](outs), s_o.at[i], r_o.at[i], partner)

    def send(i):
        @pl.when(mid)
        def _():
            toward(i, True).start()

        @pl.when(rest)
        def _():
            toward(i, False).start()

    def launch(i):
        @pl.when(jnp.logical_not(has_outer))
        def _():
            send(i)

    def go_in(i):
        own, raw, oth, _ = pieces[i]

        @pl.when(has_outer)
        def _():
            rcopy(own, raw, s_in.at[i], r_raw.at[i], (g, outer, f)).wait_recv()
            add_into(own, raw, 80)
            send(i)

    def finish(i, src, from_mid):
        @pl.when(has_outer)
        def _():
            returned(i, from_mid).start()

        local_out(i, src).start()
        remote_out(i, src).start()

    def arrived(i):
        own, raw, oth, _ = pieces[i]
        rcopy(own, oth, s_in.at[i], r_oth.at[i], (g, inner, f)).wait_recv()

    def step(i, lag=5):
        if i < len(pieces):
            go_in(i)
        if 1 <= i <= len(pieces):
            @pl.when(mid)
            def _():
                own, raw, oth, _ = pieces[i - 1]
                arrived(i - 1)
                add_into(own, oth, 80, raw)
                finish(i - 1, raw, True)
        if lag <= i < len(pieces) + lag:
            @pl.when(rest)
            def _():
                arrived(i - lag)
                finish(i - lag, pieces[i - lag][2], False)

    def drain():
        for i in range(len(pieces)):
            toward(i, True).wait_send()

            @pl.when(has_outer)
            def _():
                returned(i, True).wait_send()

            local_out(i, pieces[i][1]).wait()
            remote_out(i, pieces[i][1]).wait()

    return launch, step, drain


def cuts(size, parts, unit):
    step = size // unit
    return [(a * step, (b - a) * step) for a, b in zip(parts[:-1], parts[1:])]


def third_kernel(S, FS, hp, gmid, x_ref, attn, alpha, mine, segc, segr, gain, wo, wq_i, qkv_i, raw_i, res_i, hall_i, dd_i,
                 gh1, ps_o, dout_o, dqkv_o, dn_o, dal_o, dsq_o,
                 wq, qkv, raw, res, hall, ga, gsend, gxr, bias, hx, gqh, dkv, gq, ps, dout, dqk, lo, lq, own_d, raw_d, oth_d,
                 ld_sem, h_sem, s_gx, r_gx, s_p, s_x, r_x, out_sem, *chain_sems):
    g, z, f = lax.axis_index("grp"), lax.axis_index("seq"), lax.axis_index("fsdp")
    tok = x_ref.shape[0]
    hw = hp * HEAD
    wide = S * hw
    total = S * tok
    half = total // 2
    w2 = 3 * hw // 2
    dh = D // 2
    partner = (1 - g, z, f)
    greet([(g, lax.rem(z + i, S), f) for i in range(1, S)] + [partner])
    loads = [pltpu.make_async_copy(a, b, ld_sem.at[i]) for i, (a, b) in enumerate(
        [(qkv_i, qkv), (raw_i, raw), (res_i, res), (wq_i, wq)])]
    for c in loads:
        c.start()

    hl = own_d.shape[0]
    dd_c = pltpu.make_async_copy(dd_i.at[pl.ds(0, hl)], own_d, h_sem.at[2])
    dd_c.start()
    pieces = []
    for lo_r, n_r in cuts(hl, (0, 1, 2, 4) if hl % 64 == 0 else (0, 2, 4), 4):
        pieces.append((own_d.at[pl.ds(lo_r, n_r)], raw_d.at[pl.ds(lo_r, n_r)], oth_d.at[pl.ds(lo_r, n_r)],
                       lambda o, lo_r=lo_r, n_r=n_r: o.at[g, pl.ds(lo_r, n_r)]))
    launch, step, drain = make_chain(S, pieces, dn_o, chain_sems)
    n_p = len(pieces)

    def h_tile(t):
        return pltpu.make_async_copy(hall_i.at[:, :, pl.ds(t * 256, 256)], hall.at[t % 2], h_sem.at[t % 2])

    h_tile(0).start()
    h_tile(1).start()
    dd_c.wait()
    launch(0)
    dal_o[...] = jnp.zeros_like(dal_o)
    dsq_o[...] = jnp.zeros_like(dsq_o)
    cr = tok // 4

    def pre(i, carry):
        at = ds(i * cr, cr, 16)
        x = x_ref[at].astype(F32)
        h = x * inv_rms(x)
        av = attn[at]
        inv_a = inv_rms(av)
        ua = av * inv_a
        al = alpha[...]
        dif = ua - h
        n_ = h + al * dif
        inv_n = inv_rms(n_)
        g_n = back(n_ * inv_n, inv_n, gmid[at])
        dal_o[...] += jnp.sum(g_n * dif, axis=0, keepdims=True)
        gh1[at] = (1 - al) * g_n
        ga[at] = back(ua, inv_a, al * g_n).astype(BF)
        return carry

    lax.fori_loop(0, 4, pre, 0)
    gmix = mm_nt(ga[...], wo[...]).astype(BF)
    if wide > D:
        gmix = jnp.concatenate([gmix, jnp.zeros((tok, wide - D), BF)], axis=1)
    for k in range(S):
        gsend[k] = gmix[:, k * hw : (k + 1) * hw]

    def gx(k):
        return rcopy(gsend.at[k], gxr.at[z], s_gx.at[k], r_gx.at[z], (g, k, f))

    for k in range(S):
        @pl.when(z != k)
        def _():
            gx(k).start()

        @pl.when(z == k)
        def _():
            gxr[k] = gsend[k]


    def dwo(t, carry):
        cols = ds(t * 256, 256, 128)
        v = mm_tn(mine[:, cols], ga[...]).astype(BF)
        dout[0, cols, :] = v[:, :dh]
        dout[1, cols, :] = v[:, dh:]
        return carry

    lax.fori_loop(0, D // 256, dwo, 0)
    x_o = rcopy(dout.at[1 - g], lo, s_x.at[0], r_x.at[0], partner)
    x_o.start()
    attn_bias(S, tok, half, bias, segc, segr)
    for c in loads:
        c.wait()
    done = 0

    def part(k):
        return pltpu.make_async_copy(ps.at[k], ps_o.at[k], s_p.at[k])

    for qb in reversed(range(S)):
        q0 = qb * tok
        n = q0 + tok
        k0 = q0 if q0 < half else half

        @pl.when(z != qb)
        def _():
            rcopy(gsend.at[0], gxr.at[qb], s_gx.at[0], r_gx.at[qb], (g, qb, f)).wait_recv()

        if qb == S - 1:
            for i in range(1, n_p):
                launch(i)

        for j in range(hp):
            hx[j] = gxr[qb, :, j * HEAD : (j + 1) * HEAD]

        def head(j, carry):
            q = qkv[0, j, q0:n, :HEAD] * jnp.asarray(HEAD**-0.5, BF)
            keys = qkv[1, j, :n, :HEAD]
            gv = hx[j]
            rinv = res[j, q0:n, HEAD : HEAD + 1]
            delta = jnp.sum(gv.astype(F32) * res[j, q0:n, :HEAD], axis=-1, keepdims=True)
            s = mm_nt(q, keys)
            tail = s[:, k0:] + bias[qb, :, : n - k0].astype(F32)
            p = jnp.exp(jnp.concatenate([s[:, :k0], tail], axis=1) if k0 else tail) * rinv
            dp = mm_nt(gv, qkv[2, j, :n, :HEAD])
            dsb = (p * (dp - delta)).astype(BF)
            dq = mm(dsb, keys) * HEAD**-0.5
            dk = mm_tn(dsb, q)
            dv = mm_tn(p.astype(BF), gv)
            if qb < S - 1:
                dk = dk + dkv[j, :n, :HEAD]
                dv = dv + dkv[j, :n, HEAD:]
            if qb:
                dkv[j, :q0, :HEAD] = dk[:q0]
                dkv[j, :q0, HEAD:] = dv[:q0]
            gj = gain[pl.ds(j, 1), :]
            for c, d in ((0, dq), (1, dk[q0:])):
                v = raw[j, q0:n, c * HEAD : (c + 1) * HEAD]
                inv = inv_rms(v)
                u = v * inv
                dsq_o[pl.ds(j, 1), :] += jnp.sum(d * u, axis=0, keepdims=True)
                gqh[c, j] = back(u, inv, d * gj).astype(BF)
            gqh[2, j] = dv[q0:].astype(BF)
            return carry

        lax.fori_loop(0, hp, head, 0)
        gq[qb] = jnp.concatenate([gqh[c, j] for c in range(3) for j in range(hp)], axis=1)
        ps[qb] = mm_nt(gq[qb], wq[...]).astype(BF)

        part(qb).start()
        if done < n_p + 5:
            step(done)
            done += 1

    for t in range(D // 256):
        h_tile(t).wait()
        v = mm_tn(hall[t % 2].reshape(total, 256), gq[...].reshape(total, 3 * hw)).astype(BF)
        dqk[0, t * 256 : (t + 1) * 256, :] = v[:, :w2]
        dqk[1, t * 256 : (t + 1) * 256, :] = v[:, w2:]
        if t + 2 < D // 256:
            h_tile(t + 2).start()
    x_q = rcopy(dqk.at[1 - g], lq, s_x.at[1], r_x.at[1], partner)
    x_q.start()
    x_o.wait_recv()
    add_into(dout.at[g], lo, 128)
    o_o = pltpu.make_async_copy(dout.at[g], dout_o, out_sem.at[0])
    o_o.start()
    while done < n_p + 5:
        step(done)
        done += 1
    x_q.wait_recv()
    add_into(dqk.at[g], lq, 128)
    o_q = pltpu.make_async_copy(dqk.at[g], dqkv_o, out_sem.at[1])
    o_q.start()

    for k in range(S):
        @pl.when(z != k)
        def _():
            gx(k).wait_send()

        part(k).wait()
    x_o.wait_send()
    x_q.wait_send()
    o_o.wait()
    o_q.wait()
    drain()


def third(S, FS, hp, gmid, x, attn, alpha, mine, seg, gain, wo, wq, qkv, raw, res, hall, dd):
    tok, total = x.shape[0], seg.shape[0]
    hw = hp * HEAD
    sds = jax.ShapeDtypeStruct
    outs = [sds((tok, D), F32), sds((S, tok, D), BF), sds((D, D // 2), BF), sds((D, 3 * hw // 2), BF), sds((2, dd.shape[0] // 2, D), BF),
            sds((1, D), F32), sds((hp, HEAD), F32)]
    dma = lambda n: pltpu.SemaphoreType.DMA((n,))
    hd = pltpu.VMEM((dd.shape[0] // 2, D), BF)
    return pl.pallas_call(
        lambda *refs: third_kernel(S, FS, hp, *refs),
        out_shape=outs,
        in_specs=[VM] * 9 + [ANY] * 6,
        out_specs=[VM, ANY, ANY, ANY, ANY, VM, VM],
        scratch_shapes=[
            pltpu.VMEM((D, 3 * hw), BF), pltpu.VMEM((3, hp, total, 2 * HEAD), BF), pltpu.VMEM((hp, total, 2 * HEAD), F32),
            pltpu.VMEM((hp, total, 2 * HEAD), F32), pltpu.VMEM((2, S, tok, 256), BF),
            pltpu.VMEM((tok, D), BF), pltpu.VMEM((S, tok, hw), BF), pltpu.VMEM((S, tok, hw), BF),
            pltpu.VMEM((S, tok, total // 2), BF), pltpu.VMEM((hp, tok, HEAD), BF), pltpu.VMEM((3, hp, tok, HEAD), BF),
            pltpu.VMEM((hp, total, 2 * HEAD), F32), pltpu.VMEM((S, tok, 3 * hw), BF), pltpu.VMEM((S, tok, D), BF),
            pltpu.VMEM((2, D, D // 2), BF), pltpu.VMEM((2, D, 3 * hw // 2), BF),
            pltpu.VMEM((D, D // 2), BF), pltpu.VMEM((D, 3 * hw // 2), BF),
            hd, hd, hd,
            dma(4), dma(3), dma(S), dma(S), dma(S), dma(2), dma(2), dma(2),
        ] + [dma(5)] * 7,
        compiler_params=pltpu.CompilerParams(collective_id=3, has_side_effects=True, vmem_limit_bytes=63 * 2**20),
        name="third",
    )(gmid, x, attn, alpha.reshape(1, D), mine, seg.reshape(total, 1), seg.reshape(1, total), gain, wo, wq, qkv, raw, res, hall, dd)


def fourth_kernel(S, FS, hp, vec, x_ref, gh1, ps_i, du, dd, dout, dqkv,
                  up_o, dn_o, out_o, gx_o, qkv_o, vec_o, sqk_o,
                  own_u, raw_u, oth_u, own_d, raw_d, oth_d, own_o, raw_o, oth_o, so, xo, sq, xq, agq, ps, pr, va, vb, vf, vz,
                  ld_sem, s_u, r_u, s_xo, r_xo, s_xq, r_xq, s_au, r_au, s_ad, r_ad, s_fq, r_fq, s_v, r_v,
                  s_p, r_p, *chain_sems):
    g, z, f = lax.axis_index("grp"), lax.axis_index("seq"), lax.axis_index("fsdp")
    tok = x_ref.shape[0]
    rows = own_u.shape[1]
    fl = own_u.shape[2]
    ff = fl * FS
    hw = hp * HEAD
    dh = D // 2
    peers = [lax.rem(f + i, FS) for i in range(1, FS)]
    bpeers = [lax.rem(f + FS - i, FS) for i in range(1, FS)]
    zpeers = [lax.rem(z + i, S) for i in range(1, S)]
    above, below = (g, lax.rem(z + 1, S), f), (g, lax.rem(z + S - 1, S), f)
    partner = (1 - g, z, f)
    first_z, last_z = z == 0, z == S - 1
    R = range(FS - 1)
    greet([(g, z, p) for p in peers] + [(g, p, f) for p in zpeers] + [partner])

    def blk(p):
        return ds(p * rows, rows, 16)

    l_u = pltpu.make_async_copy(du.at[blk(f)], own_u.at[f], ld_sem.at[0])
    l_p = pltpu.make_async_copy(ps_i, ps, ld_sem.at[3])
    l_q = pltpu.make_async_copy(dqkv.at[blk(f)], sq, ld_sem.at[1])
    l_o = pltpu.make_async_copy(dout.at[blk(f)], so, ld_sem.at[2])
    hl = own_d.shape[0]
    l_d = pltpu.make_async_copy(dd.at[pl.ds(hl, hl)], own_d, ld_sem.at[4])
    for c in (l_d, l_p, l_u, l_q, l_o):
        c.start()
    c_q = [rcopy(dqkv.at[blk(p)], xq.at[i], s_xq.at[i], r_xq.at[i], (g, z, p)) for i, p in enumerate(peers)]
    c_u = [rcopy(du.at[blk(p)], own_u.at[f], s_u.at[i], r_u.at[i], (g, z, p)) for i, p in enumerate(peers)]
    c_o = [rcopy(dout.at[blk(p)], xo.at[i], s_xo.at[i], r_xo.at[i], (g, z, p)) for i, p in enumerate(peers)]
    for c in c_q + c_u + c_o:
        c.start()
    va[...] = vec[...]
    v_c = rcopy(va, vb, s_v.at[0], r_v.at[0], partner)
    v_c.start()

    pieces = []
    for lo_r, n_r in cuts(hl, (0, 1, 2), 2):
        a = pl.ds(lo_r, n_r)
        pieces.append((own_d.at[a], raw_d.at[a], oth_d.at[a], lambda o, a=a: o[2].at[g, a]))
    for p in [f] + bpeers:
        for lo_r, n_r in cuts(rows, (0, 1, 2), 2):
            a = pl.ds(lo_r, n_r)
            pieces.append((own_u.at[p, a], raw_u.at[p, a], oth_u.at[p, a],
                           lambda o, p=p, a=a: o[0].at[a, ds(g * ff + p * fl, fl, 128)]))
    for lo_r, n_r in cuts(rows, (0, 1, 2), 2):
        a = pl.ds(lo_r, n_r)
        pieces.append((own_o.at[a], raw_o.at[a], oth_o.at[a], lambda o, a=a: o[1].at[a, ds(g * dh, dh, 128)]))
    launch, step, drain = make_chain(S, pieces, (up_o, out_o, dn_o), chain_sems)

    def add_all(own, recv):
        acc = own[...].astype(F32)
        for i in R:
            acc = acc + recv[i].astype(F32)
        return acc.astype(BF)

    def go_up(b):
        return rcopy(ps.at[b], pr.at[b], s_p.at[b], r_p.at[b], above)

    def go_down(b):
        slot = jnp.where(z == b + 1, S, b)
        return rcopy(ps.at[b], pr.at[slot], s_p.at[b], r_p.at[slot], below)

    def gh_end(c):
        @pl.when(first_z)
        def _():
            go_up(S - 1 - c).start()

        @pl.when(last_z)
        def _():
            go_down(c).start()

    def gh_mid(c):
        bu, bd = S - 1 - c + z, c - (S - 1 - z)

        def up():
            @pl.when((z > 0) & (bu > z) & (bu < S))
            def _():
                go_up(bu).wait_recv()
                add_into(ps.at[bu], pr.at[bu], 64)
                go_up(bu).start()

        def down():
            @pl.when((z < S - 1) & (bd >= 0) & (bd < z))
            def _():
                rcopy(ps.at[bd], pr.at[bd], s_p.at[bd], r_p.at[bd], above).wait_recv()
                add_into(ps.at[bd], pr.at[bd], 64)
                go_down(bd).start()

        @pl.when(z < S // 2)
        def _():
            up()

        down()

        @pl.when(z >= S // 2)
        def _():
            up()

    def piece(b):
        return agq.at[b, g]

    def a_up(t, b):
        return rcopy(piece(b), piece(b), s_au.at[t], r_au.at[t], above)

    def a_down(t, b):
        return rcopy(piece(b), piece(b), s_ad.at[t], r_ad.at[t], below)

    def fq(b):
        return rcopy(piece(b), piece(b), s_fq.at[b], r_fq.at[b], partner)

    def a_start():
        @pl.when(z < S - 1)
        def _():
            a_up(0, z).start()

        @pl.when(z > 0)
        def _():
            a_down(0, z).start()

        fq(z).start()

    def a_relay(t):
        bu, bd = z - 1 - t, z + 1 + t

        @pl.when(bu >= 0)
        def _():
            a_up(t, bu).wait_recv()

            @pl.when(z < S - 1)
            def _():
                a_up(t + 1, bu).start()

            fq(bu).start()

        @pl.when(bd < S)
        def _():
            a_down(t, bd).wait_recv()

            @pl.when(z > 0)
            def _():
                a_down(t + 1, bd).start()

            fq(bd).start()

    l_d.wait()
    launch(0)
    launch(1)
    l_p.wait()
    gh_end(0)
    step(0)
    v_c.wait()
    vf[f] = va[...] + vb[...]
    v_f = [rcopy(vf.at[f], vf.at[f], s_v.at[1 + i], r_v.at[1 + i], (g, z, p)) for i, p in enumerate(peers)]
    for c in v_f:
        c.start()
    step(1)
    l_q.wait()
    for c in c_q:
        c.wait()
    agq[z, g] = add_all(sq, xq)
    a_start()
    gh_mid(1)
    l_u.wait()
    launch(2)
    launch(3)
    gh_end(1)
    step(2)
    step(3)
    gh_mid(2)
    n = 4
    for i in R:
        c_u[i].wait()
        launch(n)
        launch(n + 1)
        if 2 + i < S - 1:
            gh_end(2 + i)
        step(n)
        step(n + 1)
        n += 2
        if 3 + i < S - 1:
            gh_mid(3 + i)
        if i < S - 1:
            a_relay(i)
        if i == 0:
            for c in v_f:
                c.wait()
            acc = vf[0]
            for k in range(1, FS):
                acc = acc + vf[k]
            sub = lax.broadcasted_iota(jnp.int32, acc.shape, 0)
            vz[z] = jnp.where(sub < 3, acc, vf[f])
            v_z = [rcopy(vz.at[z], vz.at[z], s_v.at[FS + k], r_v.at[FS + k], (g, p, f)) for k, p in enumerate(zpeers)]
            for c in v_z:
                c.start()
    l_o.wait()
    for c in c_o:
        c.wait()
    own_o[...] = add_all(so, xo)
    launch(n)
    launch(n + 1)
    step(n)
    step(n + 1)
    n += 2
    for i in range(FS - 1, S - 1):
        a_relay(i)
    for c in v_z:
        c.wait()
    acc = vz[0]
    for i in range(1, S):
        acc = acc + vz[i]
    vec_o[...] = acc
    for i in range(S):
        sqk_o[i] = vz[i]
    step(n)
    step(n + 1)

    cr = tok // 4
    gx_o[...] = gh1[...]
    add_into(gx_o, ps.at[z], 64)

    @pl.when(z > 0)
    def _():
        go_up(z).wait_recv()
        add_into(gx_o, pr.at[z], 64)

    @pl.when(z < S - 1)
    def _():
        rcopy(ps.at[0], pr.at[S], s_p.at[0], r_p.at[S], above).wait_recv()
        add_into(gx_o, pr.at[S], 64)

    def post(i, carry):
        at = ds(i * cr, cr, 16)
        x = x_ref[at].astype(F32)
        inv = inv_rms(x)
        gx_o[at] = back(x * inv, inv, gx_o[at])
        return carry

    lax.fori_loop(0, 4, post, 0)
    for k in range(S):
        fq(k).wait_recv()
    full = [jnp.concatenate([agq[k, 0], agq[k, 1]], axis=1) for k in range(S)]
    cols = []
    for c in range(3):
        row = jnp.concatenate([full[k][:, c * hw : (c + 1) * hw] for k in range(S)], axis=1)
        cols.append(row[:, :D])
    qkv_o[...] = jnp.concatenate(cols, axis=1)
    for k in range(2, 5):
        step(n + k)
    for k in range(S):
        fq(k).wait_send()

        @pl.when(z != k)
        def _():
            go_up(k).wait_send()

    for t in range(S - 1):
        @pl.when((z < S - 1) & (z - t >= 0))
        def _():
            a_up(t, z).wait_send()

        @pl.when((z > 0) & (z + t < S))
        def _():
            a_down(t, z).wait_send()

    drain()


def fourth(S, FS, hp, vec, x, gh1, ps, du, dd, dout, dqkv):
    tok = x.shape[0]
    fl = du.shape[1]
    rows = D // FS
    hw = hp * HEAD
    w2 = 3 * hw // 2
    dh = D // 2
    n = 4 + 2 * FS
    sds = jax.ShapeDtypeStruct
    outs = [sds((rows, 2 * FS * fl), BF), sds((2, dd.shape[0] // 2, D), BF), sds((rows, D), BF), sds((tok, D), F32), sds((rows, 3 * D), BF),
            sds(vec.shape, F32), sds((S,) + vec.shape, F32)]
    dma = lambda k: pltpu.SemaphoreType.DMA((k,))
    F1 = FS - 1
    u, o = pltpu.VMEM((FS, rows, fl), BF), pltpu.VMEM((rows, dh), BF)
    hd = pltpu.VMEM((dd.shape[0] // 2, D), BF)
    v = pltpu.VMEM(vec.shape, F32)
    return pl.pallas_call(
        lambda *refs: fourth_kernel(S, FS, hp, *refs),
        out_shape=outs,
        in_specs=[VM] * 3 + [ANY] * 5,
        out_specs=[ANY, ANY, ANY, VM, VM, VM, VM],
        scratch_shapes=[
            u, u, u, hd, hd, hd, o, o, o, o, pltpu.VMEM((F1, rows, dh), BF),
            pltpu.VMEM((rows, w2), BF), pltpu.VMEM((F1, rows, w2), BF), pltpu.VMEM((S, 2, rows, w2), BF),
            pltpu.VMEM((S, tok, D), BF), pltpu.VMEM((S + 1, tok, D), BF),
            v, v, pltpu.VMEM((FS,) + vec.shape, F32), pltpu.VMEM((S,) + vec.shape, F32),
            dma(5), dma(F1), dma(F1), dma(F1), dma(F1), dma(F1), dma(F1),
            dma(S), dma(S), dma(S), dma(S), dma(S), dma(S), dma(FS + S), dma(FS + S), dma(S), dma(S + 1),
        ] + [dma(n)] * 7,
        compiler_params=pltpu.CompilerParams(collective_id=4, has_side_effects=True, vmem_limit_bytes=60 * 2**20),
        name="fourth",
    )(vec, x, gh1, ps, du, dd, dout, dqkv)


def body(S, FS, inputs, segments, w_qkv, w_out, w_upgate, w_down, s_qk, alpha_attn, alpha_mlp, s_up, s_gate, cotangent):
    z = lax.axis_index("seq")
    f = lax.axis_index("fsdp")
    hp = -(-HEADS // S)
    hw = hp * HEAD
    rows = w_qkv.shape[0]
    ff = s_up.shape[0]
    fl = ff // FS
    x = inputs[0]
    seg = segments[0]
    gains = jnp.pad(s_qk, (0, S * hw - D))
    gain = lax.dynamic_slice_in_dim(gains, z * hw, hw).reshape(hp, HEAD)
    hall, wq, wo, wu, raw, qkv, res, mine, attn, mid = first(S, FS, hp, x, seg, w_qkv, w_out, gain, alpha_attn, w_upgate)
    su = lax.dynamic_slice_in_dim(s_up, f * fl, fl).reshape(1, fl)
    sg = lax.dynamic_slice_in_dim(s_gate, f * fl, fl).reshape(1, fl)
    out, g_mid, du, dd, d_mlp, d_su, d_sg = second(S, FS, mid, cotangent[0], w_down, su, sg, alpha_mlp, wu, w_upgate)
    gh1, ps, dout, dqkv, dn_a, d_attn, d_sqk = third(
        S, FS, hp, g_mid, x, attn, alpha_attn, mine, seg, gain, wo, wq, qkv, raw, res, hall, dd
    )

    def row(v):
        return jnp.pad(v.reshape(1, -1), ((0, 0), (0, D - v.size)))

    vec = jnp.concatenate([row(d_mlp), row(d_attn), row(d_sqk), row(d_su), row(d_sg), jnp.zeros((3, D), F32)])
    d_up, dn_b, d_o, g_x, d_q, tot, parts = fourth(S, FS, hp, vec, x, gh1, ps, du, dd, dout, dqkv)
    d_down = jnp.concatenate([dn_a[0], dn_b[0], dn_a[1], dn_b[1]])
    sqk = parts[:, 2, :hw].reshape(-1)

    def own(v):
        return lax.dynamic_slice_in_dim(v, f * rows, rows)

    return (
        out[None], g_x[None], d_q.astype(F32), d_o.astype(F32), d_up.astype(F32), d_down.astype(F32),
        own(sqk), own(tot[1]), own(tot[0]), tot[3, :fl], tot[4, :fl],
    )


def solution(mesh):
    S, FS = mesh.shape["seq"], mesh.shape["fsdp"]
    tok = P(("grp", "fsdp"), "seq", None)
    w = P("fsdp", None)
    in_specs = (tok, P(("grp", "fsdp"), None), w, w, w, w, P(), P(), P(), P(), P(), tok)
    out_specs = (tok, tok, w, w, w, w) + (P("fsdp"),) * 5

    def run(*args):
        return body(S, FS, *args)

    return jax.shard_map(run, mesh=mesh, in_specs=in_specs, out_specs=out_specs, check_vma=False)
```

```python
import jax
import jax.numpy as jnp
from jax import lax
from jax.experimental import pallas as pl
from jax.experimental.pallas import tpu as pltpu
from jax.sharding import PartitionSpec as P

D = 1280
HEADS = 20
HEAD = 64

eps_norm = 1e-06
neg_big = -1e30
BF = jnp.bfloat16
F32 = jnp.float32
MESH = pl.DeviceIdType.MESH
ANY = pl.BlockSpec(memory_space=pl.ANY)
VM = pl.BlockSpec(memory_space=pltpu.VMEM)


def inv_rms(value):
    return lax.rsqrt(jnp.mean(value * value, axis=-1, keepdims=True) + eps_norm)


def back(unit, inv, grad):
    return (grad - unit * jnp.mean(grad * unit, axis=-1, keepdims=True)) * inv


def mm(a, b):
    return jnp.dot(a, b, preferred_element_type=F32)


def mm_nt(a, b):
    return lax.dot_general(a, b, (((1,), (1,)), ((), ())), preferred_element_type=F32)


def mm_tn(a, b):
    return lax.dot_general(a, b, (((0,), (0,)), ((), ())), preferred_element_type=F32)


def rcopy(src, dst, ss, rs, dev):
    return pltpu.make_async_remote_copy(src, dst, ss, rs, device_id=dev, device_id_type=MESH)


def greet(peers):
    bar = pltpu.get_barrier_semaphore()
    for p in peers:
        pl.semaphore_signal(bar, inc=1, device_id=p, device_id_type=MESH)
    pl.semaphore_wait(bar, len(peers))


def ds(start, size, mult):
    return pl.ds(pl.multiple_of(start, mult), size)


def visible(seg_col, seg_row, q0, k0, nq, nk):
    qi = q0 + lax.broadcasted_iota(jnp.int32, (nq, nk), 0)
    ki = k0 + lax.broadcasted_iota(jnp.int32, (nq, nk), 1)
    return (ki <= qi) & ((seg_row == 0) | (seg_row == seg_col))


def add_into(dst, src, chunk, out=None):
    out = dst if out is None else out

    def one(i, carry):
        at = ds(i * chunk, chunk, 16)
        out[at] = (dst[at].astype(F32) + src[at].astype(F32)).astype(dst.dtype)
        return carry

    lax.fori_loop(0, src.shape[0] // chunk, one, 0)


def attn_bias(S, tok, half, bias, segr):
    for qb in range(S):
        q0 = qb * tok
        column = jnp.transpose(jnp.broadcast_to(segr[:, q0 : q0 + tok], (128, tok)))[:, :1]
        k0 = q0 if q0 < half else half
        nk = q0 + tok - k0
        ok = visible(column, segr[:, k0 : k0 + nk], q0, k0, tok, nk)
        bias[qb, :, :nk] = jnp.where(ok, 0.0, neg_big).astype(BF)


def first_kernel(S, FS, hp, x_ref, segr, wqkv, wout, par, wup,
                 hall_o, wq_o, wo_o, wu_o, raw_o, qkv_o, res_o, mine_o, attn_o, mid_o,
                 hall, wq, wo, raw, qkv, res, bias, oh, mixs, mine, recv,
                 s_up, r_up, s_dn, r_dn, s_wq, r_wq, s_wo, r_wo, s_wu, r_wu, f_wq, f_wo, f_wu,
                 g_wq, g_wo, g_wu, s_mx, r_mx, out_sem):
    g, z, f = lax.axis_index("grp"), lax.axis_index("seq"), lax.axis_index("fsdp")
    tok = x_ref.shape[0]
    rows = wqkv.shape[0]
    hr = rows // 2
    hw = hp * HEAD
    ff = wup.shape[1] // 2
    fl = ff // FS
    total = S * tok
    half = total // 2
    fpeers = [lax.rem(f + i, FS) for i in range(1, FS)]
    zpeers = [lax.rem(z + i, S) for i in range(1, S)]
    greet([(g, z, p) for p in fpeers] + [(g, p, f) for p in zpeers] + [(1 - g, z, f)])

    x = x_ref[...].astype(F32)
    hall[z] = (x * inv_rms(x)).astype(BF)

    def up(t, b):
        return rcopy(hall.at[b], hall.at[b], s_up.at[t], r_up.at[t], (g, lax.rem(z + 1, S), f))

    def down(t, b):
        return rcopy(hall.at[b], hall.at[b], s_dn.at[t], r_dn.at[t], (g, lax.rem(z + S - 1, S), f))

    @pl.when(z + 1 < S)
    def _():
        up(0, z).start()

    @pl.when(z > 0)
    def _():
        down(0, z).start()

    for k in range(S):
        lo, hi = k * hw, min((k + 1) * hw, D)

        @pl.when(z == k)
        def _():
            parts = []
            for c in range(3):
                if hi > lo:
                    parts.append(wqkv[:, c * D + lo : c * D + hi])
                if hi - lo < hw:
                    parts.append(jnp.zeros((rows, hw - max(hi - lo, 0)), BF))
            wq[ds(f * rows, rows, 16)] = jnp.concatenate(parts, axis=1)

    def wq_half(src, gg):
        return wq.at[ds(src * rows + gg * hr, hr, 16)]

    def wo_half(src, gg):
        return wo.at[ds(src * rows + gg * hr, hr, 16)]

    c_wq = [rcopy(wq_half(f, g), wq_half(f, g), s_wq.at[i], r_wq.at[i], (g, z, p)) for i, p in enumerate(fpeers)]
    for c in c_wq:
        c.start()
    attn_bias(S, tok, half, bias, segr)
    wo[ds(f * rows, rows, 16)] = wout[...]
    qkv[2, :, :, HEAD:] = jnp.where(lax.broadcasted_iota(jnp.int32, (hp, total, HEAD), 2) == 0, 1.0, 0.0).astype(BF)

    bpeers = [lax.rem(f + FS - i, FS) for i in range(1, FS)]
    partner = (1 - g, z, f)
    fw_wq = [rcopy(wq_half(p, g), wq_half(p, g), f_wq.at[i], g_wq.at[i], partner) for i, p in enumerate(bpeers)]
    for i in range(FS - 1):
        c_wq[i].wait_recv()
        fw_wq[i].start()
    c_wo = [rcopy(wo_half(f, g), wo_half(f, g), s_wo.at[i], r_wo.at[i], (g, z, p)) for i, p in enumerate(fpeers)]
    for c in c_wo:
        c.start()

    def wu_cp(i, p):
        return rcopy(wup.at[:, ds(g * ff + p * fl, fl, 128)], wu_o.at[g, f], s_wu.at[i], r_wu.at[i], (g, z, p))

    c_wu = [wu_cp(i, p) for i, p in enumerate(fpeers)]
    for c in c_wu:
        c.start()
    for i in range(FS - 1):
        fw_wq[i].wait_recv()

    def step(i, carry):
        t = lax.div(i - 1, 2)
        is_up = lax.rem(i, 2) == 1
        b = jnp.where(i == 0, z, jnp.where(is_up, z - 1 - t, z + 1 + t))

        @pl.when((b >= 0) & (b < S))
        def _():
            @pl.when((i > 0) & is_up)
            def _():
                up(t, b).wait_recv()

                @pl.when(z + 1 < S)
                def _():
                    up(t + 1, b).start()

            @pl.when((i > 0) & jnp.logical_not(is_up))
            def _():
                down(t, b).wait_recv()

                @pl.when(z > 0)
                def _():
                    down(t + 1, b).start()

            acc = mm(hall[b], wq[...])
            at = ds(b * tok, tok, 16)
            for j in range(hp):
                for c in range(2):
                    v = acc[:, c * hw + j * HEAD : c * hw + (j + 1) * HEAD]
                    raw[j, at, c * HEAD : (c + 1) * HEAD] = v
                    u = v * inv_rms(v) * par[2:3, j * HEAD : (j + 1) * HEAD]
                    qkv[c, j, at, :HEAD] = u.astype(BF)
                qkv[2, j, at, :HEAD] = acc[:, 2 * hw + j * HEAD : 2 * hw + (j + 1) * HEAD].astype(BF)

        return carry

    lax.fori_loop(0, 2 * S - 1, step, 0)
    outs = [
        pltpu.make_async_copy(hall, hall_o, out_sem.at[0]),
        pltpu.make_async_copy(wq, wq_o, out_sem.at[1]),
        pltpu.make_async_copy(raw, raw_o, out_sem.at[2]),
        pltpu.make_async_copy(qkv, qkv_o, out_sem.at[3]),
    ]
    for c in outs:
        c.start()

    def mx(qb):
        return rcopy(mixs.at[qb], recv.at[z], s_mx.at[qb], r_mx.at[z], (g, qb, f))

    for qb in reversed(range(S)):
        q0 = qb * tok
        n = q0 + tok
        k0 = q0 if q0 < half else half

        def head(j, carry):
            q = qkv[0, j, q0:n, :HEAD] * jnp.asarray(HEAD**-0.5, BF)
            s = mm_nt(q, qkv[1, j, :n, :HEAD])
            tail = s[:, k0:] + bias[qb, :, : n - k0].astype(F32)
            e = jnp.exp(jnp.concatenate([s[:, :k0], tail], axis=1) if k0 else tail)
            o = mm(e.astype(BF), qkv[2, j, :n])
            rinv = 1.0 / o[:, HEAD : HEAD + 1]
            o = o[:, :HEAD] * rinv
            res[j, q0:n, :HEAD] = o
            res[j, q0:n, HEAD:] = jnp.broadcast_to(rinv, (tok, HEAD))
            oh[j] = o.astype(BF)
            return carry

        lax.fori_loop(0, hp, head, 0)
        block = jnp.concatenate([oh[j] for j in range(hp)], axis=1)
        mixs[qb] = block

        @pl.when(z != qb)
        def _():
            mx(qb).start()

        @pl.when(z == qb)
        def _():
            recv[qb] = block

        if qb == S - 1:
            fw_wo = [rcopy(wo_half(p, g), wo_half(p, g), f_wo.at[i], g_wo.at[i], partner) for i, p in enumerate(bpeers)]
            for i in range(FS - 1):
                c_wo[i].wait_recv()
                fw_wo[i].start()

    fw_wu = [rcopy(wu_o.at[g, p], wu_o.at[g, p], f_wu.at[i], g_wu.at[i], partner) for i, p in enumerate(bpeers)]
    for i in range(FS - 1):
        c_wu[i].wait_recv()
        fw_wu[i].start()
    for i in range(FS - 1):
        fw_wo[i].wait_recv()
    outs2 = [pltpu.make_async_copy(wo, wo_o, out_sem.at[4]), pltpu.make_async_copy(res, res_o, out_sem.at[5])]
    for c in outs2:
        c.start()
    for k in range(S):
        @pl.when(z != k)
        def _():
            rcopy(mixs.at[0], recv.at[k], s_mx.at[0], r_mx.at[k], (g, k, f)).wait_recv()

    mine[...] = jnp.concatenate([recv[k] for k in range(S)], axis=1)[:, :D]
    attn = mm(mine[...], wo[...])
    attn_o[...] = attn
    mine_o[...] = mine[...]
    x = x_ref[...].astype(F32)
    h = x * inv_rms(x)
    n_ = h + par[0:1] * (attn * inv_rms(attn) - h)
    mid_o[...] = n_ * inv_rms(n_)

    for t in range(S - 1):
        @pl.when((z + 1 < S) & (z - t >= 0))
        def _():
            up(t, z).wait_send()

        @pl.when((z > 0) & (z + t < S))
        def _():
            down(t, z).wait_send()

    for i in range(FS - 1):
        c_wq[i].wait_send()
        c_wo[i].wait_send()
        c_wu[i].wait_send()
        fw_wq[i].wait_send()
        fw_wo[i].wait_send()
        fw_wu[i].wait()
    for k in range(S):
        @pl.when(z != k)
        def _():
            mx(k).wait_send()
    for c in outs + outs2:
        c.wait()


def first(S, FS, hp, x, seg, wqkv, wout, par, wup):
    tok, total = x.shape[0], seg.shape[0]
    rows = wqkv.shape[0]
    hw = hp * HEAD
    fl = wup.shape[1] // 2 // FS
    sds = jax.ShapeDtypeStruct
    outs = [
        sds((S, tok, D), BF), sds((D, 3 * hw), BF), sds((D, D), BF), sds((2, FS, rows, fl), BF),
        sds((hp, total, 2 * HEAD), F32), sds((3, hp, total, 2 * HEAD), BF), sds((hp, total, 2 * HEAD), F32),
        sds((tok, D), BF), sds((tok, D), F32), sds((tok, D), F32),
    ]
    dma = lambda n: pltpu.SemaphoreType.DMA((n,))
    F1 = FS - 1
    return pl.pallas_call(
        lambda *refs: first_kernel(S, FS, hp, *refs),
        out_shape=outs,
        in_specs=[VM] * 5 + [ANY],
        out_specs=[ANY] * 7 + [VM] * 3,
        scratch_shapes=[
            pltpu.VMEM((S, tok, D), BF), pltpu.VMEM((D, 3 * hw), BF), pltpu.VMEM((D, D), BF),
            pltpu.VMEM((hp, total, 2 * HEAD), F32), pltpu.VMEM((3, hp, total, 2 * HEAD), BF),
            pltpu.VMEM((hp, total, 2 * HEAD), F32), pltpu.VMEM((S, tok, total // 2), BF),
            pltpu.VMEM((hp, tok, HEAD), BF), pltpu.VMEM((S, tok, hw), BF), pltpu.VMEM((tok, D), BF),
            pltpu.VMEM((S, tok, hw), BF),
            dma(S), dma(S), dma(S), dma(S), dma(F1), dma(F1), dma(F1), dma(F1), dma(F1), dma(F1),
            dma(F1), dma(F1), dma(F1), dma(F1), dma(F1), dma(F1), dma(S), dma(S), dma(6),
        ],
        compiler_params=pltpu.CompilerParams(collective_id=1, has_side_effects=True, vmem_limit_bytes=60 * 2**20),
        name="first",
    )(x, seg.reshape(1, total), wqkv, wout, par, wup)


def second_kernel(S, FS, NC, mid, cot, wd, par, wu_i, wup,
                  out_o, gmid_o, du_o, dd_o, vec_o,
                  wu, mida, up, gate, hid, ps, pr, rl, gma, gu, dup, ddn, lu, ld,
                  s_a, r_a, s_b, r_b, s_c, r_c, s_d, r_d, w_sem, s_x, r_x, out_sem):
    g, z, f = lax.axis_index("grp"), lax.axis_index("seq"), lax.axis_index("fsdp")
    tok = mid.shape[0]
    ct = tok // NC
    hc = ct // 2
    fl = wd.shape[0]
    ff = wup.shape[1] // 2
    rows = wup.shape[0]
    hl = fl // 2
    nt = 256 if fl % 256 == 0 else 128
    M = FS * ct
    relay = FS == 4
    peers = [lax.rem(f + i, FS) for i in range(1, FS)]
    partner = (1 - g, z, f)
    greet([(g, z, p) for p in peers] + [partner])
    R = range(FS - 1)
    A, B = pl.ds(0, hc), pl.ds(hc, hc)
    if relay:
        fx, fy, fd = f + 1 - 2 * lax.rem(f, 2), lax.rem(f + 2, 4), 3 - f
        dx, dy = (g, z, fx), (g, z, fy)

    def direct(buf, ss, rs, c, i):
        return rcopy(buf.at[c, f], buf.at[c, f], ss.at[c, i], rs.at[c, i], (g, z, peers[i]))

    def gcopy(buf, ss, rs, c, k):
        src, half, dev = ((f, A, dx), (f, B, dx), (f, B, dy), (f, A, dy), (fx, A, dy), (fy, B, dx))[k]
        view = buf.at[c, src, half]
        return rcopy(view, view, ss.at[c, k], rs.at[c, k], dev)

    def g_issue(buf, ss, rs, c):
        if relay:
            for k in (0, 2, 1, 3):
                gcopy(buf, ss, rs, c, k).start()
        else:
            for i in R:
                direct(buf, ss, rs, c, i).start()

    def g_relay(buf, ss, rs, c):
        if relay:
            for k in (0, 2):
                gcopy(buf, ss, rs, c, k).wait_recv()
                gcopy(buf, ss, rs, c, 4 if k == 0 else 5).start()

    def g_wait(buf, ss, rs, c):
        if relay:
            for k in (1, 3, 4, 5):
                gcopy(buf, ss, rs, c, k).wait_recv()
        else:
            for i in R:
                direct(buf, ss, rs, c, i).wait_recv()

    def g_sent(buf, ss, rs, c):
        if relay:
            for k in range(6):
                gcopy(buf, ss, rs, c, k).wait_send()
        else:
            for i in R:
                direct(buf, ss, rs, c, i).wait_send()

    def scopy(ss, rs, c, k):
        src, dst, dev = (
            (ps.at[c, fd, A], rl.at[c, 0], dx),
            (ps.at[c, fd, B], rl.at[c, 1], dy),
            (ps.at[c, fx, A], pr.at[c, 0, A], dx),
            (ps.at[c, fy, B], pr.at[c, 1, B], dy),
            (ps.at[c, fy, A], pr.at[c, 1, A], dy),
            (ps.at[c, fx, B], pr.at[c, 0, B], dx),
        )[k]
        return rcopy(src, dst, ss.at[c, k], rs.at[c, k], dev)

    def sdirect(ss, rs, c, i):
        return rcopy(ps.at[c, peers[i]], pr.at[c, i], ss.at[c, i], rs.at[c, i], (g, z, peers[i]))

    def s_issue(ss, rs, c):
        if relay:
            for k in range(4):
                scopy(ss, rs, c, k).start()
        else:
            for i in R:
                sdirect(ss, rs, c, i).start()

    def s_relay(ss, rs, c):
        if relay:
            for k, tgt, half in ((0, fy, A), (1, fx, B)):
                scopy(ss, rs, c, k).wait_recv()
                ps[c, tgt, half] = (ps[c, tgt, half].astype(F32) + rl[c, k].astype(F32)).astype(BF)
                scopy(ss, rs, c, 4 + k).start()

    def s_total(ss, rs, c):
        if relay:
            for k in range(2, 6):
                scopy(ss, rs, c, k).wait_recv()
        else:
            for i in R:
                sdirect(ss, rs, c, i).wait_recv()
        acc = ps[c, f].astype(F32)
        for i in range(2 if relay else FS - 1):
            acc = acc + pr[c, i].astype(F32)
        return acc

    def s_sent(ss, rs, c):
        if relay:
            for k in range(6):
                scopy(ss, rs, c, k).wait_send()
        else:
            for i in R:
                sdirect(ss, rs, c, i).wait_send()

    for c in range(NC):
        mida[c, f] = mid[c * ct : (c + 1) * ct].astype(BF)
        g_issue(mida, s_a, r_a, c)
        if c == 0:
            loads = []
            for k in range(2):
                loads.append(pltpu.make_async_copy(wup.at[:, ds(k * ff + f * fl, fl, 128)], wu.at[k, ds(f * rows, rows, 16)], w_sem.at[k, 0]))
                for i in R:
                    loads.append(pltpu.make_async_copy(wu_i.at[k, peers[i]], wu.at[k, ds(peers[i] * rows, rows, 16)], w_sem.at[k, i + 1]))
            for ld_c in loads:
                ld_c.start()
            vec_o[...] = jnp.zeros_like(vec_o)
        g_relay(mida, s_a, r_a, c)
    for ld_c in loads:
        ld_c.wait()

    for c in range(NC):
        g_wait(mida, s_a, r_a, c)

        def fwd(t, carry):
            cols = ds(t * nt, nt, 128)
            a_in = mida[c].reshape(M, D)
            u = mm(a_in, wu[0, :, cols])
            gt = mm(a_in, wu[1, :, cols])
            up[c, :, cols] = u
            gate[c, :, cols] = gt
            a = gt * par[4:5, cols]
            hid[c, :, cols] = (u * par[3:4, cols] * (a * jax.nn.sigmoid(a))).astype(BF)
            return carry

        lax.fori_loop(0, fl // nt, fwd, 0)
        if c:
            s_relay(s_b, r_b, c - 1)

        def proj(t, carry):
            cols = ds(t * 256, 256, 128)
            ps[c, :, :, cols] = mm(hid[c], wd[:, cols]).astype(BF).reshape(FS, ct, 256)
            return carry

        lax.fori_loop(0, D // 256, proj, 0)
        s_issue(s_b, r_b, c)
    s_relay(s_b, r_b, NC - 1)

    for c in range(NC):
        at = slice(c * ct, (c + 1) * ct)
        mlp = s_total(s_b, r_b, c)
        al = par[1:2]
        md = mid[at]
        inv_m = inv_rms(mlp)
        um = mlp * inv_m
        dif = um - md
        m = md + al * dif
        inv_o = inv_rms(m)
        o = m * inv_o
        out_o[at] = o.astype(BF)
        g_m = back(o, inv_o, cot[at].astype(F32))
        vec_o[0:1] += jnp.sum(g_m * dif, axis=0, keepdims=True)
        gmid_o[at] = (1 - al) * g_m
        gma[c, f] = back(um, inv_m, al * g_m).astype(BF)
        g_issue(gma, s_c, r_c, c)
        g_relay(gma, s_c, r_c, c)

    for c in range(NC):
        g_wait(gma, s_c, r_c, c)

        def bwd(t, carry):
            cols = ds(t * nt, nt, 128)
            gh = mm_nt(gma[c].reshape(M, D), wd[cols, :])
            u = up[c, :, cols]
            gt = gate[c, :, cols]
            sgc = par[4:5, cols]
            suc = par[3:4, cols]
            a = gt * sgc
            sig = jax.nn.sigmoid(a)
            gs = gh * (a * sig)
            gu[0, c, :, cols] = (gs * suc).astype(BF)
            vec_o[3:4, cols] += jnp.sum(u * gs, axis=0, keepdims=True)
            g_a = gh * u * suc * (sig * (1 + a * (1 - sig)))
            gu[1, c, :, cols] = (g_a * sgc).astype(BF)
            vec_o[4:5, cols] += jnp.sum(gt * g_a, axis=0, keepdims=True)
            return carry

        lax.fori_loop(0, fl // nt, bwd, 0)
        if c:
            s_relay(s_d, r_d, c - 1)
        s_sent(s_b, r_b, c)

        def bproj(t, carry):
            cols = ds(t * 256, 256, 128)
            v = mm_nt(gu[0, c], wu[0, cols, :]) + mm_nt(gu[1, c], wu[1, cols, :])
            ps[c, :, :, cols] = v.astype(BF).reshape(FS, ct, 256)
            return carry

        lax.fori_loop(0, D // 256, bproj, 0)
        s_issue(s_d, r_d, c)

    def dwd(t, carry):
        cols = ds(t * nt, nt, 128)
        ddn[cols, :] = mm_tn(hid[:, :, cols].reshape(NC * M, nt), gma[...].reshape(NC * M, D)).astype(BF)
        return carry

    lax.fori_loop(0, fl // nt, dwd, 0)
    s_relay(s_d, r_d, NC - 1)
    x_d = rcopy(ddn.at[ds((1 - g) * hl, hl, 16)], ld, s_x.at[0], r_x.at[0], partner)
    x_d.start()

    def dwu(k):
        def one(t, carry):
            cols = ds(t * 256, 256, 128)
            dup[k, cols, :] = mm_tn(mida[:, :, :, cols].reshape(NC * M, 256), gu[k].reshape(NC * M, fl)).astype(BF)
            return carry

        lax.fori_loop(0, D // 256, one, 0)

    dwu(1 - g)
    x_u = rcopy(dup.at[1 - g], lu, s_x.at[1], r_x.at[1], partner)
    x_u.start()
    dwu(g)
    mine = ds(g * hl, hl, 16)
    x_d.wait_recv()
    add_into(ddn.at[mine], ld, 64)
    o_d = pltpu.make_async_copy(ddn.at[mine], dd_o, out_sem.at[0])
    o_d.start()
    x_u.wait_recv()
    add_into(dup.at[g], lu, 64)
    o_u = pltpu.make_async_copy(dup.at[g], du_o, out_sem.at[1])
    o_u.start()

    for c in range(NC):
        at = slice(c * ct, (c + 1) * ct)
        gmid_o[at] = gmid_o[at] + s_total(s_d, r_d, c)
    for c in range(NC):
        g_sent(mida, s_a, r_a, c)
        g_sent(gma, s_c, r_c, c)
        s_sent(s_d, r_d, c)
    x_d.wait_send()
    x_u.wait_send()
    o_d.wait()
    o_u.wait()


def second(S, FS, mid, cot, wd, par, wu, wup):
    NC = 2
    tok = mid.shape[0]
    ct = tok // NC
    fl = wd.shape[0]
    M = FS * ct
    sds = jax.ShapeDtypeStruct
    outs = [sds((tok, D), BF), sds((tok, D), F32), sds((D, fl), BF), sds((fl // 2, D), BF),
            sds((8, D), F32)]
    dma = pltpu.SemaphoreType.DMA
    F1 = FS - 1
    return pl.pallas_call(
        lambda *refs: second_kernel(S, FS, NC, *refs),
        out_shape=outs,
        in_specs=[VM] * 4 + [ANY] * 2,
        out_specs=[VM, VM, ANY, ANY, VM],
        scratch_shapes=[
            pltpu.VMEM((2, D, fl), BF), pltpu.VMEM((NC, FS, ct, D), BF), pltpu.VMEM((NC, M, fl), F32),
            pltpu.VMEM((NC, M, fl), F32), pltpu.VMEM((NC, M, fl), BF), pltpu.VMEM((NC, FS, ct, D), BF),
            pltpu.VMEM((NC, 2 if FS == 4 else F1, ct, D), BF), pltpu.VMEM((NC, 2, ct // 2, D), BF),
            pltpu.VMEM((NC, FS, ct, D), BF), pltpu.VMEM((2, NC, M, fl), BF),
            pltpu.VMEM((2, D, fl), BF), pltpu.VMEM((fl, D), BF), pltpu.VMEM((D, fl), BF), pltpu.VMEM((fl // 2, D), BF),
        ] + [dma((NC, max(F1, 6)))] * 8 + [dma((2, FS)), dma((2,)), dma((2,)), dma((2,))],
        compiler_params=pltpu.CompilerParams(collective_id=2, has_side_effects=True, vmem_limit_bytes=63 * 2**20),
        name="second",
    )(mid, cot, wd, par, wu, wup)


def make_chain(S, pieces, outs, sems):
    s_in, r_raw, r_oth, s_ret, o_sem, s_o, r_o = sems
    g, z, f = lax.axis_index("grp"), lax.axis_index("seq"), lax.axis_index("fsdp")
    partner = (1 - g, z, f)
    lower = z < S // 2
    inner = jnp.where(lower, z + 1, z - 1)
    mid = (z == S // 2 - 1) | (z == S // 2)
    has_outer = (z > 0) & (z < S - 1)
    outer = jnp.where(has_outer, jnp.where(lower, z - 1, z + 1), inner)
    rest = jnp.logical_not(mid)

    def toward(i, to_mid):
        own, raw, oth, _ = pieces[i]
        if to_mid:
            return rcopy(own, oth, s_in.at[i], r_oth.at[i], (g, inner, f))
        return rcopy(own, raw, s_in.at[i], r_raw.at[i], (g, inner, f))

    def returned(i, from_mid):
        own, raw, oth, _ = pieces[i]
        return rcopy(raw if from_mid else oth, oth, s_ret.at[i], r_oth.at[i], (g, outer, f))

    def local_out(i, src):
        return pltpu.make_async_copy(src, pieces[i][3](outs), o_sem.at[i])

    def remote_out(i, src):
        return rcopy(src, pieces[i][3](outs), s_o.at[i], r_o.at[i], partner)

    def send(i):
        @pl.when(mid)
        def _():
            toward(i, True).start()

        @pl.when(rest)
        def _():
            toward(i, False).start()

    def launch(i):
        @pl.when(jnp.logical_not(has_outer))
        def _():
            send(i)

    def go_in(i):
        own, raw, oth, _ = pieces[i]

        @pl.when(has_outer)
        def _():
            rcopy(own, raw, s_in.at[i], r_raw.at[i], (g, outer, f)).wait_recv()
            add_into(own, raw, 80)
            send(i)

    def finish(i, src, from_mid):
        @pl.when(has_outer)
        def _():
            returned(i, from_mid).start()

        local_out(i, src).start()
        remote_out(i, src).start()

    def arrived(i):
        own, raw, oth, _ = pieces[i]
        rcopy(own, oth, s_in.at[i], r_oth.at[i], (g, inner, f)).wait_recv()

    def step(i, lag=5):
        if i < len(pieces):
            go_in(i)
        if 1 <= i <= len(pieces):
            @pl.when(mid)
            def _():
                own, raw, oth, _ = pieces[i - 1]
                arrived(i - 1)
                add_into(own, oth, 80, raw)
                finish(i - 1, raw, True)
        if lag <= i < len(pieces) + lag:
            @pl.when(rest)
            def _():
                arrived(i - lag)
                finish(i - lag, pieces[i - lag][2], False)

    def drain():
        for i in range(len(pieces)):
            toward(i, True).wait_send()

            @pl.when(has_outer)
            def _():
                returned(i, True).wait_send()

            local_out(i, pieces[i][1]).wait()
            remote_out(i, pieces[i][1]).wait()

    return launch, step, drain


def cuts(size, parts, unit):
    step = size // unit
    return [(a * step, (b - a) * step) for a, b in zip(parts[:-1], parts[1:])]


def third_kernel(S, FS, hp, gmid, x_ref, attn, mine, segr, par, wo, wq_i, qkv_i, raw_i, res_i, hall_i, dd_i,
                 gh1, ps_o, dout_o, dqkv_o, dn_o, vec_o,
                 dsq_o, gain, wq, qkv, raw, res, hall, ga, gsend, gxr, bias, hx, gqh, dkv, gq, ps, dout, dqk, lo, lq, own_d, raw_d, oth_d,
                 ld_sem, h_sem, s_gx, r_gx, s_p, s_x, r_x, out_sem, *chain_sems):
    g, z, f = lax.axis_index("grp"), lax.axis_index("seq"), lax.axis_index("fsdp")
    tok = x_ref.shape[0]
    hw = hp * HEAD
    wide = S * hw
    total = S * tok
    half = total // 2
    w2 = 3 * hw // 2
    dh = D // 2
    partner = (1 - g, z, f)
    greet([(g, lax.rem(z + i, S), f) for i in range(1, S)] + [partner])
    loads = [pltpu.make_async_copy(a, b, ld_sem.at[i]) for i, (a, b) in enumerate(
        [(qkv_i, qkv), (raw_i, raw), (res_i, res), (wq_i, wq)])]
    for c in loads:
        c.start()

    hl = own_d.shape[0]
    dd_c = pltpu.make_async_copy(dd_i.at[pl.ds(0, hl)], own_d, h_sem.at[2])
    dd_c.start()
    pieces = []
    for lo_r, n_r in cuts(hl, (0, 1, 2, 4) if hl % 64 == 0 else (0, 2, 4), 4):
        pieces.append((own_d.at[pl.ds(lo_r, n_r)], raw_d.at[pl.ds(lo_r, n_r)], oth_d.at[pl.ds(lo_r, n_r)],
                       lambda o, lo_r=lo_r, n_r=n_r: o.at[g, pl.ds(lo_r, n_r)]))
    launch, step, drain = make_chain(S, pieces, dn_o, chain_sems)
    n_p = len(pieces)

    def h_tile(t):
        return pltpu.make_async_copy(hall_i.at[:, :, pl.ds(t * 256, 256)], hall.at[t % 2], h_sem.at[t % 2])

    h_tile(0).start()
    h_tile(1).start()
    dd_c.wait()
    launch(0)
    vec_o[...] = jnp.zeros_like(vec_o)
    for j in range(hp):
        gain[j : j + 1] = par[2:3, j * HEAD : (j + 1) * HEAD]
    dsq_o[...] = jnp.zeros_like(dsq_o)
    cr = tok // 4

    def pre(i, carry):
        at = ds(i * cr, cr, 16)
        x = x_ref[at].astype(F32)
        h = x * inv_rms(x)
        av = attn[at]
        inv_a = inv_rms(av)
        ua = av * inv_a
        al = par[0:1]
        dif = ua - h
        n_ = h + al * dif
        inv_n = inv_rms(n_)
        g_n = back(n_ * inv_n, inv_n, gmid[at])
        vec_o[1:2] += jnp.sum(g_n * dif, axis=0, keepdims=True)
        gh1[at] = (1 - al) * g_n
        ga[at] = back(ua, inv_a, al * g_n).astype(BF)
        return carry

    lax.fori_loop(0, 4, pre, 0)
    gmix = mm_nt(ga[...], wo[...]).astype(BF)
    if wide > D:
        gmix = jnp.concatenate([gmix, jnp.zeros((tok, wide - D), BF)], axis=1)
    for k in range(S):
        gsend[k] = gmix[:, k * hw : (k + 1) * hw]

    def gx(k):
        return rcopy(gsend.at[k], gxr.at[z], s_gx.at[k], r_gx.at[z], (g, k, f))

    for k in range(S):
        @pl.when(z != k)
        def _():
            gx(k).start()

        @pl.when(z == k)
        def _():
            gxr[k] = gsend[k]


    def dwo(t, carry):
        cols = ds(t * 256, 256, 128)
        v = mm_tn(mine[:, cols], ga[...]).astype(BF)
        dout[0, cols, :] = v[:, :dh]
        dout[1, cols, :] = v[:, dh:]
        return carry

    lax.fori_loop(0, D // 256, dwo, 0)
    x_o = rcopy(dout.at[1 - g], lo, s_x.at[0], r_x.at[0], partner)
    x_o.start()
    attn_bias(S, tok, half, bias, segr)
    for c in loads:
        c.wait()
    done = 0

    def part(k):
        return pltpu.make_async_copy(ps.at[k], ps_o.at[k], s_p.at[k])

    for qb in reversed(range(S)):
        q0 = qb * tok
        n = q0 + tok
        k0 = q0 if q0 < half else half

        @pl.when(z != qb)
        def _():
            rcopy(gsend.at[0], gxr.at[qb], s_gx.at[0], r_gx.at[qb], (g, qb, f)).wait_recv()

        if qb == S - 1:
            for i in range(1, n_p):
                launch(i)

        for j in range(hp):
            hx[j] = gxr[qb, :, j * HEAD : (j + 1) * HEAD]

        def head(j, carry):
            q = qkv[0, j, q0:n, :HEAD] * jnp.asarray(HEAD**-0.5, BF)
            keys = qkv[1, j, :n, :HEAD]
            gv = hx[j]
            rinv = res[j, q0:n, HEAD : HEAD + 1]
            delta = jnp.sum(gv.astype(F32) * res[j, q0:n, :HEAD], axis=-1, keepdims=True)
            s = mm_nt(q, keys)
            tail = s[:, k0:] + bias[qb, :, : n - k0].astype(F32)
            p = jnp.exp(jnp.concatenate([s[:, :k0], tail], axis=1) if k0 else tail) * rinv
            dp = mm_nt(gv, qkv[2, j, :n, :HEAD])
            dsb = (p * (dp - delta)).astype(BF)
            dq = mm(dsb, keys) * HEAD**-0.5
            dk = mm_tn(dsb, q)
            dv = mm_tn(p.astype(BF), gv)
            if qb < S - 1:
                dk = dk + dkv[j, :n, :HEAD]
                dv = dv + dkv[j, :n, HEAD:]
            if qb:
                dkv[j, :q0, :HEAD] = dk[:q0]
                dkv[j, :q0, HEAD:] = dv[:q0]
            gj = gain[pl.ds(j, 1), :]
            for c, d in ((0, dq), (1, dk[q0:])):
                v = raw[j, q0:n, c * HEAD : (c + 1) * HEAD]
                inv = inv_rms(v)
                u = v * inv
                dsq_o[pl.ds(j, 1), :] += jnp.sum(d * u, axis=0, keepdims=True)
                gqh[c, j] = back(u, inv, d * gj).astype(BF)
            gqh[2, j] = dv[q0:].astype(BF)
            return carry

        lax.fori_loop(0, hp, head, 0)
        gq[qb] = jnp.concatenate([gqh[c, j] for c in range(3) for j in range(hp)], axis=1)
        ps[qb] = mm_nt(gq[qb], wq[...]).astype(BF)

        part(qb).start()
        if done < n_p + 5:
            step(done)
            done += 1

    for t in range(D // 256):
        h_tile(t).wait()
        v = mm_tn(hall[t % 2].reshape(total, 256), gq[...].reshape(total, 3 * hw)).astype(BF)
        dqk[0, t * 256 : (t + 1) * 256, :] = v[:, :w2]
        dqk[1, t * 256 : (t + 1) * 256, :] = v[:, w2:]
        if t + 2 < D // 256:
            h_tile(t + 2).start()
    x_q = rcopy(dqk.at[1 - g], lq, s_x.at[1], r_x.at[1], partner)
    x_q.start()
    x_o.wait_recv()
    add_into(dout.at[g], lo, 128)
    o_o = pltpu.make_async_copy(dout.at[g], dout_o, out_sem.at[0])
    o_o.start()
    for j in range(hp):
        vec_o[2:3, j * HEAD : (j + 1) * HEAD] = dsq_o[j : j + 1]
    while done < n_p + 5:
        step(done)
        done += 1
    x_q.wait_recv()
    add_into(dqk.at[g], lq, 128)
    o_q = pltpu.make_async_copy(dqk.at[g], dqkv_o, out_sem.at[1])
    o_q.start()

    for k in range(S):
        @pl.when(z != k)
        def _():
            gx(k).wait_send()

        part(k).wait()
    x_o.wait_send()
    x_q.wait_send()
    o_o.wait()
    o_q.wait()
    drain()


def third(S, FS, hp, gmid, x, attn, mine, seg, par, wo, wq, qkv, raw, res, hall, dd):
    tok, total = x.shape[0], seg.shape[0]
    hw = hp * HEAD
    sds = jax.ShapeDtypeStruct
    outs = [sds((tok, D), F32), sds((S, tok, D), BF), sds((D, D // 2), BF), sds((D, 3 * hw // 2), BF), sds((2, dd.shape[0] // 2, D), BF),
            sds((8, D), F32)]
    dma = lambda n: pltpu.SemaphoreType.DMA((n,))
    hd = pltpu.VMEM((dd.shape[0] // 2, D), BF)
    return pl.pallas_call(
        lambda *refs: third_kernel(S, FS, hp, *refs),
        out_shape=outs,
        in_specs=[VM] * 7 + [ANY] * 6,
        out_specs=[VM, ANY, ANY, ANY, ANY, VM],
        scratch_shapes=[
            pltpu.VMEM((hp, HEAD), F32), pltpu.VMEM((hp, HEAD), F32),
            pltpu.VMEM((D, 3 * hw), BF), pltpu.VMEM((3, hp, total, 2 * HEAD), BF), pltpu.VMEM((hp, total, 2 * HEAD), F32),
            pltpu.VMEM((hp, total, 2 * HEAD), F32), pltpu.VMEM((2, S, tok, 256), BF),
            pltpu.VMEM((tok, D), BF), pltpu.VMEM((S, tok, hw), BF), pltpu.VMEM((S, tok, hw), BF),
            pltpu.VMEM((S, tok, total // 2), BF), pltpu.VMEM((hp, tok, HEAD), BF), pltpu.VMEM((3, hp, tok, HEAD), BF),
            pltpu.VMEM((hp, total, 2 * HEAD), F32), pltpu.VMEM((S, tok, 3 * hw), BF), pltpu.VMEM((S, tok, D), BF),
            pltpu.VMEM((2, D, D // 2), BF), pltpu.VMEM((2, D, 3 * hw // 2), BF),
            pltpu.VMEM((D, D // 2), BF), pltpu.VMEM((D, 3 * hw // 2), BF),
            hd, hd, hd,
            dma(4), dma(3), dma(S), dma(S), dma(S), dma(2), dma(2), dma(2),
        ] + [dma(5)] * 7,
        compiler_params=pltpu.CompilerParams(collective_id=3, has_side_effects=True, vmem_limit_bytes=63 * 2**20),
        name="third",
    )(gmid, x, attn, mine, seg.reshape(1, total), par, wo, wq, qkv, raw, res, hall, dd)


def fourth_kernel(S, FS, hp, vec, vec2, x_ref, gh1, ps_i, du, dd, dout, dqkv,
                  up_o, dn_o, out_o, gx_o, qkv_o, vec_o, sqk_o,
                  own_u, raw_u, oth_u, own_d, raw_d, oth_d, own_o, raw_o, oth_o, so, xo, sq, xq, agq, ps, pr, va, vb, vf, vz,
                  ld_sem, s_u, r_u, s_xo, r_xo, s_xq, r_xq, s_au, r_au, s_ad, r_ad, s_fq, r_fq, s_v, r_v,
                  s_p, r_p, *chain_sems):
    g, z, f = lax.axis_index("grp"), lax.axis_index("seq"), lax.axis_index("fsdp")
    tok = x_ref.shape[0]
    rows = own_u.shape[1]
    fl = own_u.shape[2]
    ff = fl * FS
    hw = hp * HEAD
    dh = D // 2
    peers = [lax.rem(f + i, FS) for i in range(1, FS)]
    bpeers = [lax.rem(f + FS - i, FS) for i in range(1, FS)]
    zpeers = [lax.rem(z + i, S) for i in range(1, S)]
    above, below = (g, lax.rem(z + 1, S), f), (g, lax.rem(z + S - 1, S), f)
    partner = (1 - g, z, f)
    first_z, last_z = z == 0, z == S - 1
    R = range(FS - 1)
    greet([(g, z, p) for p in peers] + [(g, p, f) for p in zpeers] + [partner])

    def blk(p):
        return ds(p * rows, rows, 16)

    l_u = pltpu.make_async_copy(du.at[blk(f)], own_u.at[f], ld_sem.at[0])
    l_p = pltpu.make_async_copy(ps_i, ps, ld_sem.at[3])
    l_q = pltpu.make_async_copy(dqkv.at[blk(f)], sq, ld_sem.at[1])
    l_o = pltpu.make_async_copy(dout.at[blk(f)], so, ld_sem.at[2])
    hl = own_d.shape[0]
    l_d = pltpu.make_async_copy(dd.at[pl.ds(hl, hl)], own_d, ld_sem.at[4])
    for c in (l_d, l_p, l_u, l_q, l_o):
        c.start()
    c_q = [rcopy(dqkv.at[blk(p)], xq.at[i], s_xq.at[i], r_xq.at[i], (g, z, p)) for i, p in enumerate(peers)]
    c_u = [rcopy(du.at[blk(p)], own_u.at[f], s_u.at[i], r_u.at[i], (g, z, p)) for i, p in enumerate(peers)]
    c_o = [rcopy(dout.at[blk(p)], xo.at[i], s_xo.at[i], r_xo.at[i], (g, z, p)) for i, p in enumerate(peers)]
    for c in c_q + c_u + c_o:
        c.start()
    va[...] = vec[...] + vec2[...]
    v_c = rcopy(va, vb, s_v.at[0], r_v.at[0], partner)
    v_c.start()

    pieces = []
    for lo_r, n_r in cuts(hl, (0, 1, 2), 2):
        a = pl.ds(lo_r, n_r)
        pieces.append((own_d.at[a], raw_d.at[a], oth_d.at[a], lambda o, a=a: o[2].at[g, a]))
    for p in [f] + bpeers:
        for lo_r, n_r in cuts(rows, (0, 1, 2), 2):
            a = pl.ds(lo_r, n_r)
            pieces.append((own_u.at[p, a], raw_u.at[p, a], oth_u.at[p, a],
                           lambda o, p=p, a=a: o[0].at[a, ds(g * ff + p * fl, fl, 128)]))
    for lo_r, n_r in cuts(rows, (0, 1, 2), 2):
        a = pl.ds(lo_r, n_r)
        pieces.append((own_o.at[a], raw_o.at[a], oth_o.at[a], lambda o, a=a: o[1].at[a, ds(g * dh, dh, 128)]))
    launch, step, drain = make_chain(S, pieces, (up_o, out_o, dn_o), chain_sems)

    def add_all(own, recv):
        acc = own[...].astype(F32)
        for i in R:
            acc = acc + recv[i].astype(F32)
        return acc.astype(BF)

    def go_up(b):
        return rcopy(ps.at[b], pr.at[b], s_p.at[b], r_p.at[b], above)

    def go_down(b):
        slot = jnp.where(z == b + 1, S, b)
        return rcopy(ps.at[b], pr.at[slot], s_p.at[b], r_p.at[slot], below)

    def gh_end(c):
        @pl.when(first_z)
        def _():
            go_up(S - 1 - c).start()

        @pl.when(last_z)
        def _():
            go_down(c).start()

    def gh_mid(c):
        bu, bd = S - 1 - c + z, c - (S - 1 - z)

        def up():
            @pl.when((z > 0) & (bu > z) & (bu < S))
            def _():
                go_up(bu).wait_recv()
                add_into(ps.at[bu], pr.at[bu], 64)
                go_up(bu).start()

        def down():
            @pl.when((z < S - 1) & (bd >= 0) & (bd < z))
            def _():
                rcopy(ps.at[bd], pr.at[bd], s_p.at[bd], r_p.at[bd], above).wait_recv()
                add_into(ps.at[bd], pr.at[bd], 64)
                go_down(bd).start()

        @pl.when(z < S // 2)
        def _():
            up()

        down()

        @pl.when(z >= S // 2)
        def _():
            up()

    def piece(b):
        return agq.at[b, g]

    def a_up(t, b):
        return rcopy(piece(b), piece(b), s_au.at[t], r_au.at[t], above)

    def a_down(t, b):
        return rcopy(piece(b), piece(b), s_ad.at[t], r_ad.at[t], below)

    def fq(b):
        return rcopy(piece(b), piece(b), s_fq.at[b], r_fq.at[b], partner)

    def a_start():
        @pl.when(z < S - 1)
        def _():
            a_up(0, z).start()

        @pl.when(z > 0)
        def _():
            a_down(0, z).start()

        fq(z).start()

    def a_relay(t):
        bu, bd = z - 1 - t, z + 1 + t

        @pl.when(bu >= 0)
        def _():
            a_up(t, bu).wait_recv()

            @pl.when(z < S - 1)
            def _():
                a_up(t + 1, bu).start()

            fq(bu).start()

        @pl.when(bd < S)
        def _():
            a_down(t, bd).wait_recv()

            @pl.when(z > 0)
            def _():
                a_down(t + 1, bd).start()

            fq(bd).start()

    l_d.wait()
    launch(0)
    launch(1)
    l_p.wait()
    gh_end(0)
    v_c.wait()
    vf[f] = va[...] + vb[...]
    v_f = [rcopy(vf.at[f], vf.at[f], s_v.at[1 + i], r_v.at[1 + i], (g, z, p)) for i, p in enumerate(peers)]
    for c in v_f:
        c.start()
    l_q.wait()
    for c in c_q:
        c.wait()
    agq[z, g] = add_all(sq, xq)
    a_start()
    l_u.wait()
    l_o.wait()
    launch(2)
    launch(3)
    ends = first_z | last_z
    inner = jnp.logical_not(ends)

    def last_piece():
        for c in c_o:
            c.wait()
        own_o[...] = add_all(so, xo)

    @pl.when(ends)
    def _():
        for i in R:
            c_u[i].wait()
            launch(4 + 2 * i)
            launch(5 + 2 * i)
            if 1 + i < S - 2:
                gh_end(1 + i)
        last_piece()
        launch(4 + 2 * len(R))
        launch(5 + 2 * len(R))
        gh_end(S - 2)

    step(0)
    step(1)
    gh_mid(1)
    step(2)
    step(3)
    n = 4
    for i in R:
        if i < S - 1:
            a_relay(i)

        @pl.when(inner)
        def _():
            c_u[i].wait()

        step(n)
        step(n + 1)
        n += 2
        if 2 + i < S - 1:
            gh_mid(2 + i)
    for c in v_f:
        c.wait()
    acc = vf[0]
    for k in range(1, FS):
        acc = acc + vf[k]
    sub = lax.broadcasted_iota(jnp.int32, acc.shape, 0)
    vz[z] = jnp.where(sub < 3, acc, vf[f])
    v_z = [rcopy(vz.at[z], vz.at[z], s_v.at[FS + k], r_v.at[FS + k], (g, p, f)) for k, p in enumerate(zpeers)]
    for c in v_z:
        c.start()
    pl.when(inner)(last_piece)
    step(n)
    step(n + 1)
    n += 2
    for i in range(FS - 1, S - 1):
        a_relay(i)
    for c in v_z:
        c.wait()
    acc = vz[0]
    for i in range(1, S):
        acc = acc + vz[i]
    vec_o[...] = acc
    for i in range(S):
        sqk_o[i] = vz[i]
    step(n)
    step(n + 1)

    cr = tok // 4
    gx_o[...] = gh1[...]
    add_into(gx_o, ps.at[z], 64)

    @pl.when(z > 0)
    def _():
        go_up(z).wait_recv()
        add_into(gx_o, pr.at[z], 64)

    @pl.when(z < S - 1)
    def _():
        rcopy(ps.at[0], pr.at[S], s_p.at[0], r_p.at[S], above).wait_recv()
        add_into(gx_o, pr.at[S], 64)

    def post(i, carry):
        at = ds(i * cr, cr, 16)
        x = x_ref[at].astype(F32)
        inv = inv_rms(x)
        gx_o[at] = back(x * inv, inv, gx_o[at])
        return carry

    lax.fori_loop(0, 4, post, 0)
    for k in range(S):
        fq(k).wait_recv()
    full = [jnp.concatenate([agq[k, 0], agq[k, 1]], axis=1) for k in range(S)]
    cols = []
    for c in range(3):
        row = jnp.concatenate([full[k][:, c * hw : (c + 1) * hw] for k in range(S)], axis=1)
        cols.append(row[:, :D])
    qkv_o[...] = jnp.concatenate(cols, axis=1)
    for k in range(2, 5):
        step(n + k)
    for k in range(S):
        fq(k).wait_send()

        @pl.when(z != k)
        def _():
            go_up(k).wait_send()

    for t in range(S - 1):
        @pl.when((z < S - 1) & (z - t >= 0))
        def _():
            a_up(t, z).wait_send()

        @pl.when((z > 0) & (z + t < S))
        def _():
            a_down(t, z).wait_send()

    drain()


def fourth(S, FS, hp, vec, vec2, x, gh1, ps, du, dd, dout, dqkv):
    tok = x.shape[0]
    fl = du.shape[1]
    rows = D // FS
    hw = hp * HEAD
    w2 = 3 * hw // 2
    dh = D // 2
    n = 4 + 2 * FS
    sds = jax.ShapeDtypeStruct
    outs = [sds((rows, 2 * FS * fl), BF), sds((2, dd.shape[0] // 2, D), BF), sds((rows, D), BF), sds((tok, D), F32), sds((rows, 3 * D), BF),
            sds(vec.shape, F32), sds((S,) + vec.shape, F32)]
    dma = lambda k: pltpu.SemaphoreType.DMA((k,))
    F1 = FS - 1
    u, o = pltpu.VMEM((FS, rows, fl), BF), pltpu.VMEM((rows, dh), BF)
    hd = pltpu.VMEM((dd.shape[0] // 2, D), BF)
    v = pltpu.VMEM(vec.shape, F32)
    return pl.pallas_call(
        lambda *refs: fourth_kernel(S, FS, hp, *refs),
        out_shape=outs,
        in_specs=[VM] * 4 + [ANY] * 5,
        out_specs=[ANY, ANY, ANY, VM, VM, VM, VM],
        scratch_shapes=[
            u, u, u, hd, hd, hd, o, o, o, o, pltpu.VMEM((F1, rows, dh), BF),
            pltpu.VMEM((rows, w2), BF), pltpu.VMEM((F1, rows, w2), BF), pltpu.VMEM((S, 2, rows, w2), BF),
            pltpu.VMEM((S, tok, D), BF), pltpu.VMEM((S + 1, tok, D), BF),
            v, v, pltpu.VMEM((FS,) + vec.shape, F32), pltpu.VMEM((S,) + vec.shape, F32),
            dma(5), dma(F1), dma(F1), dma(F1), dma(F1), dma(F1), dma(F1),
            dma(S), dma(S), dma(S), dma(S), dma(S), dma(S), dma(FS + S), dma(FS + S), dma(S), dma(S + 1),
        ] + [dma(n)] * 7,
        compiler_params=pltpu.CompilerParams(collective_id=4, has_side_effects=True, vmem_limit_bytes=60 * 2**20),
        name="fourth",
    )(vec, vec2, x, gh1, ps, du, dd, dout, dqkv)


def body(S, FS, inputs, segments, w_qkv, w_out, w_upgate, w_down, s_qk, alpha_attn, alpha_mlp, s_up, s_gate, cotangent):
    z = lax.axis_index("seq")
    f = lax.axis_index("fsdp")
    hp = -(-HEADS // S)
    hw = hp * HEAD
    rows = w_qkv.shape[0]
    ff = s_up.shape[0]
    fl = ff // FS
    x = inputs[0]
    seg = segments[0]
    gains = jnp.pad(s_qk, (0, S * hw - D))

    def row(v):
        return jnp.pad(v, (0, D - v.size))

    par = jnp.stack([
        alpha_attn, alpha_mlp, row(lax.dynamic_slice_in_dim(gains, z * hw, hw)),
        row(lax.dynamic_slice_in_dim(s_up, f * fl, fl)), row(lax.dynamic_slice_in_dim(s_gate, f * fl, fl)),
    ])
    par = jnp.pad(par, ((0, 3), (0, 0)))
    hall, wq, wo, wu, raw, qkv, res, mine, attn, mid = first(S, FS, hp, x, seg, w_qkv, w_out, par, w_upgate)
    out, g_mid, du, dd, vec = second(S, FS, mid, cotangent[0], w_down, par, wu, w_upgate)
    gh1, ps, dout, dqkv, dn_a, vec2 = third(
        S, FS, hp, g_mid, x, attn, mine, seg, par, wo, wq, qkv, raw, res, hall, dd
    )
    d_up, dn_b, d_o, g_x, d_q, tot, parts = fourth(S, FS, hp, vec, vec2, x, gh1, ps, du, dd, dout, dqkv)
    d_down = jnp.concatenate([dn_a[0], dn_b[0], dn_a[1], dn_b[1]])
    sqk = parts[:, 2, :hw].reshape(-1)

    def own(v):
        return lax.dynamic_slice_in_dim(v, f * rows, rows)

    return (
        out[None], g_x[None], d_q.astype(F32), d_o.astype(F32), d_up.astype(F32), d_down.astype(F32),
        own(sqk), own(tot[1]), own(tot[0]), tot[3, :fl], tot[4, :fl],
    )


def solution(mesh):
    S, FS = mesh.shape["seq"], mesh.shape["fsdp"]
    tok = P(("grp", "fsdp"), "seq", None)
    w = P("fsdp", None)
    in_specs = (tok, P(("grp", "fsdp"), None), w, w, w, w, P(), P(), P(), P(), P(), tok)
    out_specs = (tok, tok, w, w, w, w) + (P("fsdp"),) * 5

    def run(*args):
        return body(S, FS, *args)

    return jax.shard_map(run, mesh=mesh, in_specs=in_specs, out_specs=out_specs, check_vma=False)
```

```python
import jax
import jax.numpy as jnp
from jax import lax
from jax.experimental import pallas as pl
from jax.experimental.pallas import tpu as pltpu
from jax.sharding import PartitionSpec as P

D = 1280
HEADS = 20
HEAD = 64

eps_norm = 1e-06
neg_big = -1e30
BF = jnp.bfloat16
F32 = jnp.float32
MESH = pl.DeviceIdType.MESH
ANY = pl.BlockSpec(memory_space=pl.ANY)
VM = pl.BlockSpec(memory_space=pltpu.VMEM)


def inv_rms(value):
    return lax.rsqrt(jnp.mean(value * value, axis=-1, keepdims=True) + eps_norm)


def back(unit, inv, grad):
    return (grad - unit * jnp.mean(grad * unit, axis=-1, keepdims=True)) * inv


def mm(a, b):
    return jnp.dot(a, b, preferred_element_type=F32)


def mm_nt(a, b):
    return lax.dot_general(a, b, (((1,), (1,)), ((), ())), preferred_element_type=F32)


def mm_tn(a, b):
    return lax.dot_general(a, b, (((0,), (0,)), ((), ())), preferred_element_type=F32)


def rcopy(src, dst, ss, rs, dev):
    return pltpu.make_async_remote_copy(src, dst, ss, rs, device_id=dev, device_id_type=MESH)


def greet(peers):
    bar = pltpu.get_barrier_semaphore()
    for p in peers:
        pl.semaphore_signal(bar, inc=1, device_id=p, device_id_type=MESH)
    pl.semaphore_wait(bar, len(peers))


def ds(start, size, mult):
    return pl.ds(pl.multiple_of(start, mult), size)


def visible(seg_col, seg_row, q0, k0, nq, nk):
    qi = q0 + lax.broadcasted_iota(jnp.int32, (nq, nk), 0)
    ki = k0 + lax.broadcasted_iota(jnp.int32, (nq, nk), 1)
    return (ki <= qi) & ((seg_row == 0) | (seg_row == seg_col))


def add_into(dst, src, chunk, out=None):
    out = dst if out is None else out

    def one(i, carry):
        at = ds(i * chunk, chunk, 16)
        out[at] = (dst[at].astype(F32) + src[at].astype(F32)).astype(dst.dtype)
        return carry

    lax.fori_loop(0, src.shape[0] // chunk, one, 0)


def attn_bias(S, tok, half, bias, segr):
    for qb in range(S):
        q0 = qb * tok
        column = jnp.transpose(jnp.broadcast_to(segr[:, q0 : q0 + tok], (128, tok)))[:, :1]
        k0 = q0 if q0 < half else half
        nk = q0 + tok - k0
        ok = visible(column, segr[:, k0 : k0 + nk], q0, k0, tok, nk)
        bias[qb, :, :nk] = jnp.where(ok, 0.0, neg_big).astype(BF)


def first_kernel(S, FS, hp, x_ref, segr, wqkv, wout, par, wup,
                 hall_o, wq_o, wo_o, wu_o, raw_o, qkv_o, res_o, mine_o, attn_o, mid_o,
                 hall, wq, wo, raw, qkv, res, bias, oh, mixs, mine, recv,
                 s_up, r_up, s_dn, r_dn, s_wq, r_wq, s_wo, r_wo, s_wu, r_wu, f_wq, f_wo, f_wu,
                 g_wq, g_wo, g_wu, s_mx, r_mx, out_sem):
    g, z, f = lax.axis_index("grp"), lax.axis_index("seq"), lax.axis_index("fsdp")
    tok = x_ref.shape[0]
    rows = wqkv.shape[0]
    hr = rows // 2
    hw = hp * HEAD
    ff = wup.shape[1] // 2
    fl = ff // FS
    total = S * tok
    half = total // 2
    fpeers = [lax.rem(f + i, FS) for i in range(1, FS)]
    zpeers = [lax.rem(z + i, S) for i in range(1, S)]
    greet([(g, z, p) for p in fpeers] + [(g, p, f) for p in zpeers] + [(1 - g, z, f)])

    x = x_ref[...].astype(F32)
    hall[z] = (x * inv_rms(x)).astype(BF)

    def up(t, b):
        return rcopy(hall.at[b], hall.at[b], s_up.at[t], r_up.at[t], (g, lax.rem(z + 1, S), f))

    def down(t, b):
        return rcopy(hall.at[b], hall.at[b], s_dn.at[t], r_dn.at[t], (g, lax.rem(z + S - 1, S), f))

    @pl.when(z + 1 < S)
    def _():
        up(0, z).start()

    @pl.when(z > 0)
    def _():
        down(0, z).start()

    for k in range(S):
        lo, hi = k * hw, min((k + 1) * hw, D)

        @pl.when(z == k)
        def _():
            parts = []
            for c in range(3):
                if hi > lo:
                    parts.append(wqkv[:, c * D + lo : c * D + hi])
                if hi - lo < hw:
                    parts.append(jnp.zeros((rows, hw - max(hi - lo, 0)), BF))
            wq[ds(f * rows, rows, 16)] = jnp.concatenate(parts, axis=1)

    def wq_half(src, gg):
        return wq.at[ds(src * rows + gg * hr, hr, 16)]

    def wo_half(src, gg):
        return wo.at[ds(src * rows + gg * hr, hr, 16)]

    c_wq = [rcopy(wq_half(f, g), wq_half(f, g), s_wq.at[i], r_wq.at[i], (g, z, p)) for i, p in enumerate(fpeers)]
    for c in c_wq:
        c.start()
    attn_bias(S, tok, half, bias, segr)
    wo[ds(f * rows, rows, 16)] = wout[...]
    qkv[2, :, :, HEAD:] = jnp.where(lax.broadcasted_iota(jnp.int32, (hp, total, HEAD), 2) == 0, 1.0, 0.0).astype(BF)

    bpeers = [lax.rem(f + FS - i, FS) for i in range(1, FS)]
    partner = (1 - g, z, f)
    fw_wq = [rcopy(wq_half(p, g), wq_half(p, g), f_wq.at[i], g_wq.at[i], partner) for i, p in enumerate(bpeers)]
    for i in range(FS - 1):
        c_wq[i].wait_recv()
        fw_wq[i].start()
    c_wo = [rcopy(wo_half(f, g), wo_half(f, g), s_wo.at[i], r_wo.at[i], (g, z, p)) for i, p in enumerate(fpeers)]
    for c in c_wo:
        c.start()

    def wu_cp(i, p):
        return rcopy(wup.at[:, ds(g * ff + p * fl, fl, 128)], wu_o.at[g, f], s_wu.at[i], r_wu.at[i], (g, z, p))

    c_wu = [wu_cp(i, p) for i, p in enumerate(fpeers)]
    for c in c_wu:
        c.start()
    for i in range(FS - 1):
        fw_wq[i].wait_recv()

    def step(i, carry):
        t = lax.div(i - 1, 2)
        is_up = lax.rem(i, 2) == 1
        b = jnp.where(i == 0, z, jnp.where(is_up, z - 1 - t, z + 1 + t))

        @pl.when((b >= 0) & (b < S))
        def _():
            @pl.when((i > 0) & is_up)
            def _():
                up(t, b).wait_recv()

                @pl.when(z + 1 < S)
                def _():
                    up(t + 1, b).start()

            @pl.when((i > 0) & jnp.logical_not(is_up))
            def _():
                down(t, b).wait_recv()

                @pl.when(z > 0)
                def _():
                    down(t + 1, b).start()

            acc = mm(hall[b], wq[...])
            at = ds(b * tok, tok, 16)
            for j in range(hp):
                for c in range(2):
                    v = acc[:, c * hw + j * HEAD : c * hw + (j + 1) * HEAD]
                    raw[j, at, c * HEAD : (c + 1) * HEAD] = v
                    u = v * inv_rms(v) * par[:, 2 * D + j * HEAD : 2 * D + (j + 1) * HEAD]
                    qkv[c, j, at, :HEAD] = u.astype(BF)
                qkv[2, j, at, :HEAD] = acc[:, 2 * hw + j * HEAD : 2 * hw + (j + 1) * HEAD].astype(BF)

        return carry

    lax.fori_loop(0, 2 * S - 1, step, 0)
    outs = [
        pltpu.make_async_copy(hall, hall_o, out_sem.at[0]),
        pltpu.make_async_copy(wq, wq_o, out_sem.at[1]),
        pltpu.make_async_copy(raw, raw_o, out_sem.at[2]),
        pltpu.make_async_copy(qkv, qkv_o, out_sem.at[3]),
    ]
    for c in outs:
        c.start()

    def mx(qb):
        return rcopy(mixs.at[qb], recv.at[z], s_mx.at[qb], r_mx.at[z], (g, qb, f))

    for qb in reversed(range(S)):
        q0 = qb * tok
        n = q0 + tok
        k0 = q0 if q0 < half else half

        def head(j, carry):
            q = qkv[0, j, q0:n, :HEAD] * jnp.asarray(HEAD**-0.5, BF)
            s = mm_nt(q, qkv[1, j, :n, :HEAD])
            tail = s[:, k0:] + bias[qb, :, : n - k0].astype(F32)
            e = jnp.exp(jnp.concatenate([s[:, :k0], tail], axis=1) if k0 else tail)
            o = mm(e.astype(BF), qkv[2, j, :n])
            rinv = 1.0 / o[:, HEAD : HEAD + 1]
            o = o[:, :HEAD] * rinv
            res[j, q0:n, :HEAD] = o
            res[j, q0:n, HEAD:] = jnp.broadcast_to(rinv, (tok, HEAD))
            oh[j] = o.astype(BF)
            return carry

        lax.fori_loop(0, hp, head, 0)
        block = jnp.concatenate([oh[j] for j in range(hp)], axis=1)
        mixs[qb] = block

        @pl.when(z != qb)
        def _():
            mx(qb).start()

        @pl.when(z == qb)
        def _():
            recv[qb] = block

        if qb == S - 1:
            fw_wo = [rcopy(wo_half(p, g), wo_half(p, g), f_wo.at[i], g_wo.at[i], partner) for i, p in enumerate(bpeers)]
            for i in range(FS - 1):
                c_wo[i].wait_recv()
                fw_wo[i].start()

    fw_wu = [rcopy(wu_o.at[g, p], wu_o.at[g, p], f_wu.at[i], g_wu.at[i], partner) for i, p in enumerate(bpeers)]
    for i in range(FS - 1):
        c_wu[i].wait_recv()
        fw_wu[i].start()
    for i in range(FS - 1):
        fw_wo[i].wait_recv()
    outs2 = [pltpu.make_async_copy(wo, wo_o, out_sem.at[4]), pltpu.make_async_copy(res, res_o, out_sem.at[5])]
    for c in outs2:
        c.start()
    for k in range(S):
        @pl.when(z != k)
        def _():
            rcopy(mixs.at[0], recv.at[k], s_mx.at[0], r_mx.at[k], (g, k, f)).wait_recv()

    mine[...] = jnp.concatenate([recv[k] for k in range(S)], axis=1)[:, :D]
    attn = mm(mine[...], wo[...])
    attn_o[...] = attn
    mine_o[...] = mine[...]
    x = x_ref[...].astype(F32)
    h = x * inv_rms(x)
    n_ = h + par[:, :D] * (attn * inv_rms(attn) - h)
    mid_o[...] = n_ * inv_rms(n_)

    for t in range(S - 1):
        @pl.when((z + 1 < S) & (z - t >= 0))
        def _():
            up(t, z).wait_send()

        @pl.when((z > 0) & (z + t < S))
        def _():
            down(t, z).wait_send()

    for i in range(FS - 1):
        c_wq[i].wait_send()
        c_wo[i].wait_send()
        c_wu[i].wait_send()
        fw_wq[i].wait_send()
        fw_wo[i].wait_send()
        fw_wu[i].wait()
    for k in range(S):
        @pl.when(z != k)
        def _():
            mx(k).wait_send()
    for c in outs + outs2:
        c.wait()


def first(S, FS, hp, x, seg, wqkv, wout, par, wup):
    tok, total = x.shape[0], seg.shape[0]
    rows = wqkv.shape[0]
    hw = hp * HEAD
    fl = wup.shape[1] // 2 // FS
    sds = jax.ShapeDtypeStruct
    outs = [
        sds((S, tok, D), BF), sds((D, 3 * hw), BF), sds((D, D), BF), sds((2, FS, rows, fl), BF),
        sds((hp, total, 2 * HEAD), F32), sds((3, hp, total, 2 * HEAD), BF), sds((hp, total, 2 * HEAD), F32),
        sds((tok, D), BF), sds((tok, D), F32), sds((tok, D), F32),
    ]
    dma = lambda n: pltpu.SemaphoreType.DMA((n,))
    F1 = FS - 1
    return pl.pallas_call(
        lambda *refs: first_kernel(S, FS, hp, *refs),
        out_shape=outs,
        in_specs=[VM] * 5 + [ANY],
        out_specs=[ANY] * 7 + [VM] * 3,
        scratch_shapes=[
            pltpu.VMEM((S, tok, D), BF), pltpu.VMEM((D, 3 * hw), BF), pltpu.VMEM((D, D), BF),
            pltpu.VMEM((hp, total, 2 * HEAD), F32), pltpu.VMEM((3, hp, total, 2 * HEAD), BF),
            pltpu.VMEM((hp, total, 2 * HEAD), F32), pltpu.VMEM((S, tok, total // 2), BF),
            pltpu.VMEM((hp, tok, HEAD), BF), pltpu.VMEM((S, tok, hw), BF), pltpu.VMEM((tok, D), BF),
            pltpu.VMEM((S, tok, hw), BF),
            dma(S), dma(S), dma(S), dma(S), dma(F1), dma(F1), dma(F1), dma(F1), dma(F1), dma(F1),
            dma(F1), dma(F1), dma(F1), dma(F1), dma(F1), dma(F1), dma(S), dma(S), dma(6),
        ],
        compiler_params=pltpu.CompilerParams(collective_id=1, has_side_effects=True, vmem_limit_bytes=60 * 2**20),
        name="first",
    )(x, seg.reshape(1, total), wqkv, wout, par, wup)


def second_kernel(S, FS, NC, mid, cot, wd, par, wu_i, wup,
                  out_o, gmid_o, du_o, dd_o, vec_o,
                  wu, mida, up, gate, hid, ps, pr, rl, gma, gu, dup, ddn, lu, ld,
                  s_a, r_a, s_b, r_b, s_c, r_c, s_d, r_d, w_sem, s_x, r_x, out_sem):
    g, z, f = lax.axis_index("grp"), lax.axis_index("seq"), lax.axis_index("fsdp")
    tok = mid.shape[0]
    ct = tok // NC
    hc = ct // 2
    fl = wd.shape[0]
    ff = wup.shape[1] // 2
    rows = wup.shape[0]
    hl = fl // 2
    nt = 256 if fl % 256 == 0 else 128
    M = FS * ct
    relay = FS == 4
    peers = [lax.rem(f + i, FS) for i in range(1, FS)]
    partner = (1 - g, z, f)
    greet([(g, z, p) for p in peers] + [partner])
    R = range(FS - 1)
    A, B = pl.ds(0, hc), pl.ds(hc, hc)
    if relay:
        fx, fy, fd = f + 1 - 2 * lax.rem(f, 2), lax.rem(f + 2, 4), 3 - f
        dx, dy = (g, z, fx), (g, z, fy)

    def direct(buf, ss, rs, c, i):
        return rcopy(buf.at[c, f], buf.at[c, f], ss.at[c, i], rs.at[c, i], (g, z, peers[i]))

    def gcopy(buf, ss, rs, c, k):
        src, half, dev = ((f, A, dx), (f, B, dx), (f, B, dy), (f, A, dy), (fx, A, dy), (fy, B, dx))[k]
        view = buf.at[c, src, half]
        return rcopy(view, view, ss.at[c, k], rs.at[c, k], dev)

    def g_issue(buf, ss, rs, c):
        if relay:
            for k in (0, 2, 1, 3):
                gcopy(buf, ss, rs, c, k).start()
        else:
            for i in R:
                direct(buf, ss, rs, c, i).start()

    def g_relay(buf, ss, rs, c):
        if relay:
            for k in (0, 2):
                gcopy(buf, ss, rs, c, k).wait_recv()
                gcopy(buf, ss, rs, c, 4 if k == 0 else 5).start()

    def g_wait(buf, ss, rs, c):
        if relay:
            for k in (1, 3, 4, 5):
                gcopy(buf, ss, rs, c, k).wait_recv()
        else:
            for i in R:
                direct(buf, ss, rs, c, i).wait_recv()

    def g_sent(buf, ss, rs, c):
        if relay:
            for k in range(6):
                gcopy(buf, ss, rs, c, k).wait_send()
        else:
            for i in R:
                direct(buf, ss, rs, c, i).wait_send()

    def scopy(ss, rs, c, k):
        src, dst, dev = (
            (ps.at[c, fd, A], rl.at[c, 0], dx),
            (ps.at[c, fd, B], rl.at[c, 1], dy),
            (ps.at[c, fx, A], pr.at[c, 0, A], dx),
            (ps.at[c, fy, B], pr.at[c, 1, B], dy),
            (ps.at[c, fy, A], pr.at[c, 1, A], dy),
            (ps.at[c, fx, B], pr.at[c, 0, B], dx),
        )[k]
        return rcopy(src, dst, ss.at[c, k], rs.at[c, k], dev)

    def sdirect(ss, rs, c, i):
        return rcopy(ps.at[c, peers[i]], pr.at[c, i], ss.at[c, i], rs.at[c, i], (g, z, peers[i]))

    def s_issue(ss, rs, c):
        if relay:
            for k in range(4):
                scopy(ss, rs, c, k).start()
        else:
            for i in R:
                sdirect(ss, rs, c, i).start()

    def s_relay(ss, rs, c):
        if relay:
            for k, tgt, half in ((0, fy, A), (1, fx, B)):
                scopy(ss, rs, c, k).wait_recv()
                ps[c, tgt, half] = (ps[c, tgt, half].astype(F32) + rl[c, k].astype(F32)).astype(BF)
                scopy(ss, rs, c, 4 + k).start()

    def s_total(ss, rs, c):
        if relay:
            for k in range(2, 6):
                scopy(ss, rs, c, k).wait_recv()
        else:
            for i in R:
                sdirect(ss, rs, c, i).wait_recv()
        acc = ps[c, f].astype(F32)
        for i in range(2 if relay else FS - 1):
            acc = acc + pr[c, i].astype(F32)
        return acc

    def s_sent(ss, rs, c):
        if relay:
            for k in range(6):
                scopy(ss, rs, c, k).wait_send()
        else:
            for i in R:
                sdirect(ss, rs, c, i).wait_send()

    for c in range(NC):
        mida[c, f] = mid[c * ct : (c + 1) * ct].astype(BF)
        g_issue(mida, s_a, r_a, c)
        if c == 0:
            loads = []
            for k in range(2):
                loads.append(pltpu.make_async_copy(wup.at[:, ds(k * ff + f * fl, fl, 128)], wu.at[k, ds(f * rows, rows, 16)], w_sem.at[k, 0]))
                for i in R:
                    loads.append(pltpu.make_async_copy(wu_i.at[k, peers[i]], wu.at[k, ds(peers[i] * rows, rows, 16)], w_sem.at[k, i + 1]))
            for ld_c in loads:
                ld_c.start()
            vec_o[...] = jnp.zeros_like(vec_o)
        g_relay(mida, s_a, r_a, c)
    for ld_c in loads:
        ld_c.wait()

    for c in range(NC):
        g_wait(mida, s_a, r_a, c)

        def fwd(t, carry):
            cols = ds(t * nt, nt, 128)
            a_in = mida[c].reshape(M, D)
            u = mm(a_in, wu[0, :, cols])
            gt = mm(a_in, wu[1, :, cols])
            up[c, :, cols] = u
            gate[c, :, cols] = gt
            a = gt * par[:, ds(3 * D + ff + f * fl + t * nt, nt, 128)]
            hid[c, :, cols] = (u * par[:, ds(3 * D + f * fl + t * nt, nt, 128)] * (a * jax.nn.sigmoid(a))).astype(BF)
            return carry

        lax.fori_loop(0, fl // nt, fwd, 0)
        if c:
            s_relay(s_b, r_b, c - 1)

        def proj(t, carry):
            cols = ds(t * 256, 256, 128)
            ps[c, :, :, cols] = mm(hid[c], wd[:, cols]).astype(BF).reshape(FS, ct, 256)
            return carry

        lax.fori_loop(0, D // 256, proj, 0)
        s_issue(s_b, r_b, c)
    s_relay(s_b, r_b, NC - 1)

    for c in range(NC):
        at = slice(c * ct, (c + 1) * ct)
        mlp = s_total(s_b, r_b, c)
        al = par[:, D : 2 * D]
        md = mid[at]
        inv_m = inv_rms(mlp)
        um = mlp * inv_m
        dif = um - md
        m = md + al * dif
        inv_o = inv_rms(m)
        o = m * inv_o
        out_o[at] = o.astype(BF)
        g_m = back(o, inv_o, cot[at].astype(F32))
        vec_o[0:1] += jnp.sum(g_m * dif, axis=0, keepdims=True)
        gmid_o[at] = (1 - al) * g_m
        gma[c, f] = back(um, inv_m, al * g_m).astype(BF)
        g_issue(gma, s_c, r_c, c)
        g_relay(gma, s_c, r_c, c)

    for c in range(NC):
        g_wait(gma, s_c, r_c, c)

        def bwd(t, carry):
            cols = ds(t * nt, nt, 128)
            gh = mm_nt(gma[c].reshape(M, D), wd[cols, :])
            u = up[c, :, cols]
            gt = gate[c, :, cols]
            sgc = par[:, ds(3 * D + ff + f * fl + t * nt, nt, 128)]
            suc = par[:, ds(3 * D + f * fl + t * nt, nt, 128)]
            a = gt * sgc
            sig = jax.nn.sigmoid(a)
            gs = gh * (a * sig)
            gu[0, c, :, cols] = (gs * suc).astype(BF)
            vec_o[3:4, cols] += jnp.sum(u * gs, axis=0, keepdims=True)
            g_a = gh * u * suc * (sig * (1 + a * (1 - sig)))
            gu[1, c, :, cols] = (g_a * sgc).astype(BF)
            vec_o[4:5, cols] += jnp.sum(gt * g_a, axis=0, keepdims=True)
            return carry

        lax.fori_loop(0, fl // nt, bwd, 0)
        if c:
            s_relay(s_d, r_d, c - 1)
        s_sent(s_b, r_b, c)

        def bproj(t, carry):
            cols = ds(t * 256, 256, 128)
            v = mm_nt(gu[0, c], wu[0, cols, :]) + mm_nt(gu[1, c], wu[1, cols, :])
            ps[c, :, :, cols] = v.astype(BF).reshape(FS, ct, 256)
            return carry

        lax.fori_loop(0, D // 256, bproj, 0)
        s_issue(s_d, r_d, c)

    def dwd(t, carry):
        cols = ds(t * nt, nt, 128)
        ddn[cols, :] = mm_tn(hid[:, :, cols].reshape(NC * M, nt), gma[...].reshape(NC * M, D)).astype(BF)
        return carry

    lax.fori_loop(0, fl // nt, dwd, 0)
    s_relay(s_d, r_d, NC - 1)
    x_d = rcopy(ddn.at[ds((1 - g) * hl, hl, 16)], ld, s_x.at[0], r_x.at[0], partner)
    x_d.start()

    def dwu(k):
        def one(t, carry):
            cols = ds(t * 256, 256, 128)
            dup[k, cols, :] = mm_tn(mida[:, :, :, cols].reshape(NC * M, 256), gu[k].reshape(NC * M, fl)).astype(BF)
            return carry

        lax.fori_loop(0, D // 256, one, 0)

    dwu(1 - g)
    x_u = rcopy(dup.at[1 - g], lu, s_x.at[1], r_x.at[1], partner)
    x_u.start()
    dwu(g)
    mine = ds(g * hl, hl, 16)
    x_d.wait_recv()
    add_into(ddn.at[mine], ld, 64)
    o_d = pltpu.make_async_copy(ddn.at[mine], dd_o, out_sem.at[0])
    o_d.start()
    x_u.wait_recv()
    add_into(dup.at[g], lu, 64)
    o_u = pltpu.make_async_copy(dup.at[g], du_o, out_sem.at[1])
    o_u.start()

    for c in range(NC):
        at = slice(c * ct, (c + 1) * ct)
        gmid_o[at] = gmid_o[at] + s_total(s_d, r_d, c)
    for c in range(NC):
        g_sent(mida, s_a, r_a, c)
        g_sent(gma, s_c, r_c, c)
        s_sent(s_d, r_d, c)
    x_d.wait_send()
    x_u.wait_send()
    o_d.wait()
    o_u.wait()


def second(S, FS, mid, cot, wd, par, wu, wup):
    NC = 2
    tok = mid.shape[0]
    ct = tok // NC
    fl = wd.shape[0]
    M = FS * ct
    sds = jax.ShapeDtypeStruct
    outs = [sds((tok, D), BF), sds((tok, D), F32), sds((D, fl), BF), sds((fl // 2, D), BF),
            sds((8, D), F32)]
    dma = pltpu.SemaphoreType.DMA
    F1 = FS - 1
    return pl.pallas_call(
        lambda *refs: second_kernel(S, FS, NC, *refs),
        out_shape=outs,
        in_specs=[VM] * 4 + [ANY] * 2,
        out_specs=[VM, VM, ANY, ANY, VM],
        scratch_shapes=[
            pltpu.VMEM((2, D, fl), BF), pltpu.VMEM((NC, FS, ct, D), BF), pltpu.VMEM((NC, M, fl), F32),
            pltpu.VMEM((NC, M, fl), F32), pltpu.VMEM((NC, M, fl), BF), pltpu.VMEM((NC, FS, ct, D), BF),
            pltpu.VMEM((NC, 2 if FS == 4 else F1, ct, D), BF), pltpu.VMEM((NC, 2, ct // 2, D), BF),
            pltpu.VMEM((NC, FS, ct, D), BF), pltpu.VMEM((2, NC, M, fl), BF),
            pltpu.VMEM((2, D, fl), BF), pltpu.VMEM((fl, D), BF), pltpu.VMEM((D, fl), BF), pltpu.VMEM((fl // 2, D), BF),
        ] + [dma((NC, max(F1, 6)))] * 8 + [dma((2, FS)), dma((2,)), dma((2,)), dma((2,))],
        compiler_params=pltpu.CompilerParams(collective_id=2, has_side_effects=True, vmem_limit_bytes=63 * 2**20),
        name="second",
    )(mid, cot, wd, par, wu, wup)


def make_chain(S, pieces, outs, sems):
    s_in, r_raw, r_oth, s_ret, o_sem, s_o, r_o = sems
    g, z, f = lax.axis_index("grp"), lax.axis_index("seq"), lax.axis_index("fsdp")
    partner = (1 - g, z, f)
    lower = z < S // 2
    inner = jnp.where(lower, z + 1, z - 1)
    mid = (z == S // 2 - 1) | (z == S // 2)
    has_outer = (z > 0) & (z < S - 1)
    outer = jnp.where(has_outer, jnp.where(lower, z - 1, z + 1), inner)
    rest = jnp.logical_not(mid)

    def toward(i, to_mid):
        own, raw, oth, _ = pieces[i]
        if to_mid:
            return rcopy(own, oth, s_in.at[i], r_oth.at[i], (g, inner, f))
        return rcopy(own, raw, s_in.at[i], r_raw.at[i], (g, inner, f))

    def returned(i, from_mid):
        own, raw, oth, _ = pieces[i]
        return rcopy(raw if from_mid else oth, oth, s_ret.at[i], r_oth.at[i], (g, outer, f))

    def local_out(i, src):
        return pltpu.make_async_copy(src, pieces[i][3](outs), o_sem.at[i])

    def remote_out(i, src):
        return rcopy(src, pieces[i][3](outs), s_o.at[i], r_o.at[i], partner)

    def send(i):
        @pl.when(mid)
        def _():
            toward(i, True).start()

        @pl.when(rest)
        def _():
            toward(i, False).start()

    def launch(i):
        @pl.when(jnp.logical_not(has_outer))
        def _():
            send(i)

    def go_in(i):
        own, raw, oth, _ = pieces[i]

        @pl.when(has_outer)
        def _():
            rcopy(own, raw, s_in.at[i], r_raw.at[i], (g, outer, f)).wait_recv()
            add_into(own, raw, 80)
            send(i)

    def finish(i, src, from_mid):
        @pl.when(has_outer)
        def _():
            returned(i, from_mid).start()

        local_out(i, src).start()
        remote_out(i, src).start()

    def arrived(i):
        own, raw, oth, _ = pieces[i]
        rcopy(own, oth, s_in.at[i], r_oth.at[i], (g, inner, f)).wait_recv()

    def step(i, lag=5):
        if i < len(pieces):
            go_in(i)
        if 1 <= i <= len(pieces):
            @pl.when(mid)
            def _():
                own, raw, oth, _ = pieces[i - 1]
                arrived(i - 1)
                add_into(own, oth, 80, raw)
                finish(i - 1, raw, True)
        if lag <= i < len(pieces) + lag:
            @pl.when(rest)
            def _():
                arrived(i - lag)
                finish(i - lag, pieces[i - lag][2], False)

    def drain():
        for i in range(len(pieces)):
            toward(i, True).wait_send()

            @pl.when(has_outer)
            def _():
                returned(i, True).wait_send()

            local_out(i, pieces[i][1]).wait()
            remote_out(i, pieces[i][1]).wait()

    return launch, step, drain


def cuts(size, parts, unit):
    step = size // unit
    return [(a * step, (b - a) * step) for a, b in zip(parts[:-1], parts[1:])]


def third_kernel(S, FS, hp, gmid, x_ref, attn, mine, segr, par, wo, wq_i, qkv_i, raw_i, res_i, hall_i, dd_i,
                 gh1, ps_o, dout_o, dqkv_o, dn_o, vec_o,
                 dsq_o, gain, wq, qkv, raw, res, hall, ga, gsend, gxr, bias, hx, gqh, dkv, gq, ps, dout, dqk, lo, lq, own_d, raw_d, oth_d,
                 ld_sem, h_sem, s_gx, r_gx, s_p, s_x, r_x, out_sem, *chain_sems):
    g, z, f = lax.axis_index("grp"), lax.axis_index("seq"), lax.axis_index("fsdp")
    tok = x_ref.shape[0]
    hw = hp * HEAD
    wide = S * hw
    total = S * tok
    half = total // 2
    w2 = 3 * hw // 2
    dh = D // 2
    partner = (1 - g, z, f)
    greet([(g, lax.rem(z + i, S), f) for i in range(1, S)] + [partner])
    loads = [pltpu.make_async_copy(a, b, ld_sem.at[i]) for i, (a, b) in enumerate(
        [(qkv_i, qkv), (raw_i, raw), (res_i, res), (wq_i, wq)])]
    for c in loads:
        c.start()

    hl = own_d.shape[0]
    dd_c = pltpu.make_async_copy(dd_i.at[pl.ds(0, hl)], own_d, h_sem.at[2])
    dd_c.start()
    pieces = []
    for lo_r, n_r in cuts(hl, (0, 1, 2, 4) if hl % 64 == 0 else (0, 2, 4), 4):
        pieces.append((own_d.at[pl.ds(lo_r, n_r)], raw_d.at[pl.ds(lo_r, n_r)], oth_d.at[pl.ds(lo_r, n_r)],
                       lambda o, lo_r=lo_r, n_r=n_r: o.at[g, pl.ds(lo_r, n_r)]))
    launch, step, drain = make_chain(S, pieces, dn_o, chain_sems)
    n_p = len(pieces)

    def h_tile(t):
        return pltpu.make_async_copy(hall_i.at[:, :, pl.ds(t * 256, 256)], hall.at[t % 2], h_sem.at[t % 2])

    h_tile(0).start()
    h_tile(1).start()
    dd_c.wait()
    launch(0)
    vec_o[...] = jnp.zeros_like(vec_o)
    for j in range(hp):
        gain[j : j + 1] = par[:, 2 * D + j * HEAD : 2 * D + (j + 1) * HEAD]
    dsq_o[...] = jnp.zeros_like(dsq_o)
    cr = tok // 4

    def pre(i, carry):
        at = ds(i * cr, cr, 16)
        x = x_ref[at].astype(F32)
        h = x * inv_rms(x)
        av = attn[at]
        inv_a = inv_rms(av)
        ua = av * inv_a
        al = par[:, :D]
        dif = ua - h
        n_ = h + al * dif
        inv_n = inv_rms(n_)
        g_n = back(n_ * inv_n, inv_n, gmid[at])
        vec_o[1:2] += jnp.sum(g_n * dif, axis=0, keepdims=True)
        gh1[at] = (1 - al) * g_n
        ga[at] = back(ua, inv_a, al * g_n).astype(BF)
        return carry

    lax.fori_loop(0, 4, pre, 0)
    gmix = mm_nt(ga[...], wo[...]).astype(BF)
    if wide > D:
        gmix = jnp.concatenate([gmix, jnp.zeros((tok, wide - D), BF)], axis=1)
    for k in range(S):
        gsend[k] = gmix[:, k * hw : (k + 1) * hw]

    def gx(k):
        return rcopy(gsend.at[k], gxr.at[z], s_gx.at[k], r_gx.at[z], (g, k, f))

    for k in range(S):
        @pl.when(z != k)
        def _():
            gx(k).start()

        @pl.when(z == k)
        def _():
            gxr[k] = gsend[k]


    def dwo(t, carry):
        cols = ds(t * 256, 256, 128)
        v = mm_tn(mine[:, cols], ga[...]).astype(BF)
        dout[0, cols, :] = v[:, :dh]
        dout[1, cols, :] = v[:, dh:]
        return carry

    lax.fori_loop(0, D // 256, dwo, 0)
    x_o = rcopy(dout.at[1 - g], lo, s_x.at[0], r_x.at[0], partner)
    x_o.start()
    attn_bias(S, tok, half, bias, segr)
    for c in loads:
        c.wait()
    done = 0

    def part(k):
        return pltpu.make_async_copy(ps.at[k], ps_o.at[k], s_p.at[k])

    for qb in reversed(range(S)):
        q0 = qb * tok
        n = q0 + tok
        k0 = q0 if q0 < half else half

        @pl.when(z != qb)
        def _():
            rcopy(gsend.at[0], gxr.at[qb], s_gx.at[0], r_gx.at[qb], (g, qb, f)).wait_recv()

        if qb == S - 1:
            for i in range(1, n_p):
                launch(i)

        for j in range(hp):
            hx[j] = gxr[qb, :, j * HEAD : (j + 1) * HEAD]

        def head(j, carry):
            q = qkv[0, j, q0:n, :HEAD] * jnp.asarray(HEAD**-0.5, BF)
            keys = qkv[1, j, :n, :HEAD]
            gv = hx[j]
            rinv = res[j, q0:n, HEAD : HEAD + 1]
            delta = jnp.sum(gv.astype(F32) * res[j, q0:n, :HEAD], axis=-1, keepdims=True)
            s = mm_nt(q, keys)
            tail = s[:, k0:] + bias[qb, :, : n - k0].astype(F32)
            p = jnp.exp(jnp.concatenate([s[:, :k0], tail], axis=1) if k0 else tail) * rinv
            dp = mm_nt(gv, qkv[2, j, :n, :HEAD])
            dsb = (p * (dp - delta)).astype(BF)
            dq = mm(dsb, keys) * HEAD**-0.5
            dk = mm_tn(dsb, q)
            dv = mm_tn(p.astype(BF), gv)
            if qb < S - 1:
                dk = dk + dkv[j, :n, :HEAD]
                dv = dv + dkv[j, :n, HEAD:]
            if qb:
                dkv[j, :q0, :HEAD] = dk[:q0]
                dkv[j, :q0, HEAD:] = dv[:q0]
            gj = gain[pl.ds(j, 1), :]
            for c, d in ((0, dq), (1, dk[q0:])):
                v = raw[j, q0:n, c * HEAD : (c + 1) * HEAD]
                inv = inv_rms(v)
                u = v * inv
                dsq_o[pl.ds(j, 1), :] += jnp.sum(d * u, axis=0, keepdims=True)
                gqh[c, j] = back(u, inv, d * gj).astype(BF)
            gqh[2, j] = dv[q0:].astype(BF)
            return carry

        lax.fori_loop(0, hp, head, 0)
        gq[qb] = jnp.concatenate([gqh[c, j] for c in range(3) for j in range(hp)], axis=1)
        ps[qb] = mm_nt(gq[qb], wq[...]).astype(BF)

        part(qb).start()
        if done < n_p + 5:
            step(done)
            done += 1

    for t in range(D // 256):
        h_tile(t).wait()
        v = mm_tn(hall[t % 2].reshape(total, 256), gq[...].reshape(total, 3 * hw)).astype(BF)
        dqk[0, t * 256 : (t + 1) * 256, :] = v[:, :w2]
        dqk[1, t * 256 : (t + 1) * 256, :] = v[:, w2:]
        if t + 2 < D // 256:
            h_tile(t + 2).start()
    x_q = rcopy(dqk.at[1 - g], lq, s_x.at[1], r_x.at[1], partner)
    x_q.start()
    x_o.wait_recv()
    add_into(dout.at[g], lo, 128)
    o_o = pltpu.make_async_copy(dout.at[g], dout_o, out_sem.at[0])
    o_o.start()
    for j in range(hp):
        vec_o[2:3, j * HEAD : (j + 1) * HEAD] = dsq_o[j : j + 1]
    while done < n_p + 5:
        step(done)
        done += 1
    x_q.wait_recv()
    add_into(dqk.at[g], lq, 128)
    o_q = pltpu.make_async_copy(dqk.at[g], dqkv_o, out_sem.at[1])
    o_q.start()

    for k in range(S):
        @pl.when(z != k)
        def _():
            gx(k).wait_send()

        part(k).wait()
    x_o.wait_send()
    x_q.wait_send()
    o_o.wait()
    o_q.wait()
    drain()


def third(S, FS, hp, gmid, x, attn, mine, seg, par, wo, wq, qkv, raw, res, hall, dd):
    tok, total = x.shape[0], seg.shape[0]
    hw = hp * HEAD
    sds = jax.ShapeDtypeStruct
    outs = [sds((tok, D), F32), sds((S, tok, D), BF), sds((D, D // 2), BF), sds((D, 3 * hw // 2), BF), sds((2, dd.shape[0] // 2, D), BF),
            sds((8, D), F32)]
    dma = lambda n: pltpu.SemaphoreType.DMA((n,))
    hd = pltpu.VMEM((dd.shape[0] // 2, D), BF)
    return pl.pallas_call(
        lambda *refs: third_kernel(S, FS, hp, *refs),
        out_shape=outs,
        in_specs=[VM] * 7 + [ANY] * 6,
        out_specs=[VM, ANY, ANY, ANY, ANY, VM],
        scratch_shapes=[
            pltpu.VMEM((hp, HEAD), F32), pltpu.VMEM((hp, HEAD), F32),
            pltpu.VMEM((D, 3 * hw), BF), pltpu.VMEM((3, hp, total, 2 * HEAD), BF), pltpu.VMEM((hp, total, 2 * HEAD), F32),
            pltpu.VMEM((hp, total, 2 * HEAD), F32), pltpu.VMEM((2, S, tok, 256), BF),
            pltpu.VMEM((tok, D), BF), pltpu.VMEM((S, tok, hw), BF), pltpu.VMEM((S, tok, hw), BF),
            pltpu.VMEM((S, tok, total // 2), BF), pltpu.VMEM((hp, tok, HEAD), BF), pltpu.VMEM((3, hp, tok, HEAD), BF),
            pltpu.VMEM((hp, total, 2 * HEAD), F32), pltpu.VMEM((S, tok, 3 * hw), BF), pltpu.VMEM((S, tok, D), BF),
            pltpu.VMEM((2, D, D // 2), BF), pltpu.VMEM((2, D, 3 * hw // 2), BF),
            pltpu.VMEM((D, D // 2), BF), pltpu.VMEM((D, 3 * hw // 2), BF),
            hd, hd, hd,
            dma(4), dma(3), dma(S), dma(S), dma(S), dma(2), dma(2), dma(2),
        ] + [dma(5)] * 7,
        compiler_params=pltpu.CompilerParams(collective_id=3, has_side_effects=True, vmem_limit_bytes=63 * 2**20),
        name="third",
    )(gmid, x, attn, mine, seg.reshape(1, total), par, wo, wq, qkv, raw, res, hall, dd)


def fourth_kernel(S, FS, hp, vec, vec2, x_ref, gh1, ps_i, du, dd, dout, dqkv,
                  up_o, dn_o, out_o, gx_o, qkv_o, vec_o, sqk_o,
                  own_u, raw_u, oth_u, own_d, raw_d, oth_d, own_o, raw_o, oth_o, so, xo, sq, xq, agq, ps, pr, va, vb, vf, vz,
                  ld_sem, s_u, r_u, s_xo, r_xo, s_xq, r_xq, s_au, r_au, s_ad, r_ad, s_fq, r_fq, s_v, r_v,
                  s_p, r_p, *chain_sems):
    g, z, f = lax.axis_index("grp"), lax.axis_index("seq"), lax.axis_index("fsdp")
    tok = x_ref.shape[0]
    rows = own_u.shape[1]
    fl = own_u.shape[2]
    ff = fl * FS
    hw = hp * HEAD
    dh = D // 2
    peers = [lax.rem(f + i, FS) for i in range(1, FS)]
    bpeers = [lax.rem(f + FS - i, FS) for i in range(1, FS)]
    zpeers = [lax.rem(z + i, S) for i in range(1, S)]
    above, below = (g, lax.rem(z + 1, S), f), (g, lax.rem(z + S - 1, S), f)
    partner = (1 - g, z, f)
    first_z, last_z = z == 0, z == S - 1
    R = range(FS - 1)
    greet([(g, z, p) for p in peers] + [(g, p, f) for p in zpeers] + [partner])

    def blk(p):
        return ds(p * rows, rows, 16)

    l_u = pltpu.make_async_copy(du.at[blk(f)], own_u.at[f], ld_sem.at[0])
    l_p = pltpu.make_async_copy(ps_i, ps, ld_sem.at[3])
    l_q = pltpu.make_async_copy(dqkv.at[blk(f)], sq, ld_sem.at[1])
    l_o = pltpu.make_async_copy(dout.at[blk(f)], so, ld_sem.at[2])
    hl = own_d.shape[0]
    l_d = pltpu.make_async_copy(dd.at[pl.ds(hl, hl)], own_d, ld_sem.at[4])
    for c in (l_d, l_p, l_u, l_q, l_o):
        c.start()
    c_q = [rcopy(dqkv.at[blk(p)], xq.at[i], s_xq.at[i], r_xq.at[i], (g, z, p)) for i, p in enumerate(peers)]
    c_u = [rcopy(du.at[blk(p)], own_u.at[f], s_u.at[i], r_u.at[i], (g, z, p)) for i, p in enumerate(peers)]
    c_o = [rcopy(dout.at[blk(p)], xo.at[i], s_xo.at[i], r_xo.at[i], (g, z, p)) for i, p in enumerate(peers)]
    for c in c_q + c_u + c_o:
        c.start()
    va[...] = vec[...] + vec2[...]
    v_c = rcopy(va, vb, s_v.at[0], r_v.at[0], partner)
    v_c.start()

    pieces = []
    for lo_r, n_r in cuts(hl, (0, 1, 2), 2):
        a = pl.ds(lo_r, n_r)
        pieces.append((own_d.at[a], raw_d.at[a], oth_d.at[a], lambda o, a=a: o[2].at[g, a]))
    for p in [f] + bpeers:
        for lo_r, n_r in cuts(rows, (0, 1, 2), 2):
            a = pl.ds(lo_r, n_r)
            pieces.append((own_u.at[p, a], raw_u.at[p, a], oth_u.at[p, a],
                           lambda o, p=p, a=a: o[0].at[a, ds(g * ff + p * fl, fl, 128)]))
    for lo_r, n_r in cuts(rows, (0, 1, 2), 2):
        a = pl.ds(lo_r, n_r)
        pieces.append((own_o.at[a], raw_o.at[a], oth_o.at[a], lambda o, a=a: o[1].at[a, ds(g * dh, dh, 128)]))
    launch, step, drain = make_chain(S, pieces, (up_o, out_o, dn_o), chain_sems)

    def add_all(own, recv):
        acc = own[...].astype(F32)
        for i in R:
            acc = acc + recv[i].astype(F32)
        return acc.astype(BF)

    def go_up(b):
        return rcopy(ps.at[b], pr.at[b], s_p.at[b], r_p.at[b], above)

    def go_down(b):
        slot = jnp.where(z == b + 1, S, b)
        return rcopy(ps.at[b], pr.at[slot], s_p.at[b], r_p.at[slot], below)

    def gh_end(c):
        @pl.when(first_z)
        def _():
            go_up(S - 1 - c).start()

        @pl.when(last_z)
        def _():
            go_down(c).start()

    def gh_mid(c):
        bu, bd = S - 1 - c + z, c - (S - 1 - z)

        def up():
            @pl.when((z > 0) & (bu > z) & (bu < S))
            def _():
                go_up(bu).wait_recv()
                add_into(ps.at[bu], pr.at[bu], 64)
                go_up(bu).start()

        def down():
            @pl.when((z < S - 1) & (bd >= 0) & (bd < z))
            def _():
                rcopy(ps.at[bd], pr.at[bd], s_p.at[bd], r_p.at[bd], above).wait_recv()
                add_into(ps.at[bd], pr.at[bd], 64)
                go_down(bd).start()

        @pl.when(z < S // 2)
        def _():
            up()

        down()

        @pl.when(z >= S // 2)
        def _():
            up()

    def piece(b):
        return agq.at[b, g]

    def a_up(t, b):
        return rcopy(piece(b), piece(b), s_au.at[t], r_au.at[t], above)

    def a_down(t, b):
        return rcopy(piece(b), piece(b), s_ad.at[t], r_ad.at[t], below)

    def fq(b):
        return rcopy(piece(b), piece(b), s_fq.at[b], r_fq.at[b], partner)

    def a_start():
        @pl.when(z < S - 1)
        def _():
            a_up(0, z).start()

        @pl.when(z > 0)
        def _():
            a_down(0, z).start()

        fq(z).start()

    def a_relay(t):
        bu, bd = z - 1 - t, z + 1 + t

        @pl.when(bu >= 0)
        def _():
            a_up(t, bu).wait_recv()

            @pl.when(z < S - 1)
            def _():
                a_up(t + 1, bu).start()

            fq(bu).start()

        @pl.when(bd < S)
        def _():
            a_down(t, bd).wait_recv()

            @pl.when(z > 0)
            def _():
                a_down(t + 1, bd).start()

            fq(bd).start()

    l_d.wait()
    launch(0)
    launch(1)
    l_p.wait()
    gh_end(0)
    v_c.wait()
    vf[f] = va[...] + vb[...]
    v_f = [rcopy(vf.at[f], vf.at[f], s_v.at[1 + i], r_v.at[1 + i], (g, z, p)) for i, p in enumerate(peers)]
    for c in v_f:
        c.start()
    l_q.wait()
    for c in c_q:
        c.wait()
    agq[z, g] = add_all(sq, xq)
    a_start()
    l_u.wait()
    l_o.wait()
    launch(2)
    launch(3)
    ends = first_z | last_z
    inner = jnp.logical_not(ends)

    def last_piece():
        for c in c_o:
            c.wait()
        own_o[...] = add_all(so, xo)

    @pl.when(ends)
    def _():
        for i in R:
            c_u[i].wait()
            launch(4 + 2 * i)
            launch(5 + 2 * i)
            if 1 + i < S - 2:
                gh_end(1 + i)
        last_piece()
        launch(4 + 2 * len(R))
        launch(5 + 2 * len(R))
        gh_end(S - 2)

    step(0)
    step(1)
    gh_mid(1)
    step(2)
    step(3)
    n = 4
    for i in R:
        if i < S - 1:
            a_relay(i)

        @pl.when(inner)
        def _():
            c_u[i].wait()

        step(n)
        step(n + 1)
        n += 2
        if 2 + i < S - 1:
            gh_mid(2 + i)
    for c in v_f:
        c.wait()
    acc = vf[0]
    for k in range(1, FS):
        acc = acc + vf[k]
    sub = lax.broadcasted_iota(jnp.int32, acc.shape, 0)
    vz[z] = jnp.where(sub < 3, acc, vf[f])
    v_z = [rcopy(vz.at[z], vz.at[z], s_v.at[FS + k], r_v.at[FS + k], (g, p, f)) for k, p in enumerate(zpeers)]
    for c in v_z:
        c.start()
    pl.when(inner)(last_piece)
    step(n)
    step(n + 1)
    n += 2
    for i in range(FS - 1, S - 1):
        a_relay(i)
    for c in v_z:
        c.wait()
    acc = vz[0]
    for i in range(1, S):
        acc = acc + vz[i]
    vec_o[...] = acc
    for i in range(S):
        sqk_o[i] = vz[i]
    step(n)
    step(n + 1)

    cr = tok // 4
    gx_o[...] = gh1[...]
    add_into(gx_o, ps.at[z], 64)

    @pl.when(z > 0)
    def _():
        go_up(z).wait_recv()
        add_into(gx_o, pr.at[z], 64)

    @pl.when(z < S - 1)
    def _():
        rcopy(ps.at[0], pr.at[S], s_p.at[0], r_p.at[S], above).wait_recv()
        add_into(gx_o, pr.at[S], 64)

    def post(i, carry):
        at = ds(i * cr, cr, 16)
        x = x_ref[at].astype(F32)
        inv = inv_rms(x)
        gx_o[at] = back(x * inv, inv, gx_o[at])
        return carry

    lax.fori_loop(0, 4, post, 0)
    for k in range(S):
        fq(k).wait_recv()
    full = [jnp.concatenate([agq[k, 0], agq[k, 1]], axis=1) for k in range(S)]
    cols = []
    for c in range(3):
        row = jnp.concatenate([full[k][:, c * hw : (c + 1) * hw] for k in range(S)], axis=1)
        cols.append(row[:, :D])
    qkv_o[...] = jnp.concatenate(cols, axis=1)
    for k in range(2, 5):
        step(n + k)
    for k in range(S):
        fq(k).wait_send()

        @pl.when(z != k)
        def _():
            go_up(k).wait_send()

    for t in range(S - 1):
        @pl.when((z < S - 1) & (z - t >= 0))
        def _():
            a_up(t, z).wait_send()

        @pl.when((z > 0) & (z + t < S))
        def _():
            a_down(t, z).wait_send()

    drain()


def fourth(S, FS, hp, vec, vec2, x, gh1, ps, du, dd, dout, dqkv):
    tok = x.shape[0]
    fl = du.shape[1]
    rows = D // FS
    hw = hp * HEAD
    w2 = 3 * hw // 2
    dh = D // 2
    n = 4 + 2 * FS
    sds = jax.ShapeDtypeStruct
    outs = [sds((rows, 2 * FS * fl), BF), sds((2, dd.shape[0] // 2, D), BF), sds((rows, D), BF), sds((tok, D), F32), sds((rows, 3 * D), BF),
            sds(vec.shape, F32), sds((S,) + vec.shape, F32)]
    dma = lambda k: pltpu.SemaphoreType.DMA((k,))
    F1 = FS - 1
    u, o = pltpu.VMEM((FS, rows, fl), BF), pltpu.VMEM((rows, dh), BF)
    hd = pltpu.VMEM((dd.shape[0] // 2, D), BF)
    v = pltpu.VMEM(vec.shape, F32)
    return pl.pallas_call(
        lambda *refs: fourth_kernel(S, FS, hp, *refs),
        out_shape=outs,
        in_specs=[VM] * 4 + [ANY] * 5,
        out_specs=[ANY, ANY, ANY, VM, VM, VM, VM],
        scratch_shapes=[
            u, u, u, hd, hd, hd, o, o, o, o, pltpu.VMEM((F1, rows, dh), BF),
            pltpu.VMEM((rows, w2), BF), pltpu.VMEM((F1, rows, w2), BF), pltpu.VMEM((S, 2, rows, w2), BF),
            pltpu.VMEM((S, tok, D), BF), pltpu.VMEM((S + 1, tok, D), BF),
            v, v, pltpu.VMEM((FS,) + vec.shape, F32), pltpu.VMEM((S,) + vec.shape, F32),
            dma(5), dma(F1), dma(F1), dma(F1), dma(F1), dma(F1), dma(F1),
            dma(S), dma(S), dma(S), dma(S), dma(S), dma(S), dma(FS + S), dma(FS + S), dma(S), dma(S + 1),
        ] + [dma(n)] * 7,
        compiler_params=pltpu.CompilerParams(collective_id=4, has_side_effects=True, vmem_limit_bytes=60 * 2**20),
        name="fourth",
    )(vec, vec2, x, gh1, ps, du, dd, dout, dqkv)


def body(S, FS, inputs, segments, w_qkv, w_out, w_upgate, w_down, s_qk, alpha_attn, alpha_mlp, s_up, s_gate, cotangent):
    z = lax.axis_index("seq")
    f = lax.axis_index("fsdp")
    hp = -(-HEADS // S)
    hw = hp * HEAD
    rows = w_qkv.shape[0]
    ff = s_up.shape[0]
    fl = ff // FS
    x = inputs[0]
    seg = segments[0]
    gains = jnp.pad(s_qk, (0, S * hw - D))

    def row(v):
        return jnp.pad(v, (0, D - v.size))

    par = jnp.concatenate([
        alpha_attn, alpha_mlp, row(lax.dynamic_slice_in_dim(gains, z * hw, hw)), s_up, s_gate
    ]).reshape(1, -1)
    hall, wq, wo, wu, raw, qkv, res, mine, attn, mid = first(S, FS, hp, x, seg, w_qkv, w_out, par, w_upgate)
    out, g_mid, du, dd, vec = second(S, FS, mid, cotangent[0], w_down, par, wu, w_upgate)
    gh1, ps, dout, dqkv, dn_a, vec2 = third(
        S, FS, hp, g_mid, x, attn, mine, seg, par, wo, wq, qkv, raw, res, hall, dd
    )
    d_up, dn_b, d_o, g_x, d_q, tot, parts = fourth(S, FS, hp, vec, vec2, x, gh1, ps, du, dd, dout, dqkv)
    d_down = jnp.concatenate([dn_a[0], dn_b[0], dn_a[1], dn_b[1]])
    sqk = parts[:, 2, :hw].reshape(-1)

    def own(v):
        return lax.dynamic_slice_in_dim(v, f * rows, rows)

    return (
        out[None], g_x[None], d_q.astype(F32), d_o.astype(F32), d_up.astype(F32), d_down.astype(F32),
        own(sqk), own(tot[1]), own(tot[0]), tot[3, :fl], tot[4, :fl],
    )


def solution(mesh):
    S, FS = mesh.shape["seq"], mesh.shape["fsdp"]
    tok = P(("grp", "fsdp"), "seq", None)
    w = P("fsdp", None)
    in_specs = (tok, P(("grp", "fsdp"), None), w, w, w, w, P(), P(), P(), P(), P(), tok)
    out_specs = (tok, tok, w, w, w, w) + (P("fsdp"),) * 5

    def run(*args):
        return body(S, FS, *args)

    return jax.shard_map(run, mesh=mesh, in_specs=in_specs, out_specs=out_specs, check_vma=False)
```
